256 devices in a mesh: grp: 2 (over z), spec: 128 (over x, y, core).
Axes of the slice: x: 8, y: 8, z: 2, core: 2. Of those that a mesh axis runs over, the one named last changes fastest.
The devices are a block of a 8x8x16 slice.
Arguments:
- spectrum: float32 [3072, 12288], P(('grp', 'spec')), parts along dimension 0, may hold values from 0.05 to 5
- sea_mask: int32 [12288], replicated, may hold values from 0 to 1, as said below
- wind_speed: float32 [24576], P('grp'), parts along dimension 0, may hold values from 0.3 to 3
- wind_angle: float32 [24576], P('grp'), parts along dimension 0, may hold values from -3.140625 to 3.140625
Outputs:
- new_spectrum: float32 [3072, 12288], P(('grp', 'spec')), parts along dimension 0
- wave_height: float32 [24576], P(('grp', 'spec')), parts along dimension 0
- mean_height: float32 [2], P('grp'), parts along dimension 0
The draws below stay inside these ranges and needn't reach their ends.
There are 2 independent parts, one for each index of `grp`. The reference program is written for one: setup_inputs(seed, part) draws one part's arguments, and reference() takes and returns one part's arrays. A program takes and returns all parts, laid end to end along the dimension named above; an argument that names none is the same for every part. Nothing has to cross between parts.
Inputs may be any that keep to these rules, and one draw needn't show every extreme that they name: `sea_mask`: exactly 8192 cells are sea.
All inputs are finite; a program needn't handle non-finite values.
Results may differ from the reference program's by a relative error of at most 0.00002.
Values sent between devices are 32-bit elements; how exact they have to be, the bound alone decides.
A program may use at most 64 MiB of HBM per device.

```python
import math
import jax
import jax.numpy as jnp
from jax import lax

NF = 48
ND = 32
NLON = 384
ADV_STEPS = 2
PTS_DEV = 96
BINS = 1536
CELLS = 12288
NLAT = 32
SEA = 8192
N_SPEC = 128


def draw_sea_mask(key, part):
    coarse_key, fine_key = jax.random.split(jax.random.fold_in(key, 17))
    block_rows = (NLAT + 7) // 8
    block_cols = (NLON + 7) // 8
    coarse = jax.random.randint(coarse_key, (block_rows, block_cols), 0, 64)
    fine = jax.random.randint(fine_key, (NLAT, NLON), 0, 16)
    row_ids = jnp.arange(NLAT, dtype=jnp.int32) // 8
    col_ids = jnp.arange(NLON, dtype=jnp.int32) // 8
    spread = coarse[row_ids][:, col_ids] * 16 + fine
    scores = spread.reshape(-1) * CELLS + jnp.arange(CELLS, dtype=jnp.int32)
    order = jnp.argsort(scores, stable=True)
    chosen = order[:SEA]
    return jnp.zeros((CELLS,), jnp.int32).at[chosen].set(1)


def levels(stream_key, shape, cuts, least, top_value):
    def one(position, blocks):
        draws = jax.random.uniform(jax.random.fold_in(jax.random.fold_in(stream_key, 6), position), (blocks,), jnp.float32, least / len(cuts), top_value / len(cuts))
        return jnp.repeat(jnp.exp(draws), shape[position] // blocks).reshape((-1,) + (1,) * (len(shape) - position - 1))

    factor_of = one(*cuts[0])
    for cut in cuts[1:]:
        factor_of = factor_of * one(*cut)
    return factor_of


def setup_inputs(seed: int = 0, part: int = 0) -> dict:
    key_of = jax.random.split(jax.random.key(seed), 5)
    part_splits = jax.random.split(jax.random.fold_in(key_of[4], part), 5)
    spectrum = jnp.clip(jnp.exp(math.log(5.0) - 4.6051702 * jax.random.uniform(part_splits[0], (BINS, CELLS), jnp.float32) ** levels(part_splits[0], (BINS, CELLS), ((0, 128),), -0.2, 0.2)), 0.05, 5.0)
    sea_mask = draw_sea_mask(jax.random.fold_in(key_of[4], 71), part)
    wind_speed = jnp.clip(jnp.exp(jax.random.uniform(part_splits[2], (CELLS,), jnp.float32, math.log(0.3), math.log(3.0))), 0.3, 3.0)
    wind_angle = jnp.clip(jax.random.uniform(part_splits[3], (CELLS,), jnp.float32, -3.140625, 3.140625), -3.140625, 3.140625)
    return {"spectrum": spectrum, "sea_mask": sea_mask, "wind_speed": wind_speed, "wind_angle": wind_angle}


def upwind_step(energy, courant_x, courant_y, sea_grid):
    west_cell = jnp.roll(energy, 1, axis=2)
    east_cell = jnp.roll(energy, -1, axis=2)
    edge_row = jnp.zeros_like(energy[:, :1])
    south_cell = jnp.concatenate([edge_row, energy[:, :-1]], axis=1)
    north_cell = jnp.concatenate([energy[:, 1:], edge_row], axis=1)
    updated = energy - jnp.maximum(courant_x, 0.0) * (energy - west_cell) - jnp.minimum(courant_x, 0.0) * (east_cell - energy) - jnp.maximum(courant_y, 0.0) * (energy - south_cell) - jnp.minimum(courant_y, 0.0) * (north_cell - energy)
    return updated * sea_grid

def courant_numbers(freq_index, dir_index, lat_count, dir_count):
    speed = 0.2 * jnp.exp(-math.log(1.1) * freq_index)
    heading = 2.0 * math.pi * (dir_index + 0.5) / dir_count
    rows = jnp.arange(lat_count, dtype=jnp.float32)
    latitude = (-75.0 + 150.0 * (rows + 0.5) / lat_count) * (math.pi / 180.0)
    courant_x = (speed * jnp.cos(heading))[:, None, None] / jnp.cos(latitude)[None, :, None]
    courant_y = (speed * jnp.sin(heading))[:, None, None]
    return (courant_x, courant_y)

def shift_freq(values, amount):
    if amount > 0:
        filler = jnp.zeros_like(values[:amount])
        return jnp.concatenate([filler, values[:-amount]], axis=0)
    filler = jnp.zeros_like(values[:-amount])
    return jnp.concatenate([values[-amount:], filler], axis=0)

def source_terms(energy, speed, angle):
    freq_count = energy.shape[0]
    dir_count = energy.shape[1]
    freq_ids = jnp.arange(freq_count, dtype=jnp.float32)
    frequency = jnp.exp(math.log(1.1) * (freq_ids - freq_count // 2))[:, None, None]
    heading = (2.0 * math.pi * (jnp.arange(dir_count, dtype=jnp.float32) + 0.5) / dir_count)[None, :, None]
    energy_mean = lax.optimization_barrier(jnp.mean(energy, axis=(0, 1)))
    moment_one = lax.optimization_barrier(jnp.mean(frequency * energy, axis=(0, 1)))
    mean_freq = moment_one / (energy_mean + 1e-06)
    steepness = energy_mean * mean_freq * mean_freq
    breaking = steepness * steepness / (1.0 + steepness * steepness)
    wind_gain = 0.05 * frequency * jnp.maximum(0.0, speed[None, None, :] * frequency * jnp.cos(heading - angle[None, None, :]) - 1.0)
    damping = 0.03 * frequency * breaking[None, None, :]
    valid = ((freq_ids >= 3) & (freq_ids <= freq_count - 3)).astype(jnp.float32)[:, None, None]
    interaction = jnp.zeros_like(energy)
    for mirror in (1, -1):
        plus_bins = shift_freq(jnp.roll(energy, -mirror, axis=1), -2)
        minus_bins = shift_freq(jnp.roll(energy, 3 * mirror, axis=1), 3)
        transfer_rate = 0.001 * valid * (energy * energy * (plus_bins + minus_bins) - 2.0 * energy * plus_bins * minus_bins)
        interaction = interaction - 2.0 * transfer_rate
        interaction = interaction + jnp.roll(shift_freq(transfer_rate, 2), mirror, axis=1)
        interaction = interaction + jnp.roll(shift_freq(transfer_rate, -3), -3 * mirror, axis=1)
    updated = energy + (wind_gain - damping) * energy + interaction
    raw_height = 4.0 * jnp.sqrt(lax.optimization_barrier(jnp.mean(updated, axis=(0, 1))) + 1e-06)
    return (updated, raw_height)

def reference(spectrum, sea_mask, wind_speed, wind_angle):
    sea_float = sea_mask.astype(jnp.float32)
    sea_grid = sea_float.reshape(1, NLAT, NLON)
    bands = (spectrum * sea_float[None, :]).reshape(NF, ND, NLAT, NLON)

    def advect_band(inputs):
        band, freq_value = inputs
        dir_index = jnp.arange(ND, dtype=jnp.float32)
        freq_index = jnp.zeros((ND,), jnp.float32) + freq_value
        courant_x, courant_y = courant_numbers(freq_index, dir_index, NLAT, ND)
        for substep in range(ADV_STEPS):
            band = upwind_step(band, courant_x, courant_y, sea_grid)
        return band
    advected = lax.map(advect_band, (bands, jnp.arange(NF, dtype=jnp.float32)))
    blocks = jnp.moveaxis(advected.reshape(NF, ND, N_SPEC, PTS_DEV), 2, 0)
    speed_blocks = wind_speed.reshape(N_SPEC, PTS_DEV)
    angle_blocks = wind_angle.reshape(N_SPEC, PTS_DEV)

    def block_sources(inputs):
        return source_terms(inputs[0], inputs[1], inputs[2])
    updated, raw_height = lax.map(block_sources, (blocks, speed_blocks, angle_blocks))
    new_spectrum = jnp.moveaxis(updated, 0, 2).reshape(NF * ND, CELLS)
    wave_height = sea_float * raw_height.reshape(CELLS)
    mean_height = (jnp.sum(wave_height) / SEA).reshape(1)
    return (new_spectrum, wave_height, mean_height)
```

```python
import functools
import math

import jax
import jax.numpy as jnp
import numpy as np
from jax import lax
from jax.experimental import pallas as pl
from jax.experimental.pallas import tpu as pltpu
from jax.sharding import PartitionSpec as P

NF = 48
ND = 32
NLON = 384
SUBSTEPS = 2
SEA_DEV = 64
MESH = pl.DeviceIdType.MESH
LOG_RATIO = math.log(1.1)


def peer_order(side, cores):
    hops = lambda d: min(d, side - d)
    sign = lambda d: 0 if d == 0 else (1 if d <= side // 2 else -1)
    offsets = [(x, y, c) for x in range(side) for y in range(side) for c in range(cores)][1:]
    offsets.sort(key=lambda o: (-(hops(o[0]) + hops(o[1])), o[0] * 3 + o[1] * 5, o[2]))
    classes = {}
    for o in offsets:
        classes.setdefault((sign(o[0]), sign(o[1])), []).append(o)
    placed = []
    for members in classes.values():
        placed += [((i + 0.5) / len(members), o) for i, o in enumerate(members)]
    placed.sort(key=lambda item: item[0])
    return [o for _, o in placed]


def step_kernel(
    n, side, cores, order,
    x, mask2d, speed2d, angle2d,
    out, height_out, mean_out,
    field_a, field_b, stage, shifts, go_left, go_right, hist,
    send, recv, back, home, flat, rolled, updated, heights,
    send_sem, recv_sem,
):
    bins_dev, cells = x.shape
    half = bins_dev // 2
    chunks = cells // 128
    per_row = NLON // 128
    lat_count = cells // NLON
    sea_chunks = n * SEA_DEV // 128
    me = lax.axis_index("spec")
    my_x, my_y, my_c = me // (side * cores), lax.rem(me // cores, side), lax.rem(me, cores)

    def peer(o):
        return (
            lax.rem(my_x + o[0], side) * side + lax.rem(my_y + o[1], side)
        ) * cores + lax.rem(my_c + o[2], cores)

    barrier = pltpu.get_barrier_semaphore()
    for o in order:
        pl.semaphore_signal(barrier, inc=1, device_id={"spec": peer(o)}, device_id_type=MESH)

    lane = lax.broadcasted_iota(jnp.int32, (8, 128), 1)
    row = lax.broadcasted_iota(jnp.int32, (8, 128), 0)
    low = lane < SEA_DEV

    bits = (chunks * 128).bit_length() - 1
    land = (1 - mask2d[...]).astype(jnp.bfloat16)
    before = (
        lax.broadcasted_iota(jnp.int32, (128, 128), 0) < lax.broadcasted_iota(jnp.int32, (128, 128), 1)
    ).astype(jnp.bfloat16)
    above = (
        lax.broadcasted_iota(jnp.int32, (chunks, chunks), 1)
        < lax.broadcasted_iota(jnp.int32, (chunks, chunks), 0)
    ).astype(jnp.bfloat16)
    within = jnp.dot(land, before, preferred_element_type=jnp.float32)
    rows_above = jnp.dot(above, land, preferred_element_type=jnp.float32)
    count = within + jnp.dot(
        rows_above.astype(jnp.bfloat16),
        jnp.ones((128, 128), jnp.bfloat16),
        preferred_element_type=jnp.float32,
    )
    left = jnp.where(mask2d[...] != 0, count.astype(jnp.int32), 0)
    shifts[chunks:, :] = jnp.zeros((shifts.shape[0] - chunks, 128), jnp.int32)
    wide_lane = lax.broadcasted_iota(jnp.int32, (chunks, 128), 1)
    steps = 13
    for i in range(steps):
        d = 1 << i
        shifts[0:chunks, :] = left
        if d < 128:
            near = pltpu.roll(left, 128 - d, 1)
            far = pltpu.roll(shifts[1 : chunks + 1, :], 128 - d, 1)
            incoming = jnp.where(wide_lane < 128 - d, near, far)
        else:
            incoming = shifts[d // 128 : chunks + d // 128, :]
        goes = jnp.bitwise_and(left, d)
        comes = jnp.bitwise_and(incoming, d)
        go_right[i] = goes
        go_left[i] = comes
        left = jnp.where(comes != 0, incoming, jnp.where(goes != 0, 0, left))

    zero = jnp.zeros((8, 128), jnp.float32)
    pad = per_row
    for t in range(2):
        for v in range(pad):
            for f in (field_a, field_b):
                f[t, v] = zero
                f[t, pad + chunks + v] = zero
    for v in range(chunks):
        sea = mask2d[v : v + 1, :].astype(jnp.float32)
        stage[v, 0:bins_dev, :] = x[:, v * 128 : (v + 1) * 128] * sea
        for t in range(2):
            field_a[t, pad + v, 0:half, :] = stage[v, pl.ds(t, half, stride=2), :]

    freq, cw, ce, cs, cn = [], [], [], [], []
    for t in range(2):
        bin_ids = me * bins_dev + jnp.minimum(2 * row + t, bins_dev - 1)
        k = (bin_ids // ND).astype(jnp.float32)
        j = lax.rem(bin_ids, ND).astype(jnp.float32)
        pace = 0.2 * jnp.exp(-LOG_RATIO * k)
        heading = (2.0 * math.pi / ND) * (j + 0.5)
        ax, ay = pace * jnp.cos(heading), pace * jnp.sin(heading)
        cw.append(jnp.maximum(ax, 0.0))
        ce.append(-jnp.minimum(ax, 0.0))
        cs.append(jnp.maximum(ay, 0.0))
        cn.append(-jnp.minimum(ay, 0.0))
    for s in range(SUBSTEPS):
        src, dst = (field_a, field_b) if s % 2 == 0 else (field_b, field_a)
        for r in range(lat_count):
            latitude = math.radians(-75.0 + 150.0 * (r + 0.5) / lat_count)
            widen = float(1.0 / math.cos(latitude))
            for t in range(2):
                west_c, east_c = cw[t] * widen, ce[t] * widen
                own_c = 1.0 - west_c - east_c - cs[t] - cn[t]
                first = pad + r * per_row
                e = [src[t, first + q] for q in range(per_row)]
                right = [pltpu.roll(a, 1, 1) for a in e]
                leftw = [pltpu.roll(a, 127, 1) for a in e]
                for q in range(per_row):
                    west = jnp.where(lane == 0, right[q - 1], right[q])
                    east = jnp.where(lane == 127, leftw[(q + 1) % per_row], leftw[q])
                    new = (
                        own_c * e[q] + west_c * west + east_c * east
                        + cs[t] * src[t, first + q - per_row]
                        + cn[t] * src[t, first + q + per_row]
                    )
                    v = first + q - pad
                    if s < SUBSTEPS - 1:
                        new = new * mask2d[v : v + 1, :].astype(jnp.float32)
                    dst[t, first + q] = new
                    if s == SUBSTEPS - 1:
                        dst[t, first + q, half : half + 1, :] = (speed2d, angle2d)[t][v : v + 1, :]
    final = field_a if SUBSTEPS % 2 == 0 else field_b

    lane_steps = 7
    ready = {}
    turned = [[zero] * lane_steps for _ in range(2)]
    held = [[{} for _ in range(steps)] for _ in range(2)]
    for v in range(chunks - 1, -1, -1):
        moves = [go_left[i, v : v + 1, :] != 0 for i in range(lane_steps)]
        cur = []
        for t in range(2):
            a = final[t, pad + v]
            for i in range(lane_steps):
                d = 1 << i
                rot = pltpu.roll(a, 128 - d, 1)
                b = jnp.where(lane < 128 - d, rot, turned[t][i])
                turned[t][i] = rot
                a = jnp.where(jnp.broadcast_to(moves[i], (8, 128)), b, a)
            cur.append(a)
        for i in range(lane_steps, steps):
            dv = 1 << (i - 7)
            slot = i - lane_steps
            for t in range(2):
                a = cur[t]
                if dv <= 4:
                    held[t][i][v] = a
                else:
                    hist[slot, t, v] = a
                if v + dv < chunks and (v < sea_chunks or i < steps - 1):
                    older = held[t][i].pop(v + dv) if dv <= 4 else hist[slot, t, v + dv]
                    m = jnp.broadcast_to(go_left[i, v : v + 1, :] != 0, (8, 128))
                    cur[t] = jnp.where(m, older, a)
        if v < sea_chunks:
            even, odd = cur
            send[2 * v] = jnp.where(low, even, pltpu.roll(odd, 64, 1))
            send[2 * v + 1] = jnp.where(low, pltpu.roll(even, 64, 1), odd)

    pl.semaphore_wait(barrier, n - 1)

    def exchange(src, dst, rows, k):
        for o in order:
            to = peer(o)
            pltpu.make_async_remote_copy(
                src_ref=src.at[to, pl.ds(0, rows)],
                dst_ref=dst.at[me, pl.ds(0, rows)],
                send_sem=send_sem.at[k],
                recv_sem=recv_sem.at[k],
                device_id={"spec": to},
                device_id_type=MESH,
            ).start()
        dst[me] = src[me]

    def finish(ref, rows, sem):
        part = ref.at[pl.ds(0, n - 1), pl.ds(0, rows)]
        pltpu.make_async_copy(part, part, sem).wait()

    exchange(send, recv, half, 0)

    wind = send[me][half : half + 1, :]
    other = pltpu.roll(wind, 64, 1)
    lower = low[0:1, :]
    speed = jnp.where(lower, wind, other)
    angle = jnp.where(lower, other, wind)
    pair = lax.broadcasted_iota(jnp.int32, (ND // 2, 128), 0)
    side_id = (lax.broadcasted_iota(jnp.int32, (ND // 2, 128), 1) >= SEA_DEV).astype(jnp.int32)
    low16 = side_id == 0
    dirs = (2.0 * math.pi / ND) * ((2 * pair + side_id).astype(jnp.float32) + 0.5)
    toward = speed * (jnp.cos(dirs) * jnp.cos(angle) + jnp.sin(dirs) * jnp.sin(angle))

    finish(recv, half, recv_sem.at[0])

    for p in range(n):
        flat[half * p : half * p + half, :] = recv[p, 0:half, :]

    rows_k = ND // 2

    def turns(a, amounts):
        s = pltpu.roll(a, 64, 1)
        need = {1: (1, 0), -1: (0, -1), 3: (2, 1), -3: (-1, -2)}
        by = {0: s}
        for m in amounts:
            for w in need[m]:
                if w not in by:
                    by[w] = pltpu.roll(s, w % rows_k, 0)
        return [jnp.where(low16, by[need[m][0]], by[need[m][1]]) for m in amounts]

    omega = [float(math.exp(LOG_RATIO * (k - NF // 2))) for k in range(NF)]
    m0 = m1 = None
    for k in range(NF):
        a = flat[rows_k * k : rows_k * (k + 1), :]
        m0 = a if k == 0 else m0 + a
        m1 = omega[k] * a if k == 0 else m1 + omega[k] * a
        for w, b in enumerate(turns(a, (1, -1, 3, -3))):
            rolled[w, rows_k * k : rows_k * (k + 1), :] = b

    def over_bins(a):
        a = jnp.sum(a, axis=0, keepdims=True)
        return (a + pltpu.roll(a, 64, 1)) * (1.0 / (NF * ND))

    m0, m1 = over_bins(m0), over_bins(m1)
    mean_freq = m1 / (m0 + 1e-6)
    steep = m0 * mean_freq * mean_freq
    breaking = steep * steep / (1.0 + steep * steep)

    own, from_low, total = {}, {}, None
    for k in range(NF + 3):
        from_high = None
        if 3 <= k <= NF - 3:
            a = flat[rows_k * k : rows_k * (k + 1), :]
            get = lambda w, kk: rolled[w, rows_k * kk : rows_k * (kk + 1), :]
            rates = []
            for plus, minus in ((get(1, k + 2), get(2, k - 3)), (get(0, k + 2), get(3, k - 3))):
                rates.append(0.001 * a * (a * (plus + minus) - 2.0 * plus * minus))
            up, down = turns(rates[0], (1, -3)), turns(rates[1], (-1, 3))
            own[k] = -2.0 * (rates[0] + rates[1])
            from_low[k + 2] = up[0] + down[0]
            from_high = up[1] + down[1]
        f = k - 3
        if f < 0:
            continue
        a = flat[rows_k * f : rows_k * (f + 1), :]
        gain = (0.05 * omega[f]) * jnp.maximum(0.0, omega[f] * toward - 1.0)
        new = a + (gain - (0.03 * omega[f]) * breaking) * a
        for part in (own.pop(f, None), from_low.pop(f, None), from_high):
            if part is not None:
                new = new + part
        updated[rows_k * f : rows_k * (f + 1), :] = new
        total = new if total is None else total + new
    height = 4.0 * jnp.sqrt(over_bins(total) + 1e-6)

    for p in range(n):
        back[p, half : half + 1, :] = height
        back[p, 0:half, :] = updated[half * p : half * p + half, :]

    exchange(back, home, half + 1, 1)
    finish(send, half, send_sem.at[0])
    finish(home, half + 1, recv_sem.at[1])

    turned = [[zero] * lane_steps for _ in range(2)]
    held = [[{} for _ in range(steps)] for _ in range(2)]
    height_sum = zero
    for v in range(chunks):
        if v < sea_chunks:
            a, b = home[2 * v], home[2 * v + 1]
            cur = [jnp.where(low, a, pltpu.roll(b, 64, 1)), jnp.where(low, pltpu.roll(a, 64, 1), b)]
            height_sum = height_sum + cur[0]
        else:
            cur = [zero, zero]
        for i in range(steps - 1, lane_steps - 1, -1):
            dv = 1 << (i - 7)
            slot = i - lane_steps
            for t in range(2):
                a = cur[t]
                if dv <= 4:
                    held[t][i][v] = a
                else:
                    hist[slot, t, v] = a
                if v >= dv:
                    older = held[t][i].pop(v - dv) if dv <= 4 else hist[slot, t, v - dv]
                    m = jnp.broadcast_to(go_right[i, v : v + 1, :] != 0, (8, 128))
                    cur[t] = jnp.where(m, older, a)
        sea = jnp.broadcast_to(mask2d[v : v + 1, :] != 0, (8, 128))
        for t in range(2):
            a = cur[t]
            for i in range(lane_steps - 1, -1, -1):
                d = 1 << i
                rot = pltpu.roll(a, d, 1)
                b = jnp.where(lane < d, turned[t][i], rot)
                turned[t][i] = rot
                m = jnp.broadcast_to(go_right[i, v : v + 1, :] != 0, (8, 128))
                a = jnp.where(m, b, a)
            a = jnp.where(sea, a, 0.0)
            stage[v, pl.ds(t, half, stride=2), :] = a[0:half]
            if t == 0:
                heights[v : v + 1, :] = a[half : half + 1]
        out[:, v * 128 : (v + 1) * 128] = stage[v, 0:bins_dev, :]

    points = cells // n
    group = 128 * 3 // points
    start = me // group * 3
    three = [heights[pl.ds(start + q, 1), :] for q in range(3)]
    u = lax.rem(me, group)
    picked = None
    for g in range(group):
        first, offset = g * points // 128, g * points % 128
        piece = three[first]
        if offset:
            nxt = three[min(first + 1, 2)]
            piece = jnp.where(
                lane[0:1] < 128 - offset, pltpu.roll(piece, 128 - offset, 1), pltpu.roll(nxt, 128 - offset, 1)
            )
        picked = piece if picked is None else jnp.where(u == g, piece, picked)
    height_out[...] = picked[:, 0:points]
    mean_out[...] = jnp.sum(height_sum[half : half + 1, :], axis=1, keepdims=True) * (1.0 / (SEA_DEV * n))
    finish(back, half + 1, send_sem.at[1])


def solution(mesh):
    n = mesh.shape["spec"]
    cores = 2
    side = math.isqrt(n // cores)
    order = peer_order(side, cores)

    def local(spectrum, sea_mask, wind_speed, wind_angle):
        bins_dev, cells = spectrum.shape
        chunks = cells // 128
        per_row = NLON // 128
        padded = chunks + 2 * per_row
        vmem = pl.BlockSpec(memory_space=pltpu.VMEM)
        new_spectrum, height, mean = pl.pallas_call(
            functools.partial(step_kernel, n, side, cores, order),
            name="wave_step",
            out_shape=(
                jax.ShapeDtypeStruct((bins_dev, cells), jnp.float32),
                jax.ShapeDtypeStruct((1, cells // n), jnp.float32),
                jax.ShapeDtypeStruct((1, 1), jnp.float32),
            ),
            in_specs=[vmem] * 4,
            out_specs=(vmem,) * 3,
            scratch_shapes=[
                pltpu.VMEM((2, padded, 8, 128), jnp.float32),
                pltpu.VMEM((2, padded, 8, 128), jnp.float32),
                pltpu.VMEM((chunks, 16, 128), jnp.float32),
                pltpu.VMEM((chunks + 32, 128), jnp.int32),
                pltpu.VMEM((13, chunks, 128), jnp.int32),
                pltpu.VMEM((13, chunks, 128), jnp.int32),
                pltpu.VMEM((6, 2, chunks, 8, 128), jnp.float32),
                pltpu.VMEM((n, 8, 128), jnp.float32),
                pltpu.VMEM((n, 8, 128), jnp.float32),
                pltpu.VMEM((n, 8, 128), jnp.float32),
                pltpu.VMEM((n, 8, 128), jnp.float32),
                pltpu.VMEM((NF * ND // 2, 128), jnp.float32),
                pltpu.VMEM((4, NF * ND // 2, 128), jnp.float32),
                pltpu.VMEM((NF * ND // 2, 128), jnp.float32),
                pltpu.VMEM((chunks, 128), jnp.float32),
                pltpu.SemaphoreType.DMA((2,)),
                pltpu.SemaphoreType.DMA((2,)),
            ],
            compiler_params=pltpu.CompilerParams(collective_id=0, has_side_effects=True),
        )(
            spectrum,
            sea_mask.reshape(chunks, 128),
            wind_speed.reshape(chunks, 128),
            wind_angle.reshape(chunks, 128),
        )
        return new_spectrum, height.reshape(-1), mean.reshape(1)

    return jax.shard_map(
        local,
        mesh=mesh,
        in_specs=(P(("grp", "spec"), None), P(), P("grp"), P("grp")),
        out_specs=(P(("grp", "spec"), None), P(("grp", "spec")), P("grp")),
        check_vma=False,
    )
```

```python
import functools
import math

import jax
import jax.numpy as jnp
import numpy as np
from jax import lax
from jax.experimental import pallas as pl
from jax.experimental.pallas import tpu as pltpu
from jax.sharding import PartitionSpec as P

NF = 48
ND = 32
NLON = 384
SUBSTEPS = 2
SEA_DEV = 64
MESH = pl.DeviceIdType.MESH
LOG_RATIO = math.log(1.1)
PAIRS = ND // 2
LANE_STEPS = 7
STEPS = 13
REACH = 32


def tables(lat_count):
    heading = 2.0 * np.pi * (np.arange(ND) + 0.5) / ND
    wrapped = np.concatenate([heading, heading[:24]])
    flat = lambda a: np.repeat(np.asarray(a)[:, None], 128, 1)
    paired = np.repeat(heading.reshape(PAIRS, 2), SEA_DEV, axis=1)
    latitude = np.radians(-75.0 + 150.0 * (np.arange(lat_count) + 0.5) / lat_count)
    k = np.arange(NF)
    rows, at = [], {}
    for name, block in (
        ("cos", flat(np.cos(wrapped))),
        ("sin", flat(np.sin(wrapped))),
        ("pair_cos", np.cos(paired)),
        ("pair_sin", np.sin(paired)),
        ("widen", flat(1.0 / np.cos(latitude))),
        ("omega", flat(np.exp(LOG_RATIO * (k - NF // 2)))),
        ("rate", flat(np.where((k >= 3) & (k <= NF - 3), 0.001, 0.0))),
    ):
        at[name] = sum(len(r) for r in rows)
        rows.append(block)
    return np.concatenate(rows).astype(np.float32), at


def step_kernel(
    n, side, cores, at,
    x_hbm, mask2d, speed2d, angle2d, tab,
    out, height_out, mean_out,
    x, field_a, field_b, stage, shifts, go_left, go_right, hist,
    send, recv, back, home, flat, energy, rolled, own, low_part, high_part, heights,
    send_sem, recv_sem, load_sem,
):
    bins_dev, cells = x.shape
    half = bins_dev // 2
    chunks = cells // 128
    per_row = NLON // 128
    lat_count = cells // NLON
    me = lax.axis_index("spec")
    my_x, my_y, my_c = me // (side * cores), lax.rem(me // cores, side), lax.rem(me, cores)

    load = pltpu.make_async_copy(x_hbm, x, load_sem)
    load.start()

    def peers(act):
        def hop(u):
            return side // 2 + jnp.where(lax.rem(u, 2) == 0, u // 2, -((u + 1) // 2))

        def chip(s, u):
            px = lax.rem(my_x + hop(u), side)
            py = lax.rem(my_y + hop(s - u), side)
            first = (px * side + py) * cores
            act(first + my_c)
            for c in range(1, cores):
                act(first + lax.rem(my_c + c, cores))

        def diagonal(s, carry):
            def one(u, inner):
                chip(s, u)
                return inner

            return lax.fori_loop(jnp.maximum(0, s - side + 1), jnp.minimum(side - 1, s) + 1, one, carry)

        lax.fori_loop(0, 2 * side - 2, diagonal, 0)
        for c in range(1, cores):
            act(me - my_c + lax.rem(my_c + c, cores))

    barrier = pltpu.get_barrier_semaphore()
    peers(
        lambda to: pl.semaphore_signal(barrier, inc=1, device_id={"spec": to}, device_id_type=MESH)
    )

    lane = lax.broadcasted_iota(jnp.int32, (8, 128), 1)
    row = lax.broadcasted_iota(jnp.int32, (8, 128), 0)
    low = lane < SEA_DEV

    is_sea = mask2d[...] != 0
    land = jnp.where(is_sea, 0.0, 1.0).astype(jnp.bfloat16)
    before = (
        lax.broadcasted_iota(jnp.int32, (128, 128), 0) < lax.broadcasted_iota(jnp.int32, (128, 128), 1)
    ).astype(jnp.bfloat16)
    above = (
        lax.broadcasted_iota(jnp.int32, (chunks, chunks), 1)
        < lax.broadcasted_iota(jnp.int32, (chunks, chunks), 0)
    ).astype(jnp.bfloat16)
    rows_above = jnp.dot(above, land, preferred_element_type=jnp.float32)
    count = jnp.dot(land, before, preferred_element_type=jnp.float32) + jnp.dot(
        rows_above.astype(jnp.bfloat16),
        jnp.ones((128, 128), jnp.bfloat16),
        preferred_element_type=jnp.float32,
    )
    shifts[0:chunks, :] = jnp.where(is_sea, count.astype(jnp.int32), 0)
    shifts[chunks:, :] = jnp.zeros((shifts.shape[0] - chunks, 128), jnp.int32)
    go_left[...] = jnp.zeros_like(go_left)
    go_right[...] = jnp.zeros_like(go_right)
    wide_lane = lax.broadcasted_iota(jnp.int32, (chunks, 128), 1)

    def settle(left, incoming, d):
        goes = jnp.bitwise_and(left, d)
        comes = jnp.bitwise_and(incoming, d)
        go_right[...] += goes
        go_left[...] += comes
        shifts[0:chunks, :] = jnp.where(comes != 0, incoming, jnp.where(goes != 0, 0, left))

    def lane_step(i, carry):
        d = jnp.left_shift(1, i)
        left = shifts[0:chunks, :]
        near = pltpu.roll(left, 128 - d, 1)
        far = pltpu.roll(shifts[1 : chunks + 1, :], 128 - d, 1)
        settle(left, jnp.where(wide_lane < 128 - d, near, far), d)
        return carry

    lax.fori_loop(0, LANE_STEPS, lane_step, 0)
    for i in range(LANE_STEPS, STEPS):
        dv = 1 << (i - LANE_STEPS)
        settle(shifts[0:chunks, :], shifts[dv : chunks + dv, :], 1 << i)

    zero = jnp.zeros((8, 128), jnp.float32)
    pad = per_row
    for t in range(2):
        for v in range(pad):
            for f in (field_a, field_b):
                f[t, v] = zero
                f[t, pad + chunks + v] = zero
    base = (me * bins_dev) % ND
    cw, ce, cs, cn = [], [], [], []
    for t in range(2):
        k = ((me * bins_dev + jnp.minimum(2 * row + t, bins_dev - 1)) // ND).astype(jnp.float32)
        pace = 0.2 * jnp.exp(-LOG_RATIO * k)
        ax = pace * tab[pl.ds(at["cos"] + base + t, 8, stride=2), :]
        ay = pace * tab[pl.ds(at["sin"] + base + t, 8, stride=2), :]
        cw.append(jnp.maximum(ax, 0.0))
        ce.append(-jnp.minimum(ax, 0.0))
        cs.append(jnp.maximum(ay, 0.0))
        cn.append(-jnp.minimum(ay, 0.0))
    load.wait()

    def sea_row(v):
        return mask2d[pl.ds(v, 1), :] != 0

    def split_bins(g, carry):
        for u in range(8):
            v = g * 8 + u
            cols = pl.ds(pl.multiple_of(v * 128, 128), 128)
            stage[u, 0:bins_dev, :] = jnp.where(sea_row(v), x[:, cols], 0.0)
            for t in range(2):
                field_a[t, pad + v, 0:half, :] = stage[u, pl.ds(t, half, stride=2), :]
        return carry

    lax.fori_loop(0, chunks // 8, split_bins, 0)

    for s in range(SUBSTEPS):
        src, dst = (field_a, field_b) if s % 2 == 0 else (field_b, field_a)

        def advance(g, carry, src=src, dst=dst, s=s):
            for ru in range(2):
                r = g * 2 + ru
                widen = tab[pl.ds(at["widen"] + r, 1), :]
                first = pad + r * per_row
                for t in range(2):
                    west_c, east_c = cw[t] * widen, ce[t] * widen
                    own_c = 1.0 - west_c - east_c - cs[t] - cn[t]
                    e = [src[t, first + q] for q in range(per_row)]
                    right = [pltpu.roll(a, 1, 1) for a in e]
                    left = [pltpu.roll(a, 127, 1) for a in e]
                    for q in range(per_row):
                        west = jnp.where(lane == 0, right[q - 1], right[q])
                        east = jnp.where(lane == 127, left[(q + 1) % per_row], left[q])
                        new = (
                            own_c * e[q] + west_c * west + east_c * east
                            + cs[t] * src[t, first + q - per_row]
                            + cn[t] * src[t, first + q + per_row]
                        )
                        v = first + q - pad
                        if s < SUBSTEPS - 1:
                            dst[t, first + q] = jnp.where(sea_row(v), new, 0.0)
                        else:
                            wind = (speed2d, angle2d)[t][pl.ds(v, 1), :]
                            dst[t, first + q] = jnp.where(row == half, wind, new)
            return carry

        lax.fori_loop(0, lat_count // 2, advance, 0)
    final = field_a if SUBSTEPS % 2 == 0 else field_b

    unroll = 8

    def gather(g, carry):
        turned = list(carry)
        for u in range(unroll):
            v = chunks - 1 - (g * unroll + u)
            word = jnp.broadcast_to(go_left[pl.ds(v, 1), :], (8, 128))
            moves = [jnp.bitwise_and(word, 1 << i) != 0 for i in range(STEPS)]
            cur = []
            for t in range(2):
                a = final[t, pad + v]
                for i in range(LANE_STEPS):
                    d = 1 << i
                    rot = pltpu.roll(a, 128 - d, 1)
                    b = jnp.where(lane < 128 - d, rot, turned[t * LANE_STEPS + i])
                    turned[t * LANE_STEPS + i] = rot
                    a = jnp.where(moves[i], b, a)
                for i in range(LANE_STEPS, STEPS):
                    dv = 1 << (i - LANE_STEPS)
                    hist[i - LANE_STEPS, t, v] = a
                    a = jnp.where(moves[i], hist[i - LANE_STEPS, t, v + dv], a)
                cur.append(a)
            even, odd = cur
            send[2 * v] = jnp.where(low, even, pltpu.roll(odd, 64, 1))
            send[2 * v + 1] = jnp.where(low, pltpu.roll(even, 64, 1), odd)
        return tuple(turned)

    lax.fori_loop(0, chunks // unroll, gather, (zero,) * (2 * LANE_STEPS))

    pl.semaphore_wait(barrier, n - 1)

    def exchange(src, dst, rows, k):
        def push(to):
            pltpu.make_async_remote_copy(
                src_ref=src.at[to, pl.ds(0, rows)],
                dst_ref=dst.at[me, pl.ds(0, rows)],
                send_sem=send_sem.at[k],
                recv_sem=recv_sem.at[k],
                device_id={"spec": to},
                device_id_type=MESH,
            ).start()

        peers(push)
        dst[me] = src[me]

    def finish(ref, rows, sem):
        part = ref.at[pl.ds(0, n - 1), pl.ds(0, rows)]
        pltpu.make_async_copy(part, part, sem).wait()

    exchange(send, recv, half, 0)

    wind = send[me][half : half + 1, :]
    other = pltpu.roll(wind, SEA_DEV, 1)
    speed = jnp.where(low[0:1], wind, other)
    angle = jnp.where(low[0:1], other, wind)
    toward = speed * (
        tab[at["pair_cos"] : at["pair_cos"] + PAIRS, :] * jnp.cos(angle)
        + tab[at["pair_sin"] : at["pair_sin"] + PAIRS, :] * jnp.sin(angle)
    )
    low16 = lax.broadcasted_iota(jnp.int32, (PAIRS, 128), 1) < SEA_DEV
    zero16 = jnp.zeros((PAIRS, 128), jnp.float32)
    for w in range(4):
        for k in (0, 1, 2, NF + 3, NF + 4):
            rolled[w, k] = zero16
    for k in range(2):
        low_part[k] = zero16
    for k in range(3):
        high_part[NF + k] = zero16

    def turns(a, amounts):
        s = pltpu.roll(a, SEA_DEV, 1)
        need = {1: (1, 0), -1: (0, -1), 3: (2, 1), -3: (-1, -2)}
        by = {0: s}
        for m in amounts:
            for w in need[m]:
                if w not in by:
                    by[w] = pltpu.roll(s, w % PAIRS, 0)
        return [jnp.where(low16, by[need[m][0]], by[need[m][1]]) for m in amounts]

    group = 8
    per_group = half * group // PAIRS
    finish(recv, half, recv_sem.at[0])

    def arrange(g, carry):
        m0, m1 = carry
        for i in range(group):
            flat[g, half * i : half * i + half, :] = recv[g * group + i, 0:half, :]
        for q in range(per_group):
            k = g * per_group + q
            a = flat[g, PAIRS * q : PAIRS * (q + 1), :]
            energy[k] = a
            m0 = m0 + a
            m1 = m1 + tab[pl.ds(at["omega"] + k, 1), :] * a
            for w, b in enumerate(turns(a, (1, -1, 3, -3))):
                rolled[w, k + 3] = b
        return m0, m1

    m0, m1 = lax.fori_loop(0, n // group, arrange, (zero16, zero16))

    def over_bins(a):
        a = jnp.sum(a, axis=0, keepdims=True)
        return (a + pltpu.roll(a, SEA_DEV, 1)) * (1.0 / (NF * ND))

    m0, m1 = over_bins(m0), over_bins(m1)
    mean_freq = m1 / (m0 + 1e-6)
    steep = m0 * mean_freq * mean_freq
    breaking = steep * steep / (1.0 + steep * steep)

    def transfer(g, carry):
        for q in range(per_group):
            k = g * per_group + q
            a = energy[k]
            factor = tab[pl.ds(at["rate"] + k, 1), :] * a
            rates = []
            for plus, minus in ((rolled[1, k + 5], rolled[2, k]), (rolled[0, k + 5], rolled[3, k])):
                rates.append(factor * (a * (plus + minus) - 2.0 * plus * minus))
            up, down = turns(rates[0], (1, -3)), turns(rates[1], (-1, 3))
            own[k] = -2.0 * (rates[0] + rates[1])
            low_part[k + 2] = up[0] + down[0]
            high_part[k] = up[1] + down[1]
        return carry

    lax.fori_loop(0, n // group, transfer, 0)

    def renew(g, total):
        for q in range(per_group):
            k = g * per_group + q
            a = energy[k]
            omega = tab[pl.ds(at["omega"] + k, 1), :]
            gain = (0.05 * omega) * jnp.maximum(0.0, omega * toward - 1.0)
            new = a + (gain - (0.03 * omega) * breaking) * a
            new = new + own[k] + low_part[k] + high_part[k + 3]
            total = total + new
            flat[g, PAIRS * q : PAIRS * (q + 1), :] = new
        for i in range(group):
            back[g * group + i, 0:half, :] = flat[g, half * i : half * i + half, :]
        return total

    total = lax.fori_loop(0, n // group, renew, zero16)
    height = 4.0 * jnp.sqrt(over_bins(total) + 1e-6)

    def add_height(g, carry):
        for i in range(group):
            back[g * group + i, half : half + 1, :] = height
        return carry

    lax.fori_loop(0, n // group, add_height, 0)

    exchange(back, home, half + 1, 1)
    finish(send, half, send_sem.at[0])
    finish(home, half + 1, recv_sem.at[1])

    def scatter(g, carry):
        turned = list(carry)
        for u in range(unroll):
            v = g * unroll + u
            word = jnp.broadcast_to(go_right[pl.ds(v, 1), :], (8, 128))
            moves = [jnp.bitwise_and(word, 1 << i) != 0 for i in range(STEPS)]
            sea = jnp.broadcast_to(mask2d[pl.ds(v, 1), :], (8, 128)) != 0
            a, b = home[2 * v], home[2 * v + 1]
            cur = [
                jnp.where(low, a, pltpu.roll(b, SEA_DEV, 1)),
                jnp.where(low, pltpu.roll(a, SEA_DEV, 1), b),
            ]
            for t in range(2):
                a = cur[t]
                for i in range(STEPS - 1, LANE_STEPS - 1, -1):
                    dv = 1 << (i - LANE_STEPS)
                    hist[i - LANE_STEPS, t, REACH + v] = a
                    a = jnp.where(moves[i], hist[i - LANE_STEPS, t, REACH + v - dv], a)
                for i in range(LANE_STEPS - 1, -1, -1):
                    d = 1 << i
                    rot = pltpu.roll(a, d, 1)
                    b = jnp.where(lane < d, turned[t * LANE_STEPS + i], rot)
                    turned[t * LANE_STEPS + i] = rot
                    a = jnp.where(moves[i], b, a)
                a = jnp.where(sea, a, 0.0)
                stage[u, pl.ds(t, half, stride=2), :] = a[0:half]
                if t == 0:
                    heights[pl.ds(v, 1), :] = a[half : half + 1]
            out[:, pl.ds(pl.multiple_of(v * 128, 128), 128)] = stage[u, 0:bins_dev, :]
        return tuple(turned)

    lax.fori_loop(0, chunks // unroll, scatter, (zero,) * (2 * LANE_STEPS))

    points = cells // n
    together = NLON // points
    start = me // together * per_row
    three = [heights[pl.ds(start + q, 1), :] for q in range(per_row)]
    u = lax.rem(me, together)
    picked = None
    for g in range(together):
        first, offset = g * points // 128, g * points % 128
        piece = three[first]
        if offset:
            after = three[min(first + 1, per_row - 1)]
            piece = jnp.where(
                lane[0:1] < 128 - offset,
                pltpu.roll(piece, 128 - offset, 1),
                pltpu.roll(after, 128 - offset, 1),
            )
        picked = piece if picked is None else jnp.where(u == g, piece, picked)
    height_out[...] = picked[:, 0:points]
    all_heights = jnp.sum(heights[...], axis=0, keepdims=True)
    mean_out[...] = jnp.sum(all_heights, axis=1, keepdims=True) * (1.0 / (SEA_DEV * n))
    finish(back, half + 1, send_sem.at[1])


def solution(mesh):
    n = mesh.shape["spec"]
    cores = 2
    side = math.isqrt(n // cores)

    def local(spectrum, sea_mask, wind_speed, wind_angle):
        bins_dev, cells = spectrum.shape
        chunks = cells // 128
        padded = chunks + 2 * (NLON // 128)
        tab, at = tables(cells // NLON)
        vmem = pl.BlockSpec(memory_space=pltpu.VMEM)
        words = pltpu.VMEM((chunks, 128), jnp.int32)
        by_freq = lambda *dims: pltpu.VMEM((*dims, PAIRS, 128), jnp.float32)
        messages = lambda count: pltpu.VMEM((count, 8, 128), jnp.float32)
        new_spectrum, height, mean = pl.pallas_call(
            functools.partial(step_kernel, n, side, cores, at),
            name="wave_step",
            out_shape=(
                jax.ShapeDtypeStruct((bins_dev, cells), jnp.float32),
                jax.ShapeDtypeStruct((1, cells // n), jnp.float32),
                jax.ShapeDtypeStruct((1, 1), jnp.float32),
            ),
            in_specs=[pl.BlockSpec(memory_space=pl.ANY)] + [vmem] * 4,
            out_specs=(vmem,) * 3,
            scratch_shapes=[
                pltpu.VMEM((bins_dev, cells), jnp.float32),
                pltpu.VMEM((2, padded, 8, 128), jnp.float32),
                pltpu.VMEM((2, padded, 8, 128), jnp.float32),
                pltpu.VMEM((8, 16, 128), jnp.float32),
                pltpu.VMEM((chunks + REACH, 128), jnp.int32),
                words,
                words,
                pltpu.VMEM((STEPS - LANE_STEPS, 2, chunks + REACH, 8, 128), jnp.float32),
                messages(2 * chunks),
                messages(n),
                messages(n),
                messages(2 * chunks),
                pltpu.VMEM((n // 8, 8 * bins_dev // 2, 128), jnp.float32),
                by_freq(NF),
                by_freq(4, NF + 5),
                by_freq(NF),
                by_freq(NF + 2),
                by_freq(NF + 3),
                pltpu.VMEM((chunks, 128), jnp.float32),
                pltpu.SemaphoreType.DMA((2,)),
                pltpu.SemaphoreType.DMA((2,)),
                pltpu.SemaphoreType.DMA,
            ],
            compiler_params=pltpu.CompilerParams(collective_id=0, has_side_effects=True),
        )(
            spectrum,
            sea_mask.reshape(chunks, 128),
            wind_speed.reshape(chunks, 128),
            wind_angle.reshape(chunks, 128),
            tab,
        )
        return new_spectrum, height.reshape(-1), mean.reshape(1)

    return jax.shard_map(
        local,
        mesh=mesh,
        in_specs=(P(("grp", "spec"), None), P(), P("grp"), P("grp")),
        out_specs=(P(("grp", "spec"), None), P(("grp", "spec")), P("grp")),
        check_vma=False,
    )
```

```python
import functools
import math

import jax
import jax.numpy as jnp
import numpy as np
from jax import lax
from jax.experimental import pallas as pl
from jax.experimental.pallas import tpu as pltpu
from jax.sharding import PartitionSpec as P

NF = 48
ND = 32
NLON = 384
SUBSTEPS = 2
SEA_DEV = 64
MESH = pl.DeviceIdType.MESH
LOG_RATIO = math.log(1.1)
PAIRS = ND // 2
LANE_STEPS = 7
STEPS = 13
REACH = 32
FAR = 56


def tables(lat_count):
    heading = 2.0 * np.pi * (np.arange(ND) + 0.5) / ND
    wrapped = np.concatenate([heading, heading[:24]])
    flat = lambda a: np.repeat(np.asarray(a)[:, None], 128, 1)
    paired = np.repeat(heading.reshape(PAIRS, 2), SEA_DEV, axis=1)
    latitude = np.radians(-75.0 + 150.0 * (np.arange(lat_count) + 0.5) / lat_count)
    k = np.arange(NF)
    rows, at = [], {}
    for name, block in (
        ("cos", flat(np.cos(wrapped))),
        ("sin", flat(np.sin(wrapped))),
        ("pair_cos", np.cos(paired)),
        ("pair_sin", np.sin(paired)),
        ("widen", flat(1.0 / np.cos(latitude))),
        ("omega", flat(np.exp(LOG_RATIO * (k - NF // 2)))),
        ("rate", flat(np.where((k >= 3) & (k <= NF - 3), 0.001, 0.0))),
    ):
        at[name] = sum(len(r) for r in rows)
        rows.append(block)
    return np.concatenate(rows).astype(np.float32), at


def step_kernel(
    n, side, cores, at,
    x_hbm, mask2d, speed2d, angle2d, tab,
    out, height_out, mean_out,
    x, field_a, field_b, stage, shifts, go_left, go_right, moved_a, moved_b,
    send, recv, back, home, flat, energy, rolled, own, low_part, high_part, heights,
    send_sem, recv_sem, load_sem, column_sem,
):
    bins_dev, cells = x.shape
    half = bins_dev // 2
    chunks = cells // 128
    per_row = NLON // 128
    lat_count = cells // NLON
    me = lax.axis_index("spec")
    my_x, my_y, my_c = me // (side * cores), lax.rem(me // cores, side), lax.rem(me, cores)

    load = pltpu.make_async_copy(x_hbm, x, load_sem)
    load.start()

    def peers(act):
        def hop(u):
            return side // 2 + jnp.where(lax.rem(u, 2) == 0, u // 2, -((u + 1) // 2))

        def chip(s, u):
            px = lax.rem(my_x + hop(u), side)
            py = lax.rem(my_y + hop(s - u), side)
            first = (px * side + py) * cores
            act(first + my_c)
            for c in range(1, cores):
                act(first + lax.rem(my_c + c, cores))

        def diagonal(s, carry):
            def one(u, inner):
                chip(s, u)
                return inner

            return lax.fori_loop(jnp.maximum(0, s - side + 1), jnp.minimum(side - 1, s) + 1, one, carry)

        lax.fori_loop(0, 2 * side - 2, diagonal, 0)
        for c in range(1, cores):
            act(me - my_c + lax.rem(my_c + c, cores))

    barrier = pltpu.get_barrier_semaphore()

    def call_row(i, carry):
        to = (lax.rem(my_x + i // cores, side) * side + my_y) * cores + lax.rem(my_c + lax.rem(i, cores), cores)
        pl.semaphore_signal(barrier, inc=1, device_id={"spec": to}, device_id_type=MESH)
        return carry

    def call_column(semaphore):
        def one(i, carry):
            to = (my_x * side + lax.rem(my_y + i, side)) * cores + my_c
            pl.semaphore_signal(semaphore, inc=1, device_id={"spec": to}, device_id_type=MESH)
            return carry

        lax.fori_loop(1, side, one, 0)

    lax.fori_loop(1, side * cores, call_row, 0)
    call_column(barrier)

    lane = lax.broadcasted_iota(jnp.int32, (8, 128), 1)
    row = lax.broadcasted_iota(jnp.int32, (8, 128), 0)
    low = lane < SEA_DEV

    is_sea = mask2d[...] != 0
    land = jnp.where(is_sea, 0.0, 1.0).astype(jnp.bfloat16)
    before = (
        lax.broadcasted_iota(jnp.int32, (128, 128), 0) < lax.broadcasted_iota(jnp.int32, (128, 128), 1)
    ).astype(jnp.bfloat16)
    above = (
        lax.broadcasted_iota(jnp.int32, (chunks, chunks), 1)
        < lax.broadcasted_iota(jnp.int32, (chunks, chunks), 0)
    ).astype(jnp.bfloat16)
    rows_above = jnp.dot(above, land, preferred_element_type=jnp.float32)
    count = jnp.dot(land, before, preferred_element_type=jnp.float32) + jnp.dot(
        rows_above.astype(jnp.bfloat16),
        jnp.ones((128, 128), jnp.bfloat16),
        preferred_element_type=jnp.float32,
    )
    inner = slice(REACH, REACH + chunks)
    shifts[0:chunks, :] = jnp.where(is_sea, count.astype(jnp.int32), 0)
    shifts[chunks:, :] = jnp.zeros((shifts.shape[0] - chunks, 128), jnp.int32)
    go_left[...] = jnp.zeros_like(go_left)
    go_right[...] = jnp.zeros_like(go_right)
    wide_lane = lax.broadcasted_iota(jnp.int32, (chunks, 128), 1)

    def settle(left, incoming, d):
        goes = jnp.bitwise_and(left, d)
        comes = jnp.bitwise_and(incoming, d)
        go_right[inner, :] += goes
        go_left[inner, :] += comes
        shifts[0:chunks, :] = jnp.where(comes != 0, incoming, jnp.where(goes != 0, 0, left))

    def lane_step(i, carry):
        d = jnp.left_shift(1, i)
        left = shifts[0:chunks, :]
        near = pltpu.roll(left, 128 - d, 1)
        far = pltpu.roll(shifts[1 : chunks + 1, :], 128 - d, 1)
        settle(left, jnp.where(wide_lane < 128 - d, near, far), d)
        return carry

    lax.fori_loop(0, LANE_STEPS, lane_step, 0)
    for i in range(LANE_STEPS, STEPS):
        dv = 1 << (i - LANE_STEPS)
        settle(shifts[0:chunks, :], shifts[dv : chunks + dv, :], 1 << i)

    zero = jnp.zeros((8, 128), jnp.float32)
    pad = per_row
    for t in range(2):
        for v in range(pad):
            for f in (field_a, field_b):
                f[t, v] = zero
                f[t, pad + chunks + v] = zero
    base = (me * bins_dev) % ND
    cw, ce, cs, cn = [], [], [], []
    for t in range(2):
        k = ((me * bins_dev + jnp.minimum(2 * row + t, bins_dev - 1)) // ND).astype(jnp.float32)
        pace = 0.2 * jnp.exp(-LOG_RATIO * k)
        ax = pace * tab[pl.ds(at["cos"] + base + t, 8, stride=2), :]
        ay = pace * tab[pl.ds(at["sin"] + base + t, 8, stride=2), :]
        cw.append(jnp.maximum(ax, 0.0))
        ce.append(-jnp.minimum(ax, 0.0))
        cs.append(jnp.maximum(ay, 0.0))
        cn.append(-jnp.minimum(ay, 0.0))
    load.wait()

    def sea_row(v):
        return mask2d[pl.ds(v, 1), :] != 0

    def split_bins(g, carry):
        for u in range(8):
            v = g * 8 + u
            cols = pl.ds(pl.multiple_of(v * 128, 128), 128)
            stage[u, 0:bins_dev, :] = jnp.where(sea_row(v), x[:, cols], 0.0)
            for t in range(2):
                field_a[t, pad + v, 0:half, :] = stage[u, pl.ds(t, half, stride=2), :]
        return carry

    lax.fori_loop(0, chunks // 8, split_bins, 0)

    for s in range(SUBSTEPS):
        src, dst = (field_a, field_b) if s % 2 == 0 else (field_b, field_a)

        def advance(g, carry, src=src, dst=dst, s=s):
            for ru in range(4):
                r = g * 4 + ru
                widen = tab[pl.ds(at["widen"] + r, 1), :]
                first = pad + r * per_row
                for t in range(2):
                    west_c, east_c = cw[t] * widen, ce[t] * widen
                    own_c = 1.0 - west_c - east_c - cs[t] - cn[t]
                    e = [src[t, first + q] for q in range(per_row)]
                    right = [pltpu.roll(a, 1, 1) for a in e]
                    left = [pltpu.roll(a, 127, 1) for a in e]
                    for q in range(per_row):
                        west = jnp.where(lane == 0, right[q - 1], right[q])
                        east = jnp.where(lane == 127, left[(q + 1) % per_row], left[q])
                        new = (
                            own_c * e[q] + west_c * west + east_c * east
                            + cs[t] * src[t, first + q - per_row]
                            + cn[t] * src[t, first + q + per_row]
                        )
                        v = first + q - pad
                        if s < SUBSTEPS - 1:
                            dst[t, first + q] = jnp.where(sea_row(v), new, 0.0)
                        else:
                            wind = (speed2d, angle2d)[t][pl.ds(v, 1), :]
                            dst[t, first + q] = jnp.where(row == half, wind, new)
            return carry

        lax.fori_loop(0, lat_count // 4, advance, 0)
    final = field_a if SUBSTEPS % 2 == 0 else field_b

    pl.semaphore_wait(barrier, side * cores + side - 2)
    call_column(column_sem)

    unroll = 8

    def word_of(words, v):
        return jnp.broadcast_to(words[pl.ds(REACH + v, 1), :], (8, 128))

    def has(word, i):
        return jnp.bitwise_and(word, 1 << i) != 0

    def near_rows(words, src, dst, toward_end, bit_order):
        way = 1 if toward_end else -1

        def block(g, carry):
            first = g * unroll
            span = [first + way * u if toward_end else first + unroll - 1 - u for u in range(unroll + 7)]
            word = [word_of(words, v) for v in span]
            for t in range(2):
                cur = [src[t, FAR + v] for v in span]
                for b in bit_order:
                    d = 1 << b
                    cur = [
                        jnp.where(has(word[u], LANE_STEPS + b), cur[u + d], cur[u])
                        for u in range(len(cur) - d)
                    ]
                for u in range(unroll):
                    dst[t, FAR + span[u]] = cur[u]
            return carry

        lax.fori_loop(0, chunks // unroll, block, 0)

    def far_rows(words, src, t, v, way, bit_order):
        def value(v, order):
            if not order:
                return src[t, FAR + v]
            d = way * (1 << order[-1])
            return jnp.where(
                has(word_of(words, v), LANE_STEPS + order[-1]), value(v + d, order[:-1]), value(v, order[:-1])
            )

        return value(v, bit_order)

    def lanes_left(g, carry):
        turned = list(carry)
        for u in range(unroll):
            v = chunks - 1 - (g * unroll + u)
            word = word_of(go_left, v)
            for t in range(2):
                a = final[t, pad + v]
                for i in range(LANE_STEPS):
                    d = 1 << i
                    rot = pltpu.roll(a, 128 - d, 1)
                    b = jnp.where(lane < 128 - d, rot, turned[t * LANE_STEPS + i])
                    turned[t * LANE_STEPS + i] = rot
                    a = jnp.where(has(word, i), b, a)
                moved_a[t, FAR + v] = a
        return tuple(turned)

    lax.fori_loop(0, chunks // unroll, lanes_left, (zero,) * (2 * LANE_STEPS))
    near_rows(go_left, moved_a, moved_b, True, (0, 1, 2))

    def pack(g, carry):
        for u in range(4):
            v = g * 4 + u
            even, odd = (far_rows(go_left, moved_b, t, v, 1, (3, 4, 5)) for t in range(2))
            send[2 * v] = jnp.where(low, even, pltpu.roll(odd, SEA_DEV, 1))
            send[2 * v + 1] = jnp.where(low, pltpu.roll(even, SEA_DEV, 1), odd)
        return carry

    lax.fori_loop(0, n * SEA_DEV // 128 // 4, pack, 0)

    pl.semaphore_wait(column_sem, side - 1)

    def exchange(src, dst, rows, k):
        def push(to):
            pltpu.make_async_remote_copy(
                src_ref=src.at[to, pl.ds(0, rows)],
                dst_ref=dst.at[me, pl.ds(0, rows)],
                send_sem=send_sem.at[k],
                recv_sem=recv_sem.at[k],
                device_id={"spec": to},
                device_id_type=MESH,
            ).start()

        peers(push)
        dst[me] = src[me]

    def finish(ref, rows, sem):
        part = ref.at[pl.ds(0, n - 1), pl.ds(0, rows)]
        pltpu.make_async_copy(part, part, sem).wait()

    exchange(send, recv, half, 0)

    wind = send[me][half : half + 1, :]
    other = pltpu.roll(wind, SEA_DEV, 1)
    speed = jnp.where(low[0:1], wind, other)
    angle = jnp.where(low[0:1], other, wind)
    toward = speed * (
        tab[at["pair_cos"] : at["pair_cos"] + PAIRS, :] * jnp.cos(angle)
        + tab[at["pair_sin"] : at["pair_sin"] + PAIRS, :] * jnp.sin(angle)
    )
    low16 = lax.broadcasted_iota(jnp.int32, (PAIRS, 128), 1) < SEA_DEV
    zero16 = jnp.zeros((PAIRS, 128), jnp.float32)
    for w in range(4):
        for k in (0, 1, 2, NF + 3, NF + 4):
            rolled[w, k] = zero16
    for k in range(2):
        low_part[k] = zero16
    for k in range(3):
        high_part[NF + k] = zero16

    def turns(a, amounts):
        s = pltpu.roll(a, SEA_DEV, 1)
        need = {1: (1, 0), -1: (0, -1), 3: (2, 1), -3: (-1, -2)}
        by = {0: s}
        for m in amounts:
            for w in need[m]:
                if w not in by:
                    by[w] = pltpu.roll(s, w % PAIRS, 0)
        return [jnp.where(low16, by[need[m][0]], by[need[m][1]]) for m in amounts]

    group = 8
    per_group = half * group // PAIRS
    finish(recv, half, recv_sem.at[0])

    def arrange(g, carry):
        m0, m1 = carry
        for i in range(group):
            flat[g, half * i : half * i + half, :] = recv[g * group + i, 0:half, :]
        for q in range(per_group):
            k = g * per_group + q
            a = flat[g, PAIRS * q : PAIRS * (q + 1), :]
            energy[k] = a
            m0 = m0 + a
            m1 = m1 + tab[pl.ds(at["omega"] + k, 1), :] * a
            for w, b in enumerate(turns(a, (1, -1, 3, -3))):
                rolled[w, k + 3] = b
        return m0, m1

    m0, m1 = lax.fori_loop(0, n // group, arrange, (zero16, zero16))

    def over_bins(a):
        a = jnp.sum(a, axis=0, keepdims=True)
        return (a + pltpu.roll(a, SEA_DEV, 1)) * (1.0 / (NF * ND))

    m0, m1 = over_bins(m0), over_bins(m1)
    mean_freq = m1 / (m0 + 1e-6)
    steep = m0 * mean_freq * mean_freq
    breaking = steep * steep / (1.0 + steep * steep)

    def transfer(g, carry):
        for q in range(per_group):
            k = g * per_group + q
            a = energy[k]
            factor = tab[pl.ds(at["rate"] + k, 1), :] * a
            rates = []
            for plus, minus in ((rolled[1, k + 5], rolled[2, k]), (rolled[0, k + 5], rolled[3, k])):
                rates.append(factor * (a * (plus + minus) - 2.0 * plus * minus))
            up, down = turns(rates[0], (1, -3)), turns(rates[1], (-1, 3))
            own[k] = -2.0 * (rates[0] + rates[1])
            low_part[k + 2] = up[0] + down[0]
            high_part[k] = up[1] + down[1]
        return carry

    lax.fori_loop(0, n // group, transfer, 0)

    def renew(g, total):
        for q in range(per_group):
            k = g * per_group + q
            a = energy[k]
            omega = tab[pl.ds(at["omega"] + k, 1), :]
            gain = (0.05 * omega) * jnp.maximum(0.0, omega * toward - 1.0)
            new = a + (gain - (0.03 * omega) * breaking) * a
            new = new + own[k] + low_part[k] + high_part[k + 3]
            total = total + new
            flat[g, PAIRS * q : PAIRS * (q + 1), :] = new
        for i in range(group):
            back[g * group + i, 0:half, :] = flat[g, half * i : half * i + half, :]
        return total

    total = lax.fori_loop(0, n // group, renew, zero16)
    height = 4.0 * jnp.sqrt(over_bins(total) + 1e-6)

    def add_height(g, carry):
        for i in range(group):
            back[g * group + i, half : half + 1, :] = height
        return carry

    lax.fori_loop(0, n // group, add_height, 0)

    exchange(back, home, half + 1, 1)
    finish(send, half, send_sem.at[0])
    finish(home, half + 1, recv_sem.at[1])

    def unpack(g, carry):
        for u in range(unroll):
            v = g * unroll + u
            a, b = home[2 * v], home[2 * v + 1]
            moved_a[0, FAR + v] = jnp.where(low, a, pltpu.roll(b, SEA_DEV, 1))
            moved_a[1, FAR + v] = jnp.where(low, pltpu.roll(a, SEA_DEV, 1), b)
        return carry

    lax.fori_loop(0, n * SEA_DEV // 128 // unroll, unpack, 0)

    def spread(g, carry):
        for u in range(4):
            v = g * 4 + u
            for t in range(2):
                moved_b[t, FAR + v] = far_rows(go_right, moved_a, t, v, -1, (5, 4, 3))
        return carry

    lax.fori_loop(0, chunks // 4, spread, 0)
    near_rows(go_right, moved_b, moved_a, False, (2, 1, 0))

    def lanes_right(g, carry):
        turned = list(carry)
        for u in range(unroll):
            v = g * unroll + u
            word = word_of(go_right, v)
            sea = jnp.broadcast_to(sea_row(v), (8, 128))
            for t in range(2):
                a = moved_a[t, FAR + v]
                for i in range(LANE_STEPS - 1, -1, -1):
                    d = 1 << i
                    rot = pltpu.roll(a, d, 1)
                    b = jnp.where(lane < d, turned[t * LANE_STEPS + i], rot)
                    turned[t * LANE_STEPS + i] = rot
                    a = jnp.where(has(word, i), b, a)
                a = jnp.where(sea, a, 0.0)
                stage[u, pl.ds(t, half, stride=2), :] = a[0:half]
                if t == 0:
                    heights[pl.ds(v, 1), :] = a[half : half + 1]
            out[:, pl.ds(pl.multiple_of(v * 128, 128), 128)] = stage[u, 0:bins_dev, :]
        return tuple(turned)

    lax.fori_loop(0, chunks // unroll, lanes_right, (zero,) * (2 * LANE_STEPS))

    points = cells // n
    together = NLON // points
    start = me // together * per_row
    three = [heights[pl.ds(start + q, 1), :] for q in range(per_row)]
    u = lax.rem(me, together)
    picked = None
    for g in range(together):
        first, offset = g * points // 128, g * points % 128
        piece = three[first]
        if offset:
            after = three[min(first + 1, per_row - 1)]
            piece = jnp.where(
                lane[0:1] < 128 - offset,
                pltpu.roll(piece, 128 - offset, 1),
                pltpu.roll(after, 128 - offset, 1),
            )
        picked = piece if picked is None else jnp.where(u == g, piece, picked)
    height_out[...] = picked[:, 0:points]
    all_heights = jnp.sum(heights[...], axis=0, keepdims=True)
    mean_out[...] = jnp.sum(all_heights, axis=1, keepdims=True) * (1.0 / (SEA_DEV * n))
    finish(back, half + 1, send_sem.at[1])


def solution(mesh):
    n = mesh.shape["spec"]
    cores = 2
    side = math.isqrt(n // cores)

    def local(spectrum, sea_mask, wind_speed, wind_angle):
        bins_dev, cells = spectrum.shape
        chunks = cells // 128
        padded = chunks + 2 * (NLON // 128)
        tab, at = tables(cells // NLON)
        vmem = pl.BlockSpec(memory_space=pltpu.VMEM)
        words = pltpu.VMEM((chunks + 2 * REACH, 128), jnp.int32)
        by_freq = lambda *dims: pltpu.VMEM((*dims, PAIRS, 128), jnp.float32)
        messages = lambda count: pltpu.VMEM((count, 8, 128), jnp.float32)
        new_spectrum, height, mean = pl.pallas_call(
            functools.partial(step_kernel, n, side, cores, at),
            name="wave_step",
            out_shape=(
                jax.ShapeDtypeStruct((bins_dev, cells), jnp.float32),
                jax.ShapeDtypeStruct((1, cells // n), jnp.float32),
                jax.ShapeDtypeStruct((1, 1), jnp.float32),
            ),
            in_specs=[pl.BlockSpec(memory_space=pl.ANY)] + [vmem] * 4,
            out_specs=(vmem,) * 3,
            scratch_shapes=[
                pltpu.VMEM((bins_dev, cells), jnp.float32),
                pltpu.VMEM((2, padded, 8, 128), jnp.float32),
                pltpu.VMEM((2, padded, 8, 128), jnp.float32),
                pltpu.VMEM((8, 16, 128), jnp.float32),
                pltpu.VMEM((chunks + REACH, 128), jnp.int32),
                words,
                words,
                pltpu.VMEM((2, chunks + 2 * FAR, 8, 128), jnp.float32),
                pltpu.VMEM((2, chunks + 2 * FAR, 8, 128), jnp.float32),
                messages(n),
                messages(n),
                messages(n),
                messages(n),
                pltpu.VMEM((n // 8, 8 * bins_dev // 2, 128), jnp.float32),
                by_freq(NF),
                by_freq(4, NF + 5),
                by_freq(NF),
                by_freq(NF + 2),
                by_freq(NF + 3),
                pltpu.VMEM((chunks, 128), jnp.float32),
                pltpu.SemaphoreType.DMA((2,)),
                pltpu.SemaphoreType.DMA((2,)),
                pltpu.SemaphoreType.DMA,
                pltpu.SemaphoreType.REGULAR,
            ],
            compiler_params=pltpu.CompilerParams(collective_id=0, has_side_effects=True),
        )(
            spectrum,
            sea_mask.reshape(chunks, 128),
            wind_speed.reshape(chunks, 128),
            wind_angle.reshape(chunks, 128),
            tab,
        )
        return new_spectrum, height.reshape(-1), mean.reshape(1)

    return jax.shard_map(
        local,
        mesh=mesh,
        in_specs=(P(("grp", "spec"), None), P(), P("grp"), P("grp")),
        out_specs=(P(("grp", "spec"), None), P(("grp", "spec")), P("grp")),
        check_vma=False,
    )
```

```python
import functools
import math

import jax
import jax.numpy as jnp
import numpy as np
from jax import lax
from jax.experimental import pallas as pl
from jax.experimental.pallas import tpu as pltpu
from jax.sharding import PartitionSpec as P

NF = 48
ND = 32
NLON = 384
SUBSTEPS = 2
SEA_DEV = 64
MESH = pl.DeviceIdType.MESH
LOG_RATIO = math.log(1.1)
PAIRS = ND // 2
ROW_STEPS = 6
REACH = 32
FAR = 56


def tables(lat_count):
    heading = 2.0 * np.pi * (np.arange(ND) + 0.5) / ND
    wrapped = np.concatenate([heading, heading[:24]])
    flat = lambda a: np.repeat(np.asarray(a)[:, None], 128, 1)
    paired = np.repeat(heading.reshape(PAIRS, 2), SEA_DEV, axis=1)
    latitude = np.radians(-75.0 + 150.0 * (np.arange(lat_count) + 0.5) / lat_count)
    k = np.arange(NF)
    rows, at = [], {}
    for name, block in (
        ("cos", flat(np.cos(wrapped))),
        ("sin", flat(np.sin(wrapped))),
        ("pair_cos", np.cos(paired)),
        ("pair_sin", np.sin(paired)),
        ("widen", flat(1.0 / np.cos(latitude))),
        ("omega", flat(np.exp(LOG_RATIO * (k - NF // 2)))),
        ("rate", flat(np.where((k >= 3) & (k <= NF - 3), 0.001, 0.0))),
    ):
        at[name] = sum(len(r) for r in rows)
        rows.append(block)
    return np.concatenate(rows).astype(np.float32), at


def step_kernel(
    n, side, cores, at,
    x_hbm, mask2d, speed2d, angle2d, tab,
    out, height_out, mean_out,
    x, field_a, field_b, stage, shifts, go_left, go_right, pick, put, moved_a, moved_b,
    send, recv, back, home, flat, energy, rolled, own, low_part, high_part, heights,
    send_sem, recv_sem, load_sem, column_sem,
):
    bins_dev, cells = x.shape
    half = bins_dev // 2
    chunks = cells // 128
    per_row = NLON // 128
    lat_count = cells // NLON
    me = lax.axis_index("spec")
    my_x, my_y, my_c = me // (side * cores), lax.rem(me // cores, side), lax.rem(me, cores)

    load = pltpu.make_async_copy(x_hbm, x, load_sem)
    load.start()

    def peers(act):
        def hop(u):
            return side // 2 + jnp.where(lax.rem(u, 2) == 0, u // 2, -((u + 1) // 2))

        def chip(s, u):
            px = lax.rem(my_x + hop(u), side)
            py = lax.rem(my_y + hop(s - u), side)
            first = (px * side + py) * cores
            act(first + my_c)
            for c in range(1, cores):
                act(first + lax.rem(my_c + c, cores))

        def diagonal(s, carry):
            def one(u, inner):
                chip(s, u)
                return inner

            return lax.fori_loop(jnp.maximum(0, s - side + 1), jnp.minimum(side - 1, s) + 1, one, carry)

        lax.fori_loop(0, 2 * side - 2, diagonal, 0)
        for c in range(1, cores):
            act(me - my_c + lax.rem(my_c + c, cores))

    barrier = pltpu.get_barrier_semaphore()

    def call_row(i, carry):
        to = (lax.rem(my_x + i // cores, side) * side + my_y) * cores + lax.rem(my_c + lax.rem(i, cores), cores)
        pl.semaphore_signal(barrier, inc=1, device_id={"spec": to}, device_id_type=MESH)
        return carry

    def call_column(semaphore):
        def one(i, carry):
            to = (my_x * side + lax.rem(my_y + i, side)) * cores + my_c
            pl.semaphore_signal(semaphore, inc=1, device_id={"spec": to}, device_id_type=MESH)
            return carry

        lax.fori_loop(1, side, one, 0)

    lax.fori_loop(1, side * cores, call_row, 0)
    call_column(barrier)

    lane = lax.broadcasted_iota(jnp.int32, (8, 128), 1)
    row = lax.broadcasted_iota(jnp.int32, (8, 128), 0)
    low = lane < SEA_DEV

    is_sea = mask2d[...] != 0
    land = jnp.where(is_sea, 0.0, 1.0).astype(jnp.bfloat16)
    earlier = (
        lax.broadcasted_iota(jnp.int32, (128, 128), 0) < lax.broadcasted_iota(jnp.int32, (128, 128), 1)
    ).astype(jnp.bfloat16)
    above = (
        lax.broadcasted_iota(jnp.int32, (chunks, chunks), 1)
        < lax.broadcasted_iota(jnp.int32, (chunks, chunks), 0)
    ).astype(jnp.bfloat16)
    ones = jnp.ones((128, 128), jnp.bfloat16)
    count = functools.partial(jnp.dot, preferred_element_type=jnp.float32)
    before = count(land, earlier).astype(jnp.int32)
    sea_in_row = 128 - count(land, ones).astype(jnp.int32)
    wide_lane = lax.broadcasted_iota(jnp.int32, (chunks, 128), 1)
    wide_row = lax.broadcasted_iota(jnp.int32, (chunks, 128), 0)
    rank0 = wide_row * 128 - count(count(above, land).astype(jnp.bfloat16), ones).astype(jnp.int32)
    put[...] = jnp.bitwise_and(rank0 + wide_lane - before, 127)
    to_go = jnp.where(is_sea, before, 0)
    shifts[chunks:, :] = jnp.zeros((shifts.shape[0] - chunks, 128), jnp.int32)
    go_left[...] = jnp.zeros_like(go_left)
    go_right[...] = jnp.zeros_like(go_right)

    def close_up(i, to_go):
        d = jnp.left_shift(1, i)
        incoming = pltpu.roll(to_go, 128 - d, 1)
        stay = jnp.where(jnp.bitwise_and(to_go, d) != 0, 0, to_go)
        return jnp.where(jnp.bitwise_and(incoming, d) != 0, incoming, stay)

    def plan_rows(to_go):
        nth = jnp.bitwise_and(wide_lane - rank0, 127)
        front = jnp.bitwise_and(wide_lane + to_go, 127)
        pick[...] = jnp.take_along_axis(front, nth, axis=1, mode="promise_in_bounds")
        up = wide_row - jnp.right_shift(rank0 + nth, 7)
        shifts[0:chunks, :] = jnp.where(nth < sea_in_row, up, 0)
        for b in range(ROW_STEPS):
            here, incoming = shifts[0:chunks, :], shifts[1 << b : chunks + (1 << b), :]
            goes = jnp.bitwise_and(here, 1 << b)
            comes = jnp.bitwise_and(incoming, 1 << b)
            go_right[REACH : REACH + chunks, :] += goes
            go_left[REACH : REACH + chunks, :] += comes
            shifts[0:chunks, :] = jnp.where(comes != 0, incoming, jnp.where(goes != 0, 0, here))

    zero = jnp.zeros((8, 128), jnp.float32)
    pad = per_row
    for t in range(2):
        for v in range(pad):
            for f in (field_a, field_b):
                f[t, v] = zero
                f[t, pad + chunks + v] = zero
    base = (me * bins_dev) % ND
    cw, ce, cs, cn = [], [], [], []
    for t in range(2):
        k = ((me * bins_dev + jnp.minimum(2 * row + t, bins_dev - 1)) // ND).astype(jnp.float32)
        pace = 0.2 * jnp.exp(-LOG_RATIO * k)
        ax = pace * tab[pl.ds(at["cos"] + base + t, 8, stride=2), :]
        ay = pace * tab[pl.ds(at["sin"] + base + t, 8, stride=2), :]
        cw.append(jnp.maximum(ax, 0.0))
        ce.append(-jnp.minimum(ax, 0.0))
        cs.append(jnp.maximum(ay, 0.0))
        cn.append(-jnp.minimum(ay, 0.0))
    load.wait()

    def sea_row(v):
        return mask2d[pl.ds(v, 1), :] != 0

    def split_bins(g, carry):
        for u in range(8):
            v = g * 8 + u
            cols = pl.ds(pl.multiple_of(v * 128, 128), 128)
            stage[u, 0:bins_dev, :] = jnp.where(sea_row(v), x[:, cols], 0.0)
            for t in range(2):
                field_a[t, pad + v, 0:half, :] = stage[u, pl.ds(t, half, stride=2), :]
        return carry

    lax.fori_loop(0, chunks // 8, split_bins, 0)

    def lanes(tile, index, v):
        index = jnp.broadcast_to(index[pl.ds(v, 1), :], (8, 128))
        return jnp.take_along_axis(tile, index, axis=1, mode="promise_in_bounds")

    for s in range(SUBSTEPS):
        src, dst = (field_a, field_b) if s % 2 == 0 else (field_b, field_a)

        def advance(g, to_go, src=src, dst=dst, s=s):
            if s == 0:
                to_go = close_up(g, to_go)
            for ru in range(4):
                r = g * 4 + ru
                widen = tab[pl.ds(at["widen"] + r, 1), :]
                first = pad + r * per_row
                for t in range(2):
                    west_c, east_c = cw[t] * widen, ce[t] * widen
                    own_c = 1.0 - west_c - east_c - cs[t] - cn[t]
                    e = [src[t, first + q] for q in range(per_row)]
                    right = [pltpu.roll(a, 1, 1) for a in e]
                    left = [pltpu.roll(a, 127, 1) for a in e]
                    for q in range(per_row):
                        west = jnp.where(lane == 0, right[q - 1], right[q])
                        east = jnp.where(lane == 127, left[(q + 1) % per_row], left[q])
                        new = (
                            own_c * e[q] + west_c * west + east_c * east
                            + cs[t] * src[t, first + q - per_row]
                            + cn[t] * src[t, first + q + per_row]
                        )
                        v = first + q - pad
                        if s < SUBSTEPS - 1:
                            dst[t, first + q] = jnp.where(sea_row(v), new, 0.0)
                        else:
                            wind = (speed2d, angle2d)[t][pl.ds(v, 1), :]
                            new = jnp.where(row == half, wind, new)
                            moved_a[t, FAR + v] = lanes(new, pick, v)
            return to_go

        to_go = lax.fori_loop(0, lat_count // 4, advance, to_go)
        if s == 0:
            plan_rows(to_go)

    pl.semaphore_wait(barrier, side * cores + side - 2)
    call_column(column_sem)

    unroll = 8

    def word_of(words, v):
        return jnp.broadcast_to(words[pl.ds(REACH + v, 1), :], (8, 128))

    def has(word, i):
        return jnp.bitwise_and(word, 1 << i) != 0

    def near_rows(words, src, emit, toward_end, bit_order):
        way = 1 if toward_end else -1

        def block(g, carry):
            first = g * unroll
            span = [first + way * u if toward_end else first + unroll - 1 - u for u in range(unroll + 7)]
            word = [word_of(words, v) for v in span]
            for t in range(2):
                cur = [src[t, FAR + v] for v in span]
                for b in bit_order:
                    d = 1 << b
                    cur = [
                        jnp.where(has(word[u], b), cur[u + d], cur[u])
                        for u in range(len(cur) - d)
                    ]
                for u in range(unroll):
                    emit(t, u, span[u], cur[u])
            return carry

        lax.fori_loop(0, chunks // unroll, block, 0)

    def far_rows(words, src, t, v, way, bit_order):
        def value(v, order):
            if not order:
                return src[t, FAR + v]
            d = way * (1 << order[-1])
            return jnp.where(
                has(word_of(words, v), order[-1]), value(v + d, order[:-1]), value(v, order[:-1])
            )

        return value(v, bit_order)

    def keep_near(t, u, v, tile):
        moved_b[t, FAR + v] = tile

    near_rows(go_left, moved_a, keep_near, True, (0, 1, 2))

    def pack(g, carry):
        for u in range(unroll):
            v = g * unroll + u
            even, odd = (far_rows(go_left, moved_b, t, v, 1, (3, 4, 5)) for t in range(2))
            send[2 * v] = jnp.where(low, even, pltpu.roll(odd, SEA_DEV, 1))
            send[2 * v + 1] = jnp.where(low, pltpu.roll(even, SEA_DEV, 1), odd)
        return carry

    lax.fori_loop(0, n * SEA_DEV // 128 // unroll, pack, 0)

    pl.semaphore_wait(column_sem, side - 1)

    def exchange(src, dst, rows, k):
        def push(to):
            pltpu.make_async_remote_copy(
                src_ref=src.at[to, pl.ds(0, rows)],
                dst_ref=dst.at[me, pl.ds(0, rows)],
                send_sem=send_sem.at[k],
                recv_sem=recv_sem.at[k],
                device_id={"spec": to},
                device_id_type=MESH,
            ).start()

        peers(push)
        dst[me] = src[me]

    def finish(ref, rows, sem):
        part = ref.at[pl.ds(0, n - 1), pl.ds(0, rows)]
        pltpu.make_async_copy(part, part, sem).wait()

    exchange(send, recv, half, 0)

    wind = send[me][half : half + 1, :]
    other = pltpu.roll(wind, SEA_DEV, 1)
    speed = jnp.where(low[0:1], wind, other)
    angle = jnp.where(low[0:1], other, wind)
    toward = speed * (
        tab[at["pair_cos"] : at["pair_cos"] + PAIRS, :] * jnp.cos(angle)
        + tab[at["pair_sin"] : at["pair_sin"] + PAIRS, :] * jnp.sin(angle)
    )
    low16 = lax.broadcasted_iota(jnp.int32, (PAIRS, 128), 1) < SEA_DEV
    zero16 = jnp.zeros((PAIRS, 128), jnp.float32)
    for w in range(4):
        for k in (0, 1, 2, NF + 3, NF + 4):
            rolled[w, k] = zero16
    for k in range(2):
        low_part[k] = zero16
    for k in range(3):
        high_part[NF + k] = zero16

    def turns(a, amounts):
        s = pltpu.roll(a, SEA_DEV, 1)
        need = {1: (1, 0), -1: (0, -1), 3: (2, 1), -3: (-1, -2)}
        by = {0: s}
        for m in amounts:
            for w in need[m]:
                if w not in by:
                    by[w] = pltpu.roll(s, w % PAIRS, 0)
        return [jnp.where(low16, by[need[m][0]], by[need[m][1]]) for m in amounts]

    group = 8
    per_group = half * group // PAIRS
    finish(recv, half, recv_sem.at[0])

    def arrange(h, carry):
        m0, m1 = carry
        for g in (2 * h, 2 * h + 1):
            for i in range(group):
                flat[g, half * i : half * i + half, :] = recv[g * group + i, 0:half, :]
        for g in (2 * h, 2 * h + 1):
            for q in range(per_group):
                k = g * per_group + q
                a = flat[g, PAIRS * q : PAIRS * (q + 1), :]
                energy[k] = a
                m0 = m0 + a
                m1 = m1 + tab[pl.ds(at["omega"] + k, 1), :] * a
                for w, b in enumerate(turns(a, (1, -1, 3, -3))):
                    rolled[w, k + 3] = b
        return m0, m1

    m0, m1 = lax.fori_loop(0, n // group // 2, arrange, (zero16, zero16))

    def over_bins(a):
        a = jnp.sum(a, axis=0, keepdims=True)
        return (a + pltpu.roll(a, SEA_DEV, 1)) * (1.0 / (NF * ND))

    m0, m1 = over_bins(m0), over_bins(m1)
    mean_freq = m1 / (m0 + 1e-6)
    steep = m0 * mean_freq * mean_freq
    breaking = steep * steep / (1.0 + steep * steep)

    def transfer(g, carry):
        for q in range(2 * per_group):
            k = g * 2 * per_group + q
            a = energy[k]
            factor = tab[pl.ds(at["rate"] + k, 1), :] * a
            rates = []
            for plus, minus in ((rolled[1, k + 5], rolled[2, k]), (rolled[0, k + 5], rolled[3, k])):
                rates.append(factor * (a * (plus + minus) - 2.0 * plus * minus))
            up, down = turns(rates[0], (1, -3)), turns(rates[1], (-1, 3))
            own[k] = -2.0 * (rates[0] + rates[1])
            low_part[k + 2] = up[0] + down[0]
            high_part[k] = up[1] + down[1]
        return carry

    lax.fori_loop(0, n // group // 2, transfer, 0)

    def renew(g, total):
        for q in range(per_group):
            k = g * per_group + q
            a = energy[k]
            omega = tab[pl.ds(at["omega"] + k, 1), :]
            gain = (0.05 * omega) * jnp.maximum(0.0, omega * toward - 1.0)
            new = a + (gain - (0.03 * omega) * breaking) * a
            new = new + own[k] + low_part[k] + high_part[k + 3]
            total = total + new
            flat[g, PAIRS * q : PAIRS * (q + 1), :] = new
        for i in range(group):
            back[g * group + i, 0:half, :] = flat[g, half * i : half * i + half, :]
        return total

    total = lax.fori_loop(0, n // group, renew, zero16)
    height = 4.0 * jnp.sqrt(over_bins(total) + 1e-6)

    def add_height(g, carry):
        for i in range(group):
            back[g * group + i, half : half + 1, :] = height
        return carry

    lax.fori_loop(0, n // group, add_height, 0)

    exchange(back, home, half + 1, 1)
    finish(send, half, send_sem.at[0])
    finish(home, half + 1, recv_sem.at[1])

    def unpack(g, carry):
        for u in range(2 * unroll):
            v = g * 2 * unroll + u
            a, b = home[2 * v], home[2 * v + 1]
            moved_a[0, FAR + v] = jnp.where(low, a, pltpu.roll(b, SEA_DEV, 1))
            moved_a[1, FAR + v] = jnp.where(low, pltpu.roll(a, SEA_DEV, 1), b)
        return carry

    lax.fori_loop(0, n * SEA_DEV // 128 // (2 * unroll), unpack, 0)

    def spread(g, carry):
        for u in range(4):
            v = g * 4 + u
            for t in range(2):
                moved_b[t, FAR + v] = far_rows(go_right, moved_a, t, v, -1, (5, 4, 3))
        return carry

    lax.fori_loop(0, chunks // 4, spread, 0)

    def deliver(t, u, v, tile):
        tile = jnp.where(jnp.broadcast_to(sea_row(v), (8, 128)), lanes(tile, put, v), 0.0)
        stage[u, pl.ds(t, half, stride=2), :] = tile[0:half]
        if t == 0:
            heights[pl.ds(v, 1), :] = tile[half : half + 1]
        else:
            out[:, pl.ds(pl.multiple_of(v * 128, 128), 128)] = stage[u, 0:bins_dev, :]

    near_rows(go_right, moved_b, deliver, False, (2, 1, 0))

    points = cells // n
    together = NLON // points
    start = me // together * per_row
    three = [heights[pl.ds(start + q, 1), :] for q in range(per_row)]
    u = lax.rem(me, together)
    picked = None
    for g in range(together):
        first, offset = g * points // 128, g * points % 128
        piece = three[first]
        if offset:
            after = three[min(first + 1, per_row - 1)]
            piece = jnp.where(
                lane[0:1] < 128 - offset,
                pltpu.roll(piece, 128 - offset, 1),
                pltpu.roll(after, 128 - offset, 1),
            )
        picked = piece if picked is None else jnp.where(u == g, piece, picked)
    height_out[...] = picked[:, 0:points]
    all_heights = jnp.sum(heights[...], axis=0, keepdims=True)
    mean_out[...] = jnp.sum(all_heights, axis=1, keepdims=True) * (1.0 / (SEA_DEV * n))
    finish(back, half + 1, send_sem.at[1])


def solution(mesh):
    n = mesh.shape["spec"]
    cores = 2
    side = math.isqrt(n // cores)

    def local(spectrum, sea_mask, wind_speed, wind_angle):
        bins_dev, cells = spectrum.shape
        chunks = cells // 128
        padded = chunks + 2 * (NLON // 128)
        tab, at = tables(cells // NLON)
        vmem = pl.BlockSpec(memory_space=pltpu.VMEM)
        words = pltpu.VMEM((chunks + 2 * REACH, 128), jnp.int32)
        by_freq = lambda *dims: pltpu.VMEM((*dims, PAIRS, 128), jnp.float32)
        messages = lambda count: pltpu.VMEM((count, 8, 128), jnp.float32)
        new_spectrum, height, mean = pl.pallas_call(
            functools.partial(step_kernel, n, side, cores, at),
            name="wave_step",
            out_shape=(
                jax.ShapeDtypeStruct((bins_dev, cells), jnp.float32),
                jax.ShapeDtypeStruct((1, cells // n), jnp.float32),
                jax.ShapeDtypeStruct((1, 1), jnp.float32),
            ),
            in_specs=[pl.BlockSpec(memory_space=pl.ANY)] + [vmem] * 4,
            out_specs=(vmem,) * 3,
            scratch_shapes=[
                pltpu.VMEM((bins_dev, cells), jnp.float32),
                pltpu.VMEM((2, padded, 8, 128), jnp.float32),
                pltpu.VMEM((2, padded, 8, 128), jnp.float32),
                pltpu.VMEM((8, 16, 128), jnp.float32),
                pltpu.VMEM((chunks + REACH, 128), jnp.int32),
                words,
                words,
                pltpu.VMEM((chunks, 128), jnp.int32),
                pltpu.VMEM((chunks, 128), jnp.int32),
                pltpu.VMEM((2, chunks + 2 * FAR, 8, 128), jnp.float32),
                pltpu.VMEM((2, chunks + 2 * FAR, 8, 128), jnp.float32),
                messages(n),
                messages(n),
                messages(n),
                messages(n),
                pltpu.VMEM((n // 8, 8 * bins_dev // 2, 128), jnp.float32),
                by_freq(NF),
                by_freq(4, NF + 5),
                by_freq(NF),
                by_freq(NF + 2),
                by_freq(NF + 3),
                pltpu.VMEM((chunks, 128), jnp.float32),
                pltpu.SemaphoreType.DMA((2,)),
                pltpu.SemaphoreType.DMA((2,)),
                pltpu.SemaphoreType.DMA,
                pltpu.SemaphoreType.REGULAR,
            ],
            compiler_params=pltpu.CompilerParams(collective_id=0, has_side_effects=True),
        )(
            spectrum,
            sea_mask.reshape(chunks, 128),
            wind_speed.reshape(chunks, 128),
            wind_angle.reshape(chunks, 128),
            tab,
        )
        return new_spectrum, height.reshape(-1), mean.reshape(1)

    return jax.shard_map(
        local,
        mesh=mesh,
        in_specs=(P(("grp", "spec"), None), P(), P("grp"), P("grp")),
        out_specs=(P(("grp", "spec"), None), P(("grp", "spec")), P("grp")),
        check_vma=False,
    )
```

```python
import functools
import math

import jax
import jax.numpy as jnp
import numpy as np
from jax import lax
from jax.experimental import pallas as pl
from jax.experimental.pallas import tpu as pltpu
from jax.sharding import PartitionSpec as P

NF = 48
ND = 32
NLON = 384
SUBSTEPS = 2
SEA_DEV = 64
MESH = pl.DeviceIdType.MESH
LOG_RATIO = math.log(1.1)
PAIRS = ND // 2
ROW_STEPS = 6
REACH = 32
FAR = 56


def tables(lat_count):
    heading = 2.0 * np.pi * (np.arange(ND) + 0.5) / ND
    wrapped = np.concatenate([heading, heading[:24]])
    flat = lambda a: np.repeat(np.asarray(a)[:, None], 128, 1)
    paired = np.repeat(heading.reshape(PAIRS, 2), SEA_DEV, axis=1)
    latitude = np.radians(-75.0 + 150.0 * (np.arange(lat_count) + 0.5) / lat_count)
    k = np.arange(NF)
    rows, at = [], {}
    for name, block in (
        ("cos", flat(np.cos(wrapped))),
        ("sin", flat(np.sin(wrapped))),
        ("pair_cos", np.cos(paired)),
        ("pair_sin", np.sin(paired)),
        ("widen", flat(1.0 / np.cos(latitude))),
        ("omega", flat(np.exp(LOG_RATIO * (k - NF // 2)))),
        ("rate", flat(np.where((k >= 3) & (k <= NF - 3), 0.001, 0.0))),
    ):
        at[name] = sum(len(r) for r in rows)
        rows.append(block)
    return np.concatenate(rows).astype(np.float32), at


def step_kernel(
    n, side, cores, at,
    x_hbm, mask_hbm, speed_hbm, angle_hbm, tab_hbm,
    out, height_out, mean_out,
    x, mask2d, speed2d, angle2d, tab, field_a, field_b, stage, shifts, go_left, go_right, pick, put, moved_a, moved_b,
    send, recv, back, home, flat, energy, rolled, own, low_part, high_part, heights,
    send_sem, recv_sem, load_sem, column_sem,
):
    bins_dev, cells = x.shape
    half = bins_dev // 2
    chunks = cells // 128
    per_row = NLON // 128
    lat_count = cells // NLON
    me = lax.axis_index("spec")
    my_x, my_y, my_c = me // (side * cores), lax.rem(me // cores, side), lax.rem(me, cores)

    parts = 4
    part_cols = cells // parts
    small = [
        pltpu.make_async_copy(src, dst, load_sem.at[parts + k])
        for k, (src, dst) in enumerate(
            ((mask_hbm, mask2d), (tab_hbm, tab), (speed_hbm, speed2d), (angle_hbm, angle2d))
        )
    ]

    def load(part):
        cols = pl.ds(pl.multiple_of(part * part_cols, 128), part_cols)
        return pltpu.make_async_copy(x_hbm.at[:, cols], x.at[:, cols], load_sem.at[part])

    small[0].start()
    for part in range(parts):
        load(part).start()
    for copy in small[1:]:
        copy.start()

    def hop(u):
        return side // 2 + jnp.where(lax.rem(u, 2) == 0, u // 2, -((u + 1) // 2))

    def both_cores(act, px, py):
        first = (px * side + py) * cores
        act(first + my_c)
        for c in range(1, cores):
            act(first + lax.rem(my_c + c, cores))

    def own_chip(act):
        for c in range(1, cores):
            act(me - my_c + lax.rem(my_c + c, cores))

    def peers(act):
        def diagonal(s, carry):
            def one(u, inner):
                both_cores(act, lax.rem(my_x + hop(u), side), lax.rem(my_y + hop(s - u), side))
                return inner

            return lax.fori_loop(jnp.maximum(0, s - side + 1), jnp.minimum(side - 1, s) + 1, one, carry)

        lax.fori_loop(0, 2 * side - 2, diagonal, 0)
        own_chip(act)

    def peers_by_row(act):
        def row_of(py, count):
            def one(u, inner):
                both_cores(act, lax.rem(my_x + hop(u), side), py)
                return inner

            lax.fori_loop(0, count, one, 0)

        def far_row(i, carry):
            py = lax.rem(my_y + hop(i), side)
            pl.semaphore_wait(column_sem.at[py], 1)
            row_of(py, side)
            return carry

        lax.fori_loop(0, side - 1, far_row, 0)
        row_of(my_y, side - 1)
        own_chip(act)

    barrier = pltpu.get_barrier_semaphore()

    def call_row(i, carry):
        to = (lax.rem(my_x + i // cores, side) * side + my_y) * cores + lax.rem(my_c + lax.rem(i, cores), cores)
        pl.semaphore_signal(barrier, inc=1, device_id={"spec": to}, device_id_type=MESH)
        return carry

    def call_column(semaphore):
        def one(i, carry):
            to = (my_x * side + lax.rem(my_y + i, side)) * cores + my_c
            pl.semaphore_signal(semaphore, inc=1, device_id={"spec": to}, device_id_type=MESH)
            return carry

        lax.fori_loop(1, side, one, 0)

    lax.fori_loop(1, side * cores, call_row, 0)
    call_column(barrier)
    small[0].wait()

    lane = lax.broadcasted_iota(jnp.int32, (8, 128), 1)
    row = lax.broadcasted_iota(jnp.int32, (8, 128), 0)
    low = lane < SEA_DEV

    is_sea = mask2d[...] != 0
    land = jnp.where(is_sea, 0.0, 1.0).astype(jnp.bfloat16)
    earlier = (
        lax.broadcasted_iota(jnp.int32, (128, 128), 0) < lax.broadcasted_iota(jnp.int32, (128, 128), 1)
    ).astype(jnp.bfloat16)
    above = (
        lax.broadcasted_iota(jnp.int32, (chunks, chunks), 1)
        < lax.broadcasted_iota(jnp.int32, (chunks, chunks), 0)
    ).astype(jnp.bfloat16)
    ones = jnp.ones((128, 128), jnp.bfloat16)
    count = functools.partial(jnp.dot, preferred_element_type=jnp.float32)
    before = count(land, earlier).astype(jnp.int32)
    sea_in_row = 128 - count(land, ones).astype(jnp.int32)
    wide_lane = lax.broadcasted_iota(jnp.int32, (chunks, 128), 1)
    wide_row = lax.broadcasted_iota(jnp.int32, (chunks, 128), 0)
    rank0 = wide_row * 128 - count(count(above, land).astype(jnp.bfloat16), ones).astype(jnp.int32)
    put[0] = jnp.bitwise_and(rank0 + wide_lane - before, 127)
    put[1] = jnp.bitwise_and(rank0 + wide_lane - before + SEA_DEV, 127)
    to_go = jnp.where(is_sea, before, 0)
    shifts[chunks:, :] = jnp.zeros((shifts.shape[0] - chunks, 128), jnp.int32)
    go_left[...] = jnp.zeros_like(go_left)
    go_right[...] = jnp.zeros_like(go_right)

    def close_up(i, to_go):
        d = jnp.left_shift(1, i)
        incoming = pltpu.roll(to_go, 128 - d, 1)
        stay = jnp.where(jnp.bitwise_and(to_go, d) != 0, 0, to_go)
        return jnp.where(jnp.bitwise_and(incoming, d) != 0, incoming, stay)

    def plan_rows(to_go):
        nth = jnp.bitwise_and(wide_lane - rank0, 127)
        front = jnp.bitwise_and(wide_lane + to_go, 127)
        took = jnp.take_along_axis(front, nth, axis=1, mode="promise_in_bounds")
        pick[0] = took
        pick[1] = pltpu.roll(took, SEA_DEV, 1)
        up = wide_row - jnp.right_shift(rank0 + nth, 7)
        shifts[0:chunks, :] = jnp.where(nth < sea_in_row, up, 0)
        for b in range(ROW_STEPS):
            here, incoming = shifts[0:chunks, :], shifts[1 << b : chunks + (1 << b), :]
            goes = jnp.bitwise_and(here, 1 << b)
            comes = jnp.bitwise_and(incoming, 1 << b)
            rights, lefts = (goes, comes) if b == 0 else (rights + goes, lefts + comes)
            shifts[0:chunks, :] = jnp.where(comes != 0, incoming, jnp.where(goes != 0, 0, here))
        for words, found in ((go_right, rights), (go_left, lefts)):
            words[0, REACH : REACH + chunks, :] = found
            words[1, REACH : REACH + chunks, :] = pltpu.roll(found, SEA_DEV, 1)

    zero = jnp.zeros((8, 128), jnp.float32)
    pad = per_row
    for t in range(2):
        for v in range(pad):
            for f in (field_a, field_b):
                f[t, v] = zero
                f[t, pad + chunks + v] = zero
    base = (me * bins_dev) % ND
    for copy in small[1:]:
        copy.wait()
    cw, ce, cs, cn = [], [], [], []
    for t in range(2):
        k = ((me * bins_dev + jnp.minimum(2 * row + t, bins_dev - 1)) // ND).astype(jnp.float32)
        pace = 0.2 * jnp.exp(-LOG_RATIO * k)
        ax = pace * tab[pl.ds(at["cos"] + base + t, 8, stride=2), :]
        ay = pace * tab[pl.ds(at["sin"] + base + t, 8, stride=2), :]
        cw.append(jnp.maximum(ax, 0.0))
        ce.append(-jnp.minimum(ax, 0.0))
        cs.append(jnp.maximum(ay, 0.0))
        cn.append(-jnp.minimum(ay, 0.0))

    def sea_row(v):
        return mask2d[pl.ds(v, 1), :] != 0

    def split_bins(g, carry):
        for u in range(8):
            v = g * 8 + u
            cols = pl.ds(pl.multiple_of(v * 128, 128), 128)
            stage[u, 0:bins_dev, :] = jnp.where(sea_row(v), x[:, cols], 0.0)
            for t in range(2):
                field_a[t, pad + v, 0:half, :] = stage[u, pl.ds(t, half, stride=2), :]
        return carry

    def split_part(part, carry):
        load(part).wait()
        per_part = chunks // 8 // parts
        return lax.fori_loop(part * per_part, (part + 1) * per_part, split_bins, carry)

    lax.fori_loop(0, parts, split_part, 0)

    def lanes(tile, index, v):
        index = jnp.broadcast_to(index[pl.ds(v, 1), :], (8, 128))
        return jnp.take_along_axis(tile, index, axis=1, mode="promise_in_bounds")

    for s in range(SUBSTEPS):
        src, dst = (field_a, field_b) if s % 2 == 0 else (field_b, field_a)

        def advance(g, to_go, src=src, dst=dst, s=s):
            if s == 0:
                to_go = close_up(g, to_go)
            else:
                behind = jnp.maximum(g - 1, 0) * 4 * per_row
                for u in range(4 * per_row):
                    for t in range(2):
                        v = behind + u
                        moved_a[t, FAR + v] = lanes(dst[t, pad + v], pick.at[t], v)
            for ru in range(4):
                r = jnp.minimum(g, lat_count // 4 - 1) * 4 + ru
                widen = tab[pl.ds(at["widen"] + r, 1), :]
                first = pad + r * per_row
                for t in range(2):
                    west_c, east_c = cw[t] * widen, ce[t] * widen
                    own_c = 1.0 - west_c - east_c - cs[t] - cn[t]
                    e = [src[t, first + q] for q in range(per_row)]
                    right = [pltpu.roll(a, 1, 1) for a in e]
                    left = [pltpu.roll(a, 127, 1) for a in e]
                    for q in range(per_row):
                        west = jnp.where(lane == 0, right[q - 1], right[q])
                        east = jnp.where(lane == 127, left[(q + 1) % per_row], left[q])
                        new = (
                            own_c * e[q] + west_c * west + east_c * east
                            + cs[t] * src[t, first + q - per_row]
                            + cn[t] * src[t, first + q + per_row]
                        )
                        v = first + q - pad
                        if s < SUBSTEPS - 1:
                            dst[t, first + q] = jnp.where(sea_row(v), new, 0.0)
                        else:
                            wind = (speed2d, angle2d)[t][pl.ds(v, 1), :]
                            dst[t, first + q] = jnp.where(row == half, wind, new)
            return to_go

        to_go = lax.fori_loop(0, lat_count // 4 + min(s, 1), advance, to_go)
        if s == 0:
            plan_rows(to_go)

    pl.semaphore_wait(barrier, side * cores + side - 2)
    call_column(column_sem.at[my_y])

    unroll = 8

    def word_of(words, v):
        return jnp.broadcast_to(words[pl.ds(REACH + v, 1), :], (8, 128))

    def has(word, i):
        return jnp.bitwise_and(word, 1 << i) != 0

    def near_rows(words, src, emit, toward_end, bit_order):
        way = 1 if toward_end else -1

        def block(g, carry):
            first = g * unroll
            span = [first + way * u if toward_end else first + unroll - 1 - u for u in range(unroll + 7)]
            for t in range(2):
                word = [word_of(words.at[t], v) for v in span]
                cur = [src[t, FAR + v] for v in span]
                for b in bit_order:
                    d = 1 << b
                    cur = [
                        jnp.where(has(word[u], b), cur[u + d], cur[u])
                        for u in range(len(cur) - d)
                    ]
                for u in range(unroll):
                    emit(t, u, span[u], cur[u])
            return carry

        lax.fori_loop(0, chunks // unroll, block, 0)

    def far_rows(words, src, t, v, way, bit_order):
        def value(v, order):
            if not order:
                return src[t, FAR + v]
            d = way * (1 << order[-1])
            return jnp.where(
                has(word_of(words.at[t], v), order[-1]), value(v + d, order[:-1]), value(v, order[:-1])
            )

        return value(v, bit_order)

    def keep_near(t, u, v, tile):
        moved_b[t, FAR + v] = tile

    near_rows(go_left, moved_a, keep_near, True, (0, 1, 2))

    def pack(g, carry):
        for u in range(unroll):
            v = g * unroll + u
            even, odd = (far_rows(go_left, moved_b, t, v, 1, (3, 4, 5)) for t in range(2))
            send[2 * v] = jnp.where(low, even, odd)
            send[2 * v + 1] = jnp.where(low, odd, even)
        return carry

    lax.fori_loop(0, n * SEA_DEV // 128 // unroll, pack, 0)


    def exchange(visit, src, dst, rows, k, arrival):
        def push(to):
            pltpu.make_async_remote_copy(
                src_ref=src.at[to, pl.ds(0, rows)],
                dst_ref=dst.at[me, pl.ds(0, rows)],
                send_sem=send_sem.at[k],
                recv_sem=arrival,
                device_id={"spec": to},
                device_id_type=MESH,
            ).start()

        visit(push)
        pltpu.make_async_copy(src.at[me, pl.ds(0, rows)], dst.at[me, pl.ds(0, rows)], arrival).start()

    def finish(ref, count, rows, sem):
        part = ref.at[pl.ds(0, count), pl.ds(0, rows)]
        pltpu.make_async_copy(part, part, sem).wait()

    exchange(peers_by_row, send, recv, half, 0, recv_sem.at[my_x])

    wind = send[me][half : half + 1, :]
    other = pltpu.roll(wind, SEA_DEV, 1)
    odd_side = lax.rem(me, 2) * SEA_DEV
    even_half = lambda shape: jnp.bitwise_xor(lax.broadcasted_iota(jnp.int32, shape, 1), odd_side) < SEA_DEV
    low16 = even_half((PAIRS, 128))
    speed = jnp.where(even_half((1, 128)), wind, other)
    angle = jnp.where(even_half((1, 128)), other, wind)

    def paired(name):
        rows = tab[at[name] : at[name] + PAIRS, :]
        return jnp.where(odd_side == 0, rows, pltpu.roll(rows, SEA_DEV, 1))

    toward = speed * (paired("pair_cos") * jnp.cos(angle) + paired("pair_sin") * jnp.sin(angle))
    zero16 = jnp.zeros((PAIRS, 128), jnp.float32)
    for w in range(4):
        for k in (0, 1, 2, NF + 3, NF + 4):
            rolled[w, k] = zero16
    for k in range(2):
        low_part[k] = zero16
    for k in range(3):
        high_part[NF + k] = zero16

    def turns(a, amounts):
        s = pltpu.roll(a, SEA_DEV, 1)
        need = {1: (1, 0), -1: (0, -1), 3: (2, 1), -3: (-1, -2)}
        by = {0: s}
        for m in amounts:
            for w in need[m]:
                if w not in by:
                    by[w] = pltpu.roll(s, w % PAIRS, 0)
        return [jnp.where(low16, by[need[m][0]], by[need[m][1]]) for m in amounts]

    group = 8
    per_group = half * group // PAIRS

    def arrange(i, carry):
        m0, m1 = carry
        h = lax.rem(my_x + hop(i), side)
        finish(recv, side * cores, half, recv_sem.at[h])
        for g in (2 * h, 2 * h + 1):
            for i in range(group):
                flat[g, half * i : half * i + half, :] = recv[g * group + i, 0:half, :]
        for g in (2 * h, 2 * h + 1):
            for q in range(per_group):
                k = g * per_group + q
                a = flat[g, PAIRS * q : PAIRS * (q + 1), :]
                energy[k] = a
                m0 = m0 + a
                m1 = m1 + tab[pl.ds(at["omega"] + k, 1), :] * a
                for w, b in enumerate(turns(a, (1, -1, 3, -3))):
                    rolled[w, k + 3] = b
        return m0, m1

    m0, m1 = lax.fori_loop(0, side, arrange, (zero16, zero16))

    def over_bins(a):
        a = jnp.sum(a, axis=0, keepdims=True)
        return (a + pltpu.roll(a, SEA_DEV, 1)) * (1.0 / (NF * ND))

    m0, m1 = over_bins(m0), over_bins(m1)
    mean_freq = m1 / (m0 + 1e-6)
    steep = m0 * mean_freq * mean_freq
    breaking = steep * steep / (1.0 + steep * steep)

    def transfer(g, carry):
        for q in range(2 * per_group):
            k = g * 2 * per_group + q
            a = energy[k]
            factor = tab[pl.ds(at["rate"] + k, 1), :] * a
            rates = []
            for plus, minus in ((rolled[1, k + 5], rolled[2, k]), (rolled[0, k + 5], rolled[3, k])):
                rates.append(factor * (a * (plus + minus) - 2.0 * plus * minus))
            up, down = turns(rates[0], (1, -3)), turns(rates[1], (-1, 3))
            own[k] = -2.0 * (rates[0] + rates[1])
            low_part[k + 2] = up[0] + down[0]
            high_part[k] = up[1] + down[1]
        return carry

    lax.fori_loop(0, n // group // 2, transfer, 0)

    def renew(g, total):
        for q in range(per_group):
            k = g * per_group + q
            a = energy[k]
            omega = tab[pl.ds(at["omega"] + k, 1), :]
            gain = (0.05 * omega) * jnp.maximum(0.0, omega * toward - 1.0)
            new = a + (gain - (0.03 * omega) * breaking) * a
            new = new + own[k] + low_part[k] + high_part[k + 3]
            total = total + new
            flat[g, PAIRS * q : PAIRS * (q + 1), :] = new
        for i in range(group):
            back[g * group + i, 0:half, :] = flat[g, half * i : half * i + half, :]
        return total

    total = lax.fori_loop(0, n // group, renew, zero16)
    height = 4.0 * jnp.sqrt(over_bins(total) + 1e-6)

    def add_height(g, carry):
        for i in range(group):
            back[g * group + i, half : half + 1, :] = height
        return carry

    lax.fori_loop(0, n // group, add_height, 0)

    exchange(peers, back, home, half + 1, 1, recv_sem.at[side])
    finish(send, n - 1, half, send_sem.at[0])
    finish(home, n, half + 1, recv_sem.at[side])

    def unpack(g, carry):
        for u in range(2 * unroll):
            v = g * 2 * unroll + u
            a, b = home[2 * v], home[2 * v + 1]
            moved_a[0, FAR + v] = jnp.where(low, a, b)
            moved_a[1, FAR + v] = jnp.where(low, b, a)
        return carry

    lax.fori_loop(0, n * SEA_DEV // 128 // (2 * unroll), unpack, 0)

    def spread(g, carry):
        for u in range(4):
            v = g * 4 + u
            for t in range(2):
                moved_b[t, FAR + v] = far_rows(go_right, moved_a, t, v, -1, (5, 4, 3))
        return carry

    lax.fori_loop(0, chunks // 4, spread, 0)

    def keep_apart(t, u, v, tile):
        moved_a[t, FAR + v] = tile

    near_rows(go_right, moved_b, keep_apart, False, (2, 1, 0))

    def deliver(g, carry):
        for u in range(2 * unroll):
            v = g * 2 * unroll + u
            sea = jnp.broadcast_to(sea_row(v), (8, 128))
            for t in range(2):
                tile = jnp.where(sea, lanes(moved_a[t, FAR + v], put.at[t], v), 0.0)
                stage[u, pl.ds(t, half, stride=2), :] = tile[0:half]
                if t == 0:
                    heights[pl.ds(v, 1), :] = tile[half : half + 1]
        for u in range(2 * unroll):
            v = g * 2 * unroll + u
            out[:, pl.ds(pl.multiple_of(v * 128, 128), 128)] = stage[u, 0:bins_dev, :]
        return carry

    lax.fori_loop(0, chunks // (2 * unroll), deliver, 0)

    points = cells // n
    together = NLON // points
    start = me // together * per_row
    three = [heights[pl.ds(start + q, 1), :] for q in range(per_row)]
    u = lax.rem(me, together)
    picked = None
    for g in range(together):
        first, offset = g * points // 128, g * points % 128
        piece = three[first]
        if offset:
            after = three[min(first + 1, per_row - 1)]
            piece = jnp.where(
                lane[0:1] < 128 - offset,
                pltpu.roll(piece, 128 - offset, 1),
                pltpu.roll(after, 128 - offset, 1),
            )
        picked = piece if picked is None else jnp.where(u == g, piece, picked)
    height_out[...] = picked[:, 0:points]
    all_heights = jnp.sum(heights[...], axis=0, keepdims=True)
    mean_out[...] = jnp.sum(all_heights, axis=1, keepdims=True) * (1.0 / (SEA_DEV * n))
    finish(back, n - 1, half + 1, send_sem.at[1])


def solution(mesh):
    n = mesh.shape["spec"]
    cores = 2
    side = math.isqrt(n // cores)

    def local(spectrum, sea_mask, wind_speed, wind_angle):
        bins_dev, cells = spectrum.shape
        chunks = cells // 128
        padded = chunks + 2 * (NLON // 128)
        tab, at = tables(cells // NLON)
        vmem = pl.BlockSpec(memory_space=pltpu.VMEM)
        words = pltpu.VMEM((2, chunks + 2 * REACH, 128), jnp.int32)
        by_freq = lambda *dims: pltpu.VMEM((*dims, PAIRS, 128), jnp.float32)
        messages = lambda count: pltpu.VMEM((count, 8, 128), jnp.float32)
        new_spectrum, height, mean = pl.pallas_call(
            functools.partial(step_kernel, n, side, cores, at),
            name="wave_step",
            out_shape=(
                jax.ShapeDtypeStruct((bins_dev, cells), jnp.float32),
                jax.ShapeDtypeStruct((1, cells // n), jnp.float32),
                jax.ShapeDtypeStruct((1, 1), jnp.float32),
            ),
            in_specs=[pl.BlockSpec(memory_space=pl.ANY)] * 5,
            out_specs=(vmem,) * 3,
            scratch_shapes=[
                pltpu.VMEM((bins_dev, cells), jnp.float32),
                pltpu.VMEM((chunks, 128), jnp.int32),
                pltpu.VMEM((chunks, 128), jnp.float32),
                pltpu.VMEM((chunks, 128), jnp.float32),
                pltpu.VMEM(tab.shape, jnp.float32),
                pltpu.VMEM((2, padded, 8, 128), jnp.float32),
                pltpu.VMEM((2, padded, 8, 128), jnp.float32),
                pltpu.VMEM((16, 16, 128), jnp.float32),
                pltpu.VMEM((chunks + REACH, 128), jnp.int32),
                words,
                words,
                pltpu.VMEM((2, chunks, 128), jnp.int32),
                pltpu.VMEM((2, chunks, 128), jnp.int32),
                pltpu.VMEM((2, chunks + 2 * FAR, 8, 128), jnp.float32),
                pltpu.VMEM((2, chunks + 2 * FAR, 8, 128), jnp.float32),
                messages(n),
                messages(n),
                messages(n),
                messages(n),
                pltpu.VMEM((n // 8, 8 * bins_dev // 2, 128), jnp.float32),
                by_freq(NF),
                by_freq(4, NF + 5),
                by_freq(NF),
                by_freq(NF + 2),
                by_freq(NF + 3),
                pltpu.VMEM((chunks, 128), jnp.float32),
                pltpu.SemaphoreType.DMA((2,)),
                pltpu.SemaphoreType.DMA((side + 1,)),
                pltpu.SemaphoreType.DMA((8,)),
                pltpu.SemaphoreType.REGULAR((side,)),
            ],
            compiler_params=pltpu.CompilerParams(collective_id=0, has_side_effects=True),
        )(
            spectrum,
            sea_mask.reshape(chunks, 128),
            wind_speed.reshape(chunks, 128),
            wind_angle.reshape(chunks, 128),
            tab,
        )
        return new_spectrum, height.reshape(-1), mean.reshape(1)

    return jax.shard_map(
        local,
        mesh=mesh,
        in_specs=(P(("grp", "spec"), None), P(), P("grp"), P("grp")),
        out_specs=(P(("grp", "spec"), None), P(("grp", "spec")), P("grp")),
        check_vma=False,
    )
```

```python
import functools
import math

import jax
import jax.numpy as jnp
import numpy as np
from jax import lax
from jax.experimental import pallas as pl
from jax.experimental.pallas import tpu as pltpu
from jax.sharding import PartitionSpec as P

NF = 48
ND = 32
NLON = 384
SUBSTEPS = 2
SEA_DEV = 64
MESH = pl.DeviceIdType.MESH
LOG_RATIO = math.log(1.1)
PAIRS = ND // 2
ROW_STEPS = 6
REACH = 32
FAR = 56


def tables(lat_count):
    heading = 2.0 * np.pi * (np.arange(ND) + 0.5) / ND
    wrapped = np.concatenate([heading, heading[:24]])
    flat = lambda a: np.repeat(np.asarray(a)[:, None], 128, 1)
    paired = np.repeat(heading.reshape(PAIRS, 2), SEA_DEV, axis=1)
    latitude = np.radians(-75.0 + 150.0 * (np.arange(lat_count) + 0.5) / lat_count)
    k = np.arange(NF)
    rows, at = [], {}
    for name, block in (
        ("cos", flat(np.cos(wrapped))),
        ("sin", flat(np.sin(wrapped))),
        ("pair_cos", np.cos(paired)),
        ("pair_sin", np.sin(paired)),
        ("widen", flat(1.0 / np.cos(latitude))),
        ("omega", flat(np.exp(LOG_RATIO * (k - NF // 2)))),
        ("rate", flat(np.where((k >= 3) & (k <= NF - 3), 0.001, 0.0))),
    ):
        at[name] = sum(len(r) for r in rows)
        rows.append(block)
    return np.concatenate(rows).astype(np.float32), at


def step_kernel(
    n, side, cores, at,
    x_hbm, mask_hbm, speed_hbm, angle_hbm, tab_hbm,
    out, height_out, mean_out,
    x, mask2d, speed2d, angle2d, tab, field_a, field_b, stage, shifts, go_left, go_right, pick, put, moved_a, moved_b,
    send, recv, back, home, flat, energy, rolled, own, low_part, high_part, heights,
    send_sem, recv_sem, load_sem, column_sem,
):
    bins_dev, cells = x.shape
    half = bins_dev // 2
    chunks = cells // 128
    per_row = NLON // 128
    lat_count = cells // NLON
    me = lax.axis_index("spec")
    my_x, my_y, my_c = me // (side * cores), lax.rem(me // cores, side), lax.rem(me, cores)

    parts = 4
    part_cols = cells // parts
    small = [
        pltpu.make_async_copy(src, dst, load_sem.at[parts + k])
        for k, (src, dst) in enumerate(
            ((mask_hbm, mask2d), (tab_hbm, tab), (speed_hbm, speed2d), (angle_hbm, angle2d))
        )
    ]

    def load(part):
        cols = pl.ds(pl.multiple_of(part * part_cols, 128), part_cols)
        return pltpu.make_async_copy(x_hbm.at[:, cols], x.at[:, cols], load_sem.at[part])

    small[0].start()
    for part in range(parts):
        load(part).start()
    for copy in small[1:]:
        copy.start()

    def hop(u):
        return side // 2 + jnp.where(lax.rem(u, 2) == 0, u // 2, -((u + 1) // 2))

    def both_cores(act, px, py):
        first = (px * side + py) * cores
        act(first + my_c)
        for c in range(1, cores):
            act(first + lax.rem(my_c + c, cores))

    def own_chip(act):
        for c in range(1, cores):
            act(me - my_c + lax.rem(my_c + c, cores))

    def peers(act):
        def diagonal(s, carry):
            def one(u, inner):
                both_cores(act, lax.rem(my_x + hop(u), side), lax.rem(my_y + hop(s - u), side))
                return inner

            return lax.fori_loop(jnp.maximum(0, s - side + 1), jnp.minimum(side - 1, s) + 1, one, carry)

        lax.fori_loop(0, 2 * side - 2, diagonal, 0)
        own_chip(act)

    def peers_by_row(act):
        def row_of(py, count):
            def one(u, inner):
                both_cores(act, lax.rem(my_x + hop(u), side), py)
                return inner

            lax.fori_loop(0, count, one, 0)

        def far_row(i, carry):
            py = lax.rem(my_y + hop(i), side)

            @pl.when(py != 0)
            def _():
                pl.semaphore_wait(column_sem.at[py], 1)
                row_of(py, side)

            return carry

        lax.fori_loop(0, side - 1, far_row, 0)
        row_of(my_y, side - 1)
        own_chip(act)

        @pl.when(my_y != 0)
        def _():
            pl.semaphore_wait(column_sem.at[0], 1)
            row_of(0, side)


    barrier = pltpu.get_barrier_semaphore()

    def call_row(i, carry):
        to = (lax.rem(my_x + i // cores, side) * side + my_y) * cores + lax.rem(my_c + lax.rem(i, cores), cores)
        pl.semaphore_signal(barrier, inc=1, device_id={"spec": to}, device_id_type=MESH)
        return carry

    def call_column(semaphore):
        def one(i, carry):
            to = (my_x * side + lax.rem(my_y + i, side)) * cores + my_c
            pl.semaphore_signal(semaphore, inc=1, device_id={"spec": to}, device_id_type=MESH)
            return carry

        lax.fori_loop(1, side, one, 0)

    lax.fori_loop(1, side * cores, call_row, 0)
    call_column(barrier)
    small[0].wait()

    lane = lax.broadcasted_iota(jnp.int32, (8, 128), 1)
    row = lax.broadcasted_iota(jnp.int32, (8, 128), 0)
    low = lane < SEA_DEV

    is_sea = mask2d[...] != 0
    land = jnp.where(is_sea, 0.0, 1.0).astype(jnp.bfloat16)
    earlier = (
        lax.broadcasted_iota(jnp.int32, (128, 128), 0) < lax.broadcasted_iota(jnp.int32, (128, 128), 1)
    ).astype(jnp.bfloat16)
    above = (
        lax.broadcasted_iota(jnp.int32, (chunks, chunks), 1)
        < lax.broadcasted_iota(jnp.int32, (chunks, chunks), 0)
    ).astype(jnp.bfloat16)
    ones = jnp.ones((128, 128), jnp.bfloat16)
    count = functools.partial(jnp.dot, preferred_element_type=jnp.float32)
    before = count(land, earlier).astype(jnp.int32)
    sea_in_row = 128 - count(land, ones).astype(jnp.int32)
    wide_lane = lax.broadcasted_iota(jnp.int32, (chunks, 128), 1)
    wide_row = lax.broadcasted_iota(jnp.int32, (chunks, 128), 0)
    rank0 = wide_row * 128 - count(count(above, land).astype(jnp.bfloat16), ones).astype(jnp.int32)
    put[0] = jnp.bitwise_and(rank0 + wide_lane - before, 127)
    put[1] = jnp.bitwise_and(rank0 + wide_lane - before + SEA_DEV, 127)
    to_go = jnp.where(is_sea, before, 0)
    shifts[chunks:, :] = jnp.zeros((shifts.shape[0] - chunks, 128), jnp.int32)
    go_left[...] = jnp.zeros_like(go_left)
    go_right[...] = jnp.zeros_like(go_right)

    def close_up(i, to_go):
        d = jnp.left_shift(1, i)
        incoming = pltpu.roll(to_go, 128 - d, 1)
        stay = jnp.where(jnp.bitwise_and(to_go, d) != 0, 0, to_go)
        return jnp.where(jnp.bitwise_and(incoming, d) != 0, incoming, stay)

    def plan_rows(to_go):
        nth = jnp.bitwise_and(wide_lane - rank0, 127)
        front = jnp.bitwise_and(wide_lane + to_go, 127)
        took = jnp.take_along_axis(front, nth, axis=1, mode="promise_in_bounds")
        pick[0] = took
        pick[1] = pltpu.roll(took, SEA_DEV, 1)
        up = wide_row - jnp.right_shift(rank0 + nth, 7)
        shifts[0:chunks, :] = jnp.where(nth < sea_in_row, up, 0)
        for b in range(ROW_STEPS):
            here, incoming = shifts[0:chunks, :], shifts[1 << b : chunks + (1 << b), :]
            goes = jnp.bitwise_and(here, 1 << b)
            comes = jnp.bitwise_and(incoming, 1 << b)
            rights, lefts = (goes, comes) if b == 0 else (rights + goes, lefts + comes)
            shifts[0:chunks, :] = jnp.where(comes != 0, incoming, jnp.where(goes != 0, 0, here))
        for words, found in ((go_right, rights), (go_left, lefts)):
            words[0, REACH : REACH + chunks, :] = found
            words[1, REACH : REACH + chunks, :] = pltpu.roll(found, SEA_DEV, 1)

    zero = jnp.zeros((8, 128), jnp.float32)
    pad = per_row
    for t in range(2):
        for v in range(pad):
            for f in (field_a, field_b):
                f[t, v] = zero
                f[t, pad + chunks + v] = zero
    base = (me * bins_dev) % ND
    for copy in small[1:]:
        copy.wait()
    cw, ce, cs, cn = [], [], [], []
    for t in range(2):
        k = ((me * bins_dev + jnp.minimum(2 * row + t, bins_dev - 1)) // ND).astype(jnp.float32)
        pace = 0.2 * jnp.exp(-LOG_RATIO * k)
        ax = pace * tab[pl.ds(at["cos"] + base + t, 8, stride=2), :]
        ay = pace * tab[pl.ds(at["sin"] + base + t, 8, stride=2), :]
        cw.append(jnp.maximum(ax, 0.0))
        ce.append(-jnp.minimum(ax, 0.0))
        cs.append(jnp.maximum(ay, 0.0))
        cn.append(-jnp.minimum(ay, 0.0))

    def sea_row(v):
        return mask2d[pl.ds(v, 1), :] != 0

    def split_bins(g, carry):
        for u in range(8):
            v = g * 8 + u
            cols = pl.ds(pl.multiple_of(v * 128, 128), 128)
            stage[u, 0:bins_dev, :] = jnp.where(sea_row(v), x[:, cols], 0.0)
            for t in range(2):
                field_a[t, pad + v, 0:half, :] = stage[u, pl.ds(t, half, stride=2), :]
        return carry

    def split_part(part, carry):
        load(part).wait()
        per_part = chunks // 8 // parts
        return lax.fori_loop(part * per_part, (part + 1) * per_part, split_bins, carry)

    lax.fori_loop(0, parts, split_part, 0)

    def lanes(tile, index, v):
        index = jnp.broadcast_to(index[pl.ds(v, 1), :], (8, 128))
        return jnp.take_along_axis(tile, index, axis=1, mode="promise_in_bounds")

    for s in range(SUBSTEPS):
        src, dst = (field_a, field_b) if s % 2 == 0 else (field_b, field_a)

        def advance(g, to_go, src=src, dst=dst, s=s):
            if s == 0:
                to_go = close_up(g, to_go)
            else:
                behind = jnp.maximum(g - 1, 0) * 4 * per_row
                for u in range(4 * per_row):
                    for t in range(2):
                        v = behind + u
                        moved_a[t, FAR + v] = lanes(dst[t, pad + v], pick.at[t], v)
            for ru in range(4):
                r = jnp.minimum(g, lat_count // 4 - 1) * 4 + ru
                widen = tab[pl.ds(at["widen"] + r, 1), :]
                first = pad + r * per_row
                for t in range(2):
                    west_c, east_c = cw[t] * widen, ce[t] * widen
                    own_c = 1.0 - west_c - east_c - cs[t] - cn[t]
                    e = [src[t, first + q] for q in range(per_row)]
                    right = [pltpu.roll(a, 1, 1) for a in e]
                    left = [pltpu.roll(a, 127, 1) for a in e]
                    for q in range(per_row):
                        west = jnp.where(lane == 0, right[q - 1], right[q])
                        east = jnp.where(lane == 127, left[(q + 1) % per_row], left[q])
                        new = (
                            own_c * e[q] + west_c * west + east_c * east
                            + cs[t] * src[t, first + q - per_row]
                            + cn[t] * src[t, first + q + per_row]
                        )
                        v = first + q - pad
                        if s < SUBSTEPS - 1:
                            dst[t, first + q] = jnp.where(sea_row(v), new, 0.0)
                        else:
                            wind = (speed2d, angle2d)[t][pl.ds(v, 1), :]
                            dst[t, first + q] = jnp.where(row == half, wind, new)
            return to_go

        to_go = lax.fori_loop(0, lat_count // 4 + min(s, 1), advance, to_go)
        if s == 0:
            plan_rows(to_go)

    pl.semaphore_wait(barrier, side * cores + side - 2)
    call_column(column_sem.at[my_y])

    unroll = 8

    def word_of(words, v):
        return jnp.broadcast_to(words[pl.ds(REACH + v, 1), :], (8, 128))

    def has(word, i):
        return jnp.bitwise_and(word, 1 << i) != 0

    def near_rows(words, src, emit, toward_end, bit_order):
        way = 1 if toward_end else -1

        def block(g, carry):
            first = g * unroll
            span = [first + way * u if toward_end else first + unroll - 1 - u for u in range(unroll + 7)]
            for t in range(2):
                word = [word_of(words.at[t], v) for v in span]
                cur = [src[t, FAR + v] for v in span]
                for b in bit_order:
                    d = 1 << b
                    cur = [
                        jnp.where(has(word[u], b), cur[u + d], cur[u])
                        for u in range(len(cur) - d)
                    ]
                for u in range(unroll):
                    emit(t, u, span[u], cur[u])
            return carry

        lax.fori_loop(0, chunks // unroll, block, 0)

    def far_rows(words, src, t, v, way, bit_order):
        def value(v, order):
            if not order:
                return src[t, FAR + v]
            d = way * (1 << order[-1])
            return jnp.where(
                has(word_of(words.at[t], v), order[-1]), value(v + d, order[:-1]), value(v, order[:-1])
            )

        return value(v, bit_order)

    def keep_near(t, u, v, tile):
        moved_b[t, FAR + v] = tile

    near_rows(go_left, moved_a, keep_near, True, (0, 1, 2))

    def pack(g, carry):
        for u in range(unroll):
            v = g * unroll + u
            even, odd = (far_rows(go_left, moved_b, t, v, 1, (3, 4, 5)) for t in range(2))
            send[2 * v] = jnp.where(low, even, odd)
            send[2 * v + 1] = jnp.where(low, odd, even)
        return carry

    lax.fori_loop(0, n * SEA_DEV // 128 // unroll, pack, 0)


    def exchange(visit, src, dst, rows, k, arrival):
        def push(to):
            pltpu.make_async_remote_copy(
                src_ref=src.at[to, pl.ds(0, rows)],
                dst_ref=dst.at[me, pl.ds(0, rows)],
                send_sem=send_sem.at[k],
                recv_sem=arrival,
                device_id={"spec": to},
                device_id_type=MESH,
            ).start()

        visit(push)
        pltpu.make_async_copy(src.at[me, pl.ds(0, rows)], dst.at[me, pl.ds(0, rows)], arrival).start()

    def finish(ref, count, rows, sem):
        part = ref.at[pl.ds(0, count), pl.ds(0, rows)]
        pltpu.make_async_copy(part, part, sem).wait()

    exchange(peers_by_row, send, recv, half, 0, recv_sem.at[my_x])

    wind = send[me][half : half + 1, :]
    other = pltpu.roll(wind, SEA_DEV, 1)
    odd_side = lax.rem(me, 2) * SEA_DEV
    even_half = lambda shape: jnp.bitwise_xor(lax.broadcasted_iota(jnp.int32, shape, 1), odd_side) < SEA_DEV
    low16 = even_half((PAIRS, 128))
    speed = jnp.where(even_half((1, 128)), wind, other)
    angle = jnp.where(even_half((1, 128)), other, wind)

    def paired(name):
        rows = tab[at[name] : at[name] + PAIRS, :]
        return jnp.where(odd_side == 0, rows, pltpu.roll(rows, SEA_DEV, 1))

    toward = speed * (paired("pair_cos") * jnp.cos(angle) + paired("pair_sin") * jnp.sin(angle))
    zero16 = jnp.zeros((PAIRS, 128), jnp.float32)
    for w in range(4):
        for k in (0, 1, 2, NF + 3, NF + 4):
            rolled[w, k] = zero16
    for k in range(2):
        low_part[k] = zero16
    for k in range(3):
        high_part[NF + k] = zero16

    def turns(a, amounts):
        s = pltpu.roll(a, SEA_DEV, 1)
        need = {1: (1, 0), -1: (0, -1), 3: (2, 1), -3: (-1, -2)}
        by = {0: s}
        for m in amounts:
            for w in need[m]:
                if w not in by:
                    by[w] = pltpu.roll(s, w % PAIRS, 0)
        return [jnp.where(low16, by[need[m][0]], by[need[m][1]]) for m in amounts]

    group = 8
    per_group = half * group // PAIRS

    def arrange(i, carry):
        m0, m1 = carry
        h = lax.rem(my_x + hop(i), side)
        finish(recv, side * cores, half, recv_sem.at[h])
        for g in (2 * h, 2 * h + 1):
            for i in range(group):
                flat[g, half * i : half * i + half, :] = recv[g * group + i, 0:half, :]
        for g in (2 * h, 2 * h + 1):
            for q in range(per_group):
                k = g * per_group + q
                a = flat[g, PAIRS * q : PAIRS * (q + 1), :]
                energy[k] = a
                m0 = m0 + a
                m1 = m1 + tab[pl.ds(at["omega"] + k, 1), :] * a
                for w, b in enumerate(turns(a, (1, -1, 3, -3))):
                    rolled[w, k + 3] = b
        return m0, m1

    m0, m1 = lax.fori_loop(0, side, arrange, (zero16, zero16))

    def over_bins(a):
        a = jnp.sum(a, axis=0, keepdims=True)
        return (a + pltpu.roll(a, SEA_DEV, 1)) * (1.0 / (NF * ND))

    m0, m1 = over_bins(m0), over_bins(m1)
    mean_freq = m1 / (m0 + 1e-6)
    steep = m0 * mean_freq * mean_freq
    breaking = steep * steep / (1.0 + steep * steep)

    def transfer(g, carry):
        for q in range(2 * per_group):
            k = g * 2 * per_group + q
            a = energy[k]
            factor = tab[pl.ds(at["rate"] + k, 1), :] * a
            rates = []
            for plus, minus in ((rolled[1, k + 5], rolled[2, k]), (rolled[0, k + 5], rolled[3, k])):
                rates.append(factor * (a * (plus + minus) - 2.0 * plus * minus))
            up, down = turns(rates[0], (1, -3)), turns(rates[1], (-1, 3))
            own[k] = -2.0 * (rates[0] + rates[1])
            low_part[k + 2] = up[0] + down[0]
            high_part[k] = up[1] + down[1]
        return carry

    lax.fori_loop(0, n // group // 2, transfer, 0)

    def renew(g, total):
        for q in range(per_group):
            k = g * per_group + q
            a = energy[k]
            omega = tab[pl.ds(at["omega"] + k, 1), :]
            gain = (0.05 * omega) * jnp.maximum(0.0, omega * toward - 1.0)
            new = a + (gain - (0.03 * omega) * breaking) * a
            new = new + own[k] + low_part[k] + high_part[k + 3]
            total = total + new
            flat[g, PAIRS * q : PAIRS * (q + 1), :] = new
        for i in range(group):
            back[g * group + i, 0:half, :] = flat[g, half * i : half * i + half, :]
        return total

    total = lax.fori_loop(0, n // group, renew, zero16)
    height = 4.0 * jnp.sqrt(over_bins(total) + 1e-6)

    def add_height(g, carry):
        for i in range(group):
            back[g * group + i, half : half + 1, :] = height
        return carry

    lax.fori_loop(0, n // group, add_height, 0)

    exchange(peers, back, home, half + 1, 1, recv_sem.at[side])
    finish(send, n - 1, half, send_sem.at[0])
    finish(home, n, half + 1, recv_sem.at[side])

    def unpack(g, carry):
        for u in range(2 * unroll):
            v = g * 2 * unroll + u
            a, b = home[2 * v], home[2 * v + 1]
            moved_a[0, FAR + v] = jnp.where(low, a, b)
            moved_a[1, FAR + v] = jnp.where(low, b, a)
        return carry

    lax.fori_loop(0, n * SEA_DEV // 128 // (2 * unroll), unpack, 0)

    def spread(g, carry):
        for u in range(4):
            v = g * 4 + u
            for t in range(2):
                moved_b[t, FAR + v] = far_rows(go_right, moved_a, t, v, -1, (5, 4, 3))
        return carry

    lax.fori_loop(0, chunks // 4, spread, 0)

    def keep_apart(t, u, v, tile):
        moved_a[t, FAR + v] = tile

    near_rows(go_right, moved_b, keep_apart, False, (2, 1, 0))

    def deliver(g, carry):
        for u in range(2 * unroll):
            v = g * 2 * unroll + u
            sea = jnp.broadcast_to(sea_row(v), (8, 128))
            for t in range(2):
                tile = jnp.where(sea, lanes(moved_a[t, FAR + v], put.at[t], v), 0.0)
                stage[u, pl.ds(t, half, stride=2), :] = tile[0:half]
                if t == 0:
                    heights[pl.ds(v, 1), :] = tile[half : half + 1]
        for u in range(2 * unroll):
            v = g * 2 * unroll + u
            out[:, pl.ds(pl.multiple_of(v * 128, 128), 128)] = stage[u, 0:bins_dev, :]
        return carry

    lax.fori_loop(0, chunks // (2 * unroll), deliver, 0)

    points = cells // n
    together = NLON // points
    start = me // together * per_row
    three = [heights[pl.ds(start + q, 1), :] for q in range(per_row)]
    u = lax.rem(me, together)
    picked = None
    for g in range(together):
        first, offset = g * points // 128, g * points % 128
        piece = three[first]
        if offset:
            after = three[min(first + 1, per_row - 1)]
            piece = jnp.where(
                lane[0:1] < 128 - offset,
                pltpu.roll(piece, 128 - offset, 1),
                pltpu.roll(after, 128 - offset, 1),
            )
        picked = piece if picked is None else jnp.where(u == g, piece, picked)
    height_out[...] = picked[:, 0:points]
    all_heights = jnp.sum(heights[...], axis=0, keepdims=True)
    mean_out[...] = jnp.sum(all_heights, axis=1, keepdims=True) * (1.0 / (SEA_DEV * n))
    finish(back, n - 1, half + 1, send_sem.at[1])


def solution(mesh):
    n = mesh.shape["spec"]
    cores = 2
    side = math.isqrt(n // cores)

    def local(spectrum, sea_mask, wind_speed, wind_angle):
        bins_dev, cells = spectrum.shape
        chunks = cells // 128
        padded = chunks + 2 * (NLON // 128)
        tab, at = tables(cells // NLON)
        vmem = pl.BlockSpec(memory_space=pltpu.VMEM)
        words = pltpu.VMEM((2, chunks + 2 * REACH, 128), jnp.int32)
        by_freq = lambda *dims: pltpu.VMEM((*dims, PAIRS, 128), jnp.float32)
        messages = lambda count: pltpu.VMEM((count, 8, 128), jnp.float32)
        new_spectrum, height, mean = pl.pallas_call(
            functools.partial(step_kernel, n, side, cores, at),
            name="wave_step",
            out_shape=(
                jax.ShapeDtypeStruct((bins_dev, cells), jnp.float32),
                jax.ShapeDtypeStruct((1, cells // n), jnp.float32),
                jax.ShapeDtypeStruct((1, 1), jnp.float32),
            ),
            in_specs=[pl.BlockSpec(memory_space=pl.ANY)] * 5,
            out_specs=(vmem,) * 3,
            scratch_shapes=[
                pltpu.VMEM((bins_dev, cells), jnp.float32),
                pltpu.VMEM((chunks, 128), jnp.int32),
                pltpu.VMEM((chunks, 128), jnp.float32),
                pltpu.VMEM((chunks, 128), jnp.float32),
                pltpu.VMEM(tab.shape, jnp.float32),
                pltpu.VMEM((2, padded, 8, 128), jnp.float32),
                pltpu.VMEM((2, padded, 8, 128), jnp.float32),
                pltpu.VMEM((16, 16, 128), jnp.float32),
                pltpu.VMEM((chunks + REACH, 128), jnp.int32),
                words,
                words,
                pltpu.VMEM((2, chunks, 128), jnp.int32),
                pltpu.VMEM((2, chunks, 128), jnp.int32),
                pltpu.VMEM((2, chunks + 2 * FAR, 8, 128), jnp.float32),
                pltpu.VMEM((2, chunks + 2 * FAR, 8, 128), jnp.float32),
                messages(n),
                messages(n),
                messages(n),
                messages(n),
                pltpu.VMEM((n // 8, 8 * bins_dev // 2, 128), jnp.float32),
                by_freq(NF),
                by_freq(4, NF + 5),
                by_freq(NF),
                by_freq(NF + 2),
                by_freq(NF + 3),
                pltpu.VMEM((chunks, 128), jnp.float32),
                pltpu.SemaphoreType.DMA((2,)),
                pltpu.SemaphoreType.DMA((side + 1,)),
                pltpu.SemaphoreType.DMA((8,)),
                pltpu.SemaphoreType.REGULAR((side,)),
            ],
            compiler_params=pltpu.CompilerParams(collective_id=0, has_side_effects=True),
        )(
            spectrum,
            sea_mask.reshape(chunks, 128),
            wind_speed.reshape(chunks, 128),
            wind_angle.reshape(chunks, 128),
            tab,
        )
        return new_spectrum, height.reshape(-1), mean.reshape(1)

    return jax.shard_map(
        local,
        mesh=mesh,
        in_specs=(P(("grp", "spec"), None), P(), P("grp"), P("grp")),
        out_specs=(P(("grp", "spec"), None), P(("grp", "spec")), P("grp")),
        check_vma=False,
    )
```

```python
import functools
import math

import jax
import jax.numpy as jnp
import numpy as np
from jax import lax
from jax.experimental import pallas as pl
from jax.experimental.pallas import tpu as pltpu
from jax.sharding import PartitionSpec as P

NF = 48
ND = 32
NLON = 384
SUBSTEPS = 2
SEA_DEV = 64
MESH = pl.DeviceIdType.MESH
LOG_RATIO = math.log(1.1)
PAIRS = ND // 2
ROW_STEPS = 6
REACH = 32
UNROLL = 8
VMEM_BYTES = 24 * 1024 * 1024
FAR = 56


def tables(lat_count):
    heading = 2.0 * np.pi * (np.arange(ND) + 0.5) / ND
    wrapped = np.concatenate([heading, heading[:24]])
    flat = lambda a: np.repeat(np.asarray(a)[:, None], 128, 1)
    paired = np.repeat(heading.reshape(PAIRS, 2), SEA_DEV, axis=1)
    latitude = np.radians(-75.0 + 150.0 * (np.arange(lat_count) + 0.5) / lat_count)
    k = np.arange(NF)
    rows, at = [], {}
    for name, block in (
        ("cos", flat(np.cos(wrapped))),
        ("sin", flat(np.sin(wrapped))),
        ("pair_cos", np.cos(paired)),
        ("pair_sin", np.sin(paired)),
        ("widen", flat(1.0 / np.cos(latitude))),
        ("omega", flat(np.exp(LOG_RATIO * (k - NF // 2)))),
        ("rate", flat(np.where((k >= 3) & (k <= NF - 3), 0.001, 0.0))),
    ):
        at[name] = sum(len(r) for r in rows)
        rows.append(block)
    return np.concatenate(rows).astype(np.float32), at


def word_of(words, v):
    return jnp.broadcast_to(words[pl.ds(REACH + v, 1), :], (8, 128))


def has(word, i):
    return jnp.bitwise_and(word, 1 << i) != 0


def lanes(tile, index, v):
    index = jnp.broadcast_to(index[pl.ds(v, 1), :], (8, 128))
    return jnp.take_along_axis(tile, index, axis=1, mode="promise_in_bounds")


def near_rows(chunks, words, src, emit, toward_end, bit_order):
    way = 1 if toward_end else -1

    def block(g, carry):
        first = g * UNROLL
        span = [first + way * u if toward_end else first + UNROLL - 1 - u for u in range(UNROLL + 7)]
        for t in range(2):
            word = [word_of(words.at[t], v) for v in span]
            cur = [src[t, FAR + v] for v in span]
            for b in bit_order:
                d = 1 << b
                cur = [
                    jnp.where(has(word[u], b), cur[u + d], cur[u])
                    for u in range(len(cur) - d)
                ]
            for u in range(UNROLL):
                emit(t, u, span[u], cur[u])
        return carry

    lax.fori_loop(0, chunks // UNROLL, block, 0)


def far_rows(words, src, t, v, way, bit_order):
    def value(v, order):
        if not order:
            return src[t, FAR + v]
        d = way * (1 << order[-1])
        return jnp.where(
            has(word_of(words.at[t], v), order[-1]), value(v + d, order[:-1]), value(v, order[:-1])
        )

    return value(v, bit_order)


def step_kernel(
    n, side, cores, at,
    x_hbm, mask_hbm, speed_hbm, angle_hbm, tab_hbm,
    home, go_right, put,
    x, mask2d, speed2d, angle2d, tab, field_a, field_b, stage, shifts, go_left, pick, moved_a, moved_b,
    send, recv, back, flat, energy, rolled, own, low_part, high_part,
    send_sem, recv_sem, load_sem, column_sem,
):
    bins_dev, cells = x.shape
    half = bins_dev // 2
    chunks = cells // 128
    per_row = NLON // 128
    lat_count = cells // NLON
    me = lax.axis_index("spec")
    my_x, my_y, my_c = me // (side * cores), lax.rem(me // cores, side), lax.rem(me, cores)

    parts = 4
    part_cols = cells // parts
    small = [
        pltpu.make_async_copy(src, dst, load_sem.at[parts + k])
        for k, (src, dst) in enumerate(
            ((mask_hbm, mask2d), (tab_hbm, tab), (speed_hbm, speed2d), (angle_hbm, angle2d))
        )
    ]

    def load(part):
        cols = pl.ds(pl.multiple_of(part * part_cols, 128), part_cols)
        return pltpu.make_async_copy(x_hbm.at[:, cols], x.at[:, cols], load_sem.at[part])

    small[0].start()
    for part in range(parts):
        load(part).start()
    for copy in small[1:]:
        copy.start()

    def hop(u):
        return side // 2 + jnp.where(lax.rem(u, 2) == 0, u // 2, -((u + 1) // 2))

    def both_cores(act, px, py):
        first = (px * side + py) * cores
        act(first + my_c)
        for c in range(1, cores):
            act(first + lax.rem(my_c + c, cores))

    def own_chip(act):
        for c in range(1, cores):
            act(me - my_c + lax.rem(my_c + c, cores))

    def peers(act):
        def diagonal(s, carry):
            def one(u, inner):
                both_cores(act, lax.rem(my_x + hop(u), side), lax.rem(my_y + hop(s - u), side))
                return inner

            return lax.fori_loop(jnp.maximum(0, s - side + 1), jnp.minimum(side - 1, s) + 1, one, carry)

        lax.fori_loop(0, 2 * side - 2, diagonal, 0)
        own_chip(act)

    def peers_by_row(act):
        def row_of(py, count):
            def one(u, inner):
                both_cores(act, lax.rem(my_x + hop(u), side), py)
                return inner

            lax.fori_loop(0, count, one, 0)

        def far_row(i, carry):
            py = lax.rem(my_y + hop(i), side)

            @pl.when(py != 0)
            def _():
                pl.semaphore_wait(column_sem.at[py], 1)
                row_of(py, side)

            return carry

        lax.fori_loop(0, side - 1, far_row, 0)
        row_of(my_y, side - 1)
        own_chip(act)

        @pl.when(my_y != 0)
        def _():
            pl.semaphore_wait(column_sem.at[0], 1)
            row_of(0, side)


    barrier = pltpu.get_barrier_semaphore()

    def call_row(i, carry):
        to = (lax.rem(my_x + i // cores, side) * side + my_y) * cores + lax.rem(my_c + lax.rem(i, cores), cores)
        pl.semaphore_signal(barrier, inc=1, device_id={"spec": to}, device_id_type=MESH)
        return carry

    def call_column(semaphore):
        def one(i, carry):
            to = (my_x * side + lax.rem(my_y + i, side)) * cores + my_c
            pl.semaphore_signal(semaphore, inc=1, device_id={"spec": to}, device_id_type=MESH)
            return carry

        lax.fori_loop(1, side, one, 0)

    lax.fori_loop(1, side * cores, call_row, 0)
    call_column(barrier)
    small[0].wait()

    lane = lax.broadcasted_iota(jnp.int32, (8, 128), 1)
    row = lax.broadcasted_iota(jnp.int32, (8, 128), 0)
    low = lane < SEA_DEV

    is_sea = mask2d[...] != 0
    land = jnp.where(is_sea, 0.0, 1.0).astype(jnp.bfloat16)
    earlier = (
        lax.broadcasted_iota(jnp.int32, (128, 128), 0) < lax.broadcasted_iota(jnp.int32, (128, 128), 1)
    ).astype(jnp.bfloat16)
    above = (
        lax.broadcasted_iota(jnp.int32, (chunks, chunks), 1)
        < lax.broadcasted_iota(jnp.int32, (chunks, chunks), 0)
    ).astype(jnp.bfloat16)
    ones = jnp.ones((128, 128), jnp.bfloat16)
    count = functools.partial(jnp.dot, preferred_element_type=jnp.float32)
    before = count(land, earlier).astype(jnp.int32)
    sea_in_row = 128 - count(land, ones).astype(jnp.int32)
    wide_lane = lax.broadcasted_iota(jnp.int32, (chunks, 128), 1)
    wide_row = lax.broadcasted_iota(jnp.int32, (chunks, 128), 0)
    rank0 = wide_row * 128 - count(count(above, land).astype(jnp.bfloat16), ones).astype(jnp.int32)
    put[0] = jnp.bitwise_and(rank0 + wide_lane - before, 127)
    put[1] = jnp.bitwise_and(rank0 + wide_lane - before + SEA_DEV, 127)
    to_go = jnp.where(is_sea, before, 0)
    shifts[chunks:, :] = jnp.zeros((shifts.shape[0] - chunks, 128), jnp.int32)
    go_left[...] = jnp.zeros_like(go_left)
    go_right[...] = jnp.zeros_like(go_right)

    def close_up(i, to_go):
        d = jnp.left_shift(1, i)
        incoming = pltpu.roll(to_go, 128 - d, 1)
        stay = jnp.where(jnp.bitwise_and(to_go, d) != 0, 0, to_go)
        return jnp.where(jnp.bitwise_and(incoming, d) != 0, incoming, stay)

    def plan_rows(to_go):
        nth = jnp.bitwise_and(wide_lane - rank0, 127)
        front = jnp.bitwise_and(wide_lane + to_go, 127)
        took = jnp.take_along_axis(front, nth, axis=1, mode="promise_in_bounds")
        pick[0] = took
        pick[1] = pltpu.roll(took, SEA_DEV, 1)
        up = wide_row - jnp.right_shift(rank0 + nth, 7)
        shifts[0:chunks, :] = jnp.where(nth < sea_in_row, up, 0)
        for b in range(ROW_STEPS):
            here, incoming = shifts[0:chunks, :], shifts[1 << b : chunks + (1 << b), :]
            goes = jnp.bitwise_and(here, 1 << b)
            comes = jnp.bitwise_and(incoming, 1 << b)
            rights, lefts = (goes, comes) if b == 0 else (rights + goes, lefts + comes)
            shifts[0:chunks, :] = jnp.where(comes != 0, incoming, jnp.where(goes != 0, 0, here))
        for words, found in ((go_right, rights), (go_left, lefts)):
            words[0, REACH : REACH + chunks, :] = found
            words[1, REACH : REACH + chunks, :] = pltpu.roll(found, SEA_DEV, 1)

    zero = jnp.zeros((8, 128), jnp.float32)
    pad = per_row
    for t in range(2):
        for v in range(pad):
            for f in (field_a, field_b):
                f[t, v] = zero
                f[t, pad + chunks + v] = zero
    base = (me * bins_dev) % ND
    for copy in small[1:]:
        copy.wait()
    cw, ce, cs, cn = [], [], [], []
    for t in range(2):
        k = ((me * bins_dev + jnp.minimum(2 * row + t, bins_dev - 1)) // ND).astype(jnp.float32)
        pace = 0.2 * jnp.exp(-LOG_RATIO * k)
        ax = pace * tab[pl.ds(at["cos"] + base + t, 8, stride=2), :]
        ay = pace * tab[pl.ds(at["sin"] + base + t, 8, stride=2), :]
        cw.append(jnp.maximum(ax, 0.0))
        ce.append(-jnp.minimum(ax, 0.0))
        cs.append(jnp.maximum(ay, 0.0))
        cn.append(-jnp.minimum(ay, 0.0))

    def sea_row(v):
        return mask2d[pl.ds(v, 1), :] != 0

    def split_bins(g, carry):
        for u in range(8):
            v = g * 8 + u
            cols = pl.ds(pl.multiple_of(v * 128, 128), 128)
            stage[u, 0:bins_dev, :] = jnp.where(sea_row(v), x[:, cols], 0.0)
            for t in range(2):
                field_a[t, pad + v, 0:half, :] = stage[u, pl.ds(t, half, stride=2), :]
        return carry

    def split_part(part, carry):
        load(part).wait()
        per_part = chunks // 8 // parts
        return lax.fori_loop(part * per_part, (part + 1) * per_part, split_bins, carry)

    lax.fori_loop(0, parts, split_part, 0)

    for s in range(SUBSTEPS):
        src, dst = (field_a, field_b) if s % 2 == 0 else (field_b, field_a)

        def advance(g, to_go, src=src, dst=dst, s=s):
            if s == 0:
                to_go = close_up(g, to_go)
            else:
                behind = jnp.maximum(g - 1, 0) * 4 * per_row
                for u in range(4 * per_row):
                    for t in range(2):
                        v = behind + u
                        moved_a[t, FAR + v] = lanes(dst[t, pad + v], pick.at[t], v)
            for ru in range(4):
                r = jnp.minimum(g, lat_count // 4 - 1) * 4 + ru
                widen = tab[pl.ds(at["widen"] + r, 1), :]
                first = pad + r * per_row
                for t in range(2):
                    west_c, east_c = cw[t] * widen, ce[t] * widen
                    own_c = 1.0 - west_c - east_c - cs[t] - cn[t]
                    e = [src[t, first + q] for q in range(per_row)]
                    right = [pltpu.roll(a, 1, 1) for a in e]
                    left = [pltpu.roll(a, 127, 1) for a in e]
                    for q in range(per_row):
                        west = jnp.where(lane == 0, right[q - 1], right[q])
                        east = jnp.where(lane == 127, left[(q + 1) % per_row], left[q])
                        new = (
                            own_c * e[q] + west_c * west + east_c * east
                            + cs[t] * src[t, first + q - per_row]
                            + cn[t] * src[t, first + q + per_row]
                        )
                        v = first + q - pad
                        if s < SUBSTEPS - 1:
                            dst[t, first + q] = jnp.where(sea_row(v), new, 0.0)
                        else:
                            wind = (speed2d, angle2d)[t][pl.ds(v, 1), :]
                            dst[t, first + q] = jnp.where(row == half, wind, new)
            return to_go

        to_go = lax.fori_loop(0, lat_count // 4 + min(s, 1), advance, to_go)
        if s == 0:
            plan_rows(to_go)

    pl.semaphore_wait(barrier, side * cores + side - 2)
    call_column(column_sem.at[my_y])


    def keep_near(t, u, v, tile):
        moved_b[t, FAR + v] = tile

    near_rows(chunks, go_left, moved_a, keep_near, True, (0, 1, 2))

    def pack(g, carry):
        for u in range(UNROLL):
            v = g * UNROLL + u
            even, odd = (far_rows(go_left, moved_b, t, v, 1, (3, 4, 5)) for t in range(2))
            send[2 * v] = jnp.where(low, even, odd)
            send[2 * v + 1] = jnp.where(low, odd, even)
        return carry

    lax.fori_loop(0, n * SEA_DEV // 128 // UNROLL, pack, 0)


    def exchange(visit, src, dst, rows, k, arrival):
        def push(to):
            pltpu.make_async_remote_copy(
                src_ref=src.at[to, pl.ds(0, rows)],
                dst_ref=dst.at[me, pl.ds(0, rows)],
                send_sem=send_sem.at[k],
                recv_sem=arrival,
                device_id={"spec": to},
                device_id_type=MESH,
            ).start()

        visit(push)
        pltpu.make_async_copy(src.at[me, pl.ds(0, rows)], dst.at[me, pl.ds(0, rows)], arrival).start()

    def finish(ref, count, rows, sem):
        part = ref.at[pl.ds(0, count), pl.ds(0, rows)]
        pltpu.make_async_copy(part, part, sem).wait()

    exchange(peers_by_row, send, recv, half, 0, recv_sem.at[my_x])

    wind = send[me][half : half + 1, :]
    other = pltpu.roll(wind, SEA_DEV, 1)
    odd_side = lax.rem(me, 2) * SEA_DEV
    even_half = lambda shape: jnp.bitwise_xor(lax.broadcasted_iota(jnp.int32, shape, 1), odd_side) < SEA_DEV
    low16 = even_half((PAIRS, 128))
    speed = jnp.where(even_half((1, 128)), wind, other)
    angle = jnp.where(even_half((1, 128)), other, wind)

    def paired(name):
        rows = tab[at[name] : at[name] + PAIRS, :]
        return jnp.where(odd_side == 0, rows, pltpu.roll(rows, SEA_DEV, 1))

    toward = speed * (paired("pair_cos") * jnp.cos(angle) + paired("pair_sin") * jnp.sin(angle))
    zero16 = jnp.zeros((PAIRS, 128), jnp.float32)
    for w in range(4):
        for k in (0, 1, 2, NF + 3, NF + 4):
            rolled[w, k] = zero16
    for k in range(2):
        low_part[k] = zero16
    for k in range(3):
        high_part[NF + k] = zero16

    def turns(a, amounts):
        s = pltpu.roll(a, SEA_DEV, 1)
        need = {1: (1, 0), -1: (0, -1), 3: (2, 1), -3: (-1, -2)}
        by = {0: s}
        for m in amounts:
            for w in need[m]:
                if w not in by:
                    by[w] = pltpu.roll(s, w % PAIRS, 0)
        return [jnp.where(low16, by[need[m][0]], by[need[m][1]]) for m in amounts]

    group = 8
    per_group = half * group // PAIRS

    def arrange(i, carry):
        m0, m1 = carry
        h = lax.rem(my_x + hop(i), side)
        finish(recv, side * cores, half, recv_sem.at[h])
        for g in (2 * h, 2 * h + 1):
            for i in range(group):
                flat[g, half * i : half * i + half, :] = recv[g * group + i, 0:half, :]
        for g in (2 * h, 2 * h + 1):
            for q in range(per_group):
                k = g * per_group + q
                a = flat[g, PAIRS * q : PAIRS * (q + 1), :]
                energy[k] = a
                m0 = m0 + a
                m1 = m1 + tab[pl.ds(at["omega"] + k, 1), :] * a
                for w, b in enumerate(turns(a, (1, -1, 3, -3))):
                    rolled[w, k + 3] = b
        return m0, m1

    m0, m1 = lax.fori_loop(0, side, arrange, (zero16, zero16))

    def over_bins(a):
        a = jnp.sum(a, axis=0, keepdims=True)
        return (a + pltpu.roll(a, SEA_DEV, 1)) * (1.0 / (NF * ND))

    m0, m1 = over_bins(m0), over_bins(m1)
    mean_freq = m1 / (m0 + 1e-6)
    steep = m0 * mean_freq * mean_freq
    breaking = steep * steep / (1.0 + steep * steep)

    def transfer(g, carry):
        for q in range(2 * per_group):
            k = g * 2 * per_group + q
            a = energy[k]
            factor = tab[pl.ds(at["rate"] + k, 1), :] * a
            rates = []
            for plus, minus in ((rolled[1, k + 5], rolled[2, k]), (rolled[0, k + 5], rolled[3, k])):
                rates.append(factor * (a * (plus + minus) - 2.0 * plus * minus))
            up, down = turns(rates[0], (1, -3)), turns(rates[1], (-1, 3))
            own[k] = -2.0 * (rates[0] + rates[1])
            low_part[k + 2] = up[0] + down[0]
            high_part[k] = up[1] + down[1]
        return carry

    lax.fori_loop(0, n // group // 2, transfer, 0)

    def renew(g, total):
        for q in range(per_group):
            k = g * per_group + q
            a = energy[k]
            omega = tab[pl.ds(at["omega"] + k, 1), :]
            gain = (0.05 * omega) * jnp.maximum(0.0, omega * toward - 1.0)
            new = a + (gain - (0.03 * omega) * breaking) * a
            new = new + own[k] + low_part[k] + high_part[k + 3]
            total = total + new
            flat[g, PAIRS * q : PAIRS * (q + 1), :] = new
        for i in range(group):
            back[g * group + i, 0:half, :] = flat[g, half * i : half * i + half, :]
        return total

    total = lax.fori_loop(0, n // group, renew, zero16)
    height = 4.0 * jnp.sqrt(over_bins(total) + 1e-6)

    def add_height(g, carry):
        for i in range(group):
            back[g * group + i, half : half + 1, :] = height
        return carry

    lax.fori_loop(0, n // group, add_height, 0)

    exchange(peers, back, home, half + 1, 1, recv_sem.at[side])
    finish(send, n - 1, half, send_sem.at[0])
    finish(home, n, half + 1, recv_sem.at[side])
    finish(back, n - 1, half + 1, send_sem.at[1])


def unpack_kernel(
    n, bins_dev,
    home, go_right, put, mask2d,
    out, height_out, mean_out,
    moved_a, moved_b, stage, heights,
):
    chunks = mask2d.shape[0]
    half = bins_dev // 2
    cells = chunks * 128
    per_row = NLON // 128
    me = lax.axis_index("spec")
    lane = lax.broadcasted_iota(jnp.int32, (8, 128), 1)
    low = lane < SEA_DEV

    def unpack(g, carry):
        for u in range(2 * UNROLL):
            v = g * 2 * UNROLL + u
            a, b = home[2 * v], home[2 * v + 1]
            moved_a[0, FAR + v] = jnp.where(low, a, b)
            moved_a[1, FAR + v] = jnp.where(low, b, a)
        return carry

    lax.fori_loop(0, n * SEA_DEV // 128 // (2 * UNROLL), unpack, 0)

    def spread(g, carry):
        for u in range(4):
            v = g * 4 + u
            for t in range(2):
                moved_b[t, FAR + v] = far_rows(go_right, moved_a, t, v, -1, (5, 4, 3))
        return carry

    lax.fori_loop(0, chunks // 4, spread, 0)

    def keep_apart(t, u, v, tile):
        moved_a[t, FAR + v] = tile

    near_rows(chunks, go_right, moved_b, keep_apart, False, (2, 1, 0))

    def deliver(g, carry):
        for u in range(2 * UNROLL):
            v = g * 2 * UNROLL + u
            sea = jnp.broadcast_to(mask2d[pl.ds(v, 1), :] != 0, (8, 128))
            for t in range(2):
                tile = jnp.where(sea, lanes(moved_a[t, FAR + v], put.at[t], v), 0.0)
                stage[u, pl.ds(t, half, stride=2), :] = tile[0:half]
                if t == 0:
                    heights[pl.ds(v, 1), :] = tile[half : half + 1]
        for u in range(2 * UNROLL):
            v = g * 2 * UNROLL + u
            out[:, pl.ds(pl.multiple_of(v * 128, 128), 128)] = stage[u, 0:bins_dev, :]
        return carry

    lax.fori_loop(0, chunks // (2 * UNROLL), deliver, 0)

    points = cells // n
    together = NLON // points
    start = me // together * per_row
    three = [heights[pl.ds(start + q, 1), :] for q in range(per_row)]
    u = lax.rem(me, together)
    picked = None
    for g in range(together):
        first, offset = g * points // 128, g * points % 128
        piece = three[first]
        if offset:
            after = three[min(first + 1, per_row - 1)]
            piece = jnp.where(
                lane[0:1] < 128 - offset,
                pltpu.roll(piece, 128 - offset, 1),
                pltpu.roll(after, 128 - offset, 1),
            )
        picked = piece if picked is None else jnp.where(u == g, piece, picked)
    height_out[...] = picked[:, 0:points]
    all_heights = jnp.sum(heights[...], axis=0, keepdims=True)
    mean_out[...] = jnp.sum(all_heights, axis=1, keepdims=True) * (1.0 / (SEA_DEV * n))


def solution(mesh):
    n = mesh.shape["spec"]
    cores = 2
    side = math.isqrt(n // cores)

    def local(spectrum, sea_mask, wind_speed, wind_angle):
        bins_dev, cells = spectrum.shape
        chunks = cells // 128
        padded = chunks + 2 * (NLON // 128)
        tab, at = tables(cells // NLON)
        vmem = pl.BlockSpec(memory_space=pltpu.VMEM)
        words = pltpu.VMEM((2, chunks + 2 * REACH, 128), jnp.int32)
        by_freq = lambda *dims: pltpu.VMEM((*dims, PAIRS, 128), jnp.float32)
        messages = lambda count: pltpu.VMEM((count, 8, 128), jnp.float32)
        home, go_right, put = pl.pallas_call(
            functools.partial(step_kernel, n, side, cores, at),
            name="wave_step",
            out_shape=(
                jax.ShapeDtypeStruct((n, 8, 128), jnp.float32),
                jax.ShapeDtypeStruct((2, chunks + 2 * REACH, 128), jnp.int32),
                jax.ShapeDtypeStruct((2, chunks, 128), jnp.int32),
            ),
            in_specs=[pl.BlockSpec(memory_space=pltpu.HBM)] * 5,
            out_specs=(vmem,) * 3,
            scratch_shapes=[
                pltpu.VMEM((bins_dev, cells), jnp.float32),
                pltpu.VMEM((chunks, 128), jnp.int32),
                pltpu.VMEM((chunks, 128), jnp.float32),
                pltpu.VMEM((chunks, 128), jnp.float32),
                pltpu.VMEM(tab.shape, jnp.float32),
                pltpu.VMEM((2, padded, 8, 128), jnp.float32),
                pltpu.VMEM((2, padded, 8, 128), jnp.float32),
                pltpu.VMEM((8, 16, 128), jnp.float32),
                pltpu.VMEM((chunks + REACH, 128), jnp.int32),
                words,
                pltpu.VMEM((2, chunks, 128), jnp.int32),
                pltpu.VMEM((2, chunks + 2 * FAR, 8, 128), jnp.float32),
                pltpu.VMEM((2, chunks + 2 * FAR, 8, 128), jnp.float32),
                messages(n),
                messages(n),
                messages(n),
                pltpu.VMEM((n // 8, 8 * bins_dev // 2, 128), jnp.float32),
                by_freq(NF),
                by_freq(4, NF + 5),
                by_freq(NF),
                by_freq(NF + 2),
                by_freq(NF + 3),
                pltpu.SemaphoreType.DMA((2,)),
                pltpu.SemaphoreType.DMA((side + 1,)),
                pltpu.SemaphoreType.DMA((8,)),
                pltpu.SemaphoreType.REGULAR((side,)),
            ],
            compiler_params=pltpu.CompilerParams(
                collective_id=0, has_side_effects=True, vmem_limit_bytes=VMEM_BYTES
            ),
        )(
            *(
                pltpu.with_memory_space_constraint(a, pltpu.HBM)
                for a in (
                    spectrum,
                    sea_mask.reshape(chunks, 128),
                    wind_speed.reshape(chunks, 128),
                    wind_angle.reshape(chunks, 128),
                    jnp.asarray(tab),
                )
            )
        )
        moved = pltpu.VMEM((2, chunks + 2 * FAR, 8, 128), jnp.float32)
        new_spectrum, height, mean = pl.pallas_call(
            functools.partial(unpack_kernel, n, bins_dev),
            name="unpack",
            out_shape=(
                jax.ShapeDtypeStruct((bins_dev, cells), jnp.float32),
                jax.ShapeDtypeStruct((1, cells // n), jnp.float32),
                jax.ShapeDtypeStruct((1, 1), jnp.float32),
            ),
            in_specs=[vmem] * 4,
            out_specs=(vmem,) * 3,
            scratch_shapes=[
                moved,
                moved,
                pltpu.VMEM((16, 16, 128), jnp.float32),
                pltpu.VMEM((chunks, 128), jnp.float32),
            ],
            compiler_params=pltpu.CompilerParams(vmem_limit_bytes=VMEM_BYTES),
        )(home, go_right, put, sea_mask.reshape(chunks, 128))
        return new_spectrum, height.reshape(-1), mean.reshape(1)

    return jax.shard_map(
        local,
        mesh=mesh,
        in_specs=(P(("grp", "spec"), None), P(), P("grp"), P("grp")),
        out_specs=(P(("grp", "spec"), None), P(("grp", "spec")), P("grp")),
        check_vma=False,
    )
```

```python
import functools
import math

import jax
import jax.numpy as jnp
import numpy as np
from jax import lax
from jax.experimental import pallas as pl
from jax.experimental.pallas import tpu as pltpu
from jax.sharding import PartitionSpec as P

NF = 48
ND = 32
NLON = 384
SUBSTEPS = 2
SEA_DEV = 64
MESH = pl.DeviceIdType.MESH
LOG_RATIO = math.log(1.1)
PAIRS = ND // 2
ROW_STEPS = 6
REACH = 32
UNROLL = 8
VMEM_BYTES = 24 * 1024 * 1024
FAR = 56


def tables(lat_count):
    heading = 2.0 * np.pi * (np.arange(ND) + 0.5) / ND
    wrapped = np.concatenate([heading, heading[:24]])
    flat = lambda a: np.repeat(np.asarray(a)[:, None], 128, 1)
    paired = np.repeat(heading.reshape(PAIRS, 2), SEA_DEV, axis=1)
    latitude = np.radians(-75.0 + 150.0 * (np.arange(lat_count) + 0.5) / lat_count)
    k = np.arange(NF)
    rows, at = [], {}
    for name, block in (
        ("cos", flat(np.cos(wrapped))),
        ("sin", flat(np.sin(wrapped))),
        ("pair_cos", np.cos(paired)),
        ("pair_sin", np.sin(paired)),
        ("widen", flat(1.0 / np.cos(latitude))),
        ("omega", flat(np.exp(LOG_RATIO * (k - NF // 2)))),
        ("rate", flat(np.where((k >= 3) & (k <= NF - 3), 0.001, 0.0))),
    ):
        at[name] = sum(len(r) for r in rows)
        rows.append(block)
    return np.concatenate(rows).astype(np.float32), at


def word_of(words, v):
    return jnp.broadcast_to(words[pl.ds(REACH + v, 1), :], (8, 128))


def has(word, i):
    return jnp.bitwise_and(word, 1 << i) != 0


def lanes(tile, index, v):
    index = jnp.broadcast_to(index[pl.ds(v, 1), :], (8, 128))
    return jnp.take_along_axis(tile, index, axis=1, mode="promise_in_bounds")


def near_rows(chunks, words, src, emit, toward_end, bit_order):
    way = 1 if toward_end else -1

    def block(g, carry):
        first = g * UNROLL
        span = [first + way * u if toward_end else first + UNROLL - 1 - u for u in range(UNROLL + 7)]
        for t in range(2):
            word = [word_of(words.at[t], v) for v in span]
            cur = [src[t, FAR + v] for v in span]
            for b in bit_order:
                d = 1 << b
                cur = [
                    jnp.where(has(word[u], b), cur[u + d], cur[u])
                    for u in range(len(cur) - d)
                ]
            for u in range(UNROLL):
                emit(t, u, span[u], cur[u])
        return carry

    lax.fori_loop(0, chunks // UNROLL, block, 0)


def far_rows(words, src, t, v, way, bit_order):
    def value(v, order):
        if not order:
            return src[t, FAR + v]
        d = way * (1 << order[-1])
        return jnp.where(
            has(word_of(words.at[t], v), order[-1]), value(v + d, order[:-1]), value(v, order[:-1])
        )

    return value(v, bit_order)


def step_kernel(
    n, side, cores, at,
    x_hbm, mask_hbm, speed_hbm, angle_hbm, tab_hbm,
    home, go_right, put,
    x, mask2d, sea_float, speed2d, angle2d, tab, field_a, field_b, stage, shifts, go_left, pick, moved_a, moved_b,
    send, recv, back, flat, energy, rolled, own, low_part, high_part,
    send_sem, recv_sem, load_sem, column_sem, first_sem,
):
    bins_dev, cells = x.shape
    half = bins_dev // 2
    chunks = cells // 128
    per_row = NLON // 128
    lat_count = cells // NLON
    me = lax.axis_index("spec")
    my_x, my_y, my_c = me // (side * cores), lax.rem(me // cores, side), lax.rem(me, cores)

    parts = 4
    part_cols = cells // parts
    small = [
        pltpu.make_async_copy(src, dst, load_sem.at[parts + k])
        for k, (src, dst) in enumerate(
            ((mask_hbm, mask2d), (tab_hbm, tab), (speed_hbm, speed2d), (angle_hbm, angle2d))
        )
    ]

    def load(part):
        cols = pl.ds(pl.multiple_of(part * part_cols, 128), part_cols)
        return pltpu.make_async_copy(x_hbm.at[:, cols], x.at[:, cols], load_sem.at[part])

    small[0].start()
    for part in range(parts):
        load(part).start()
    for copy in small[1:]:
        copy.start()

    def wrap(a):
        return jnp.bitwise_and(a, side - 1) if side & (side - 1) == 0 else lax.rem(a, side)

    def hop(u):
        return side // 2 + (1 - 2 * jnp.bitwise_and(u, 1)) * jnp.right_shift(u + 1, 1)

    def both_cores(act, px, py):
        first = (px * side + py) * cores
        act(first + my_c)
        for c in range(1, cores):
            act(first + jnp.where(my_c + c >= cores, my_c + c - cores, my_c + c))

    def own_chip(act):
        for c in range(1, cores):
            act(me - my_c + lax.rem(my_c + c, cores))

    def peers(act, rows=side):
        def diagonal(s, carry):
            def one(u, inner):
                both_cores(act, wrap(my_x + hop(u)), wrap(my_y + hop(s - u)))
                return inner

            return lax.fori_loop(jnp.maximum(0, s - rows + 1), jnp.minimum(side - 1, s) + 1, one, carry)

        lax.fori_loop(0, side + rows - 2 + (rows < side), diagonal, 0)
        if rows == side:
            own_chip(act)

    is_first = me == 0
    below_first = jnp.logical_and(jnp.logical_and(my_x == 0, my_c == 0), my_y != 0)

    def signal(semaphore, to):
        pl.semaphore_signal(semaphore, inc=1, device_id={"spec": to}, device_id_type=MESH)

    def down_column(act):
        def one(u, carry):
            act((my_x * side + wrap(my_y + hop(u))) * cores + my_c)
            return carry

        lax.fori_loop(0, side - 1, one, 0)

    def along_row(act):
        def one(u, carry):
            both_cores(act, wrap(my_x + hop(u)), my_y)
            return carry

        lax.fori_loop(0, side - 1, one, 0)
        own_chip(act)

    def peers_but_late(act):
        def but_first(to):
            @pl.when(to != 0)
            def _():
                act(to)

        along_row(but_first)

        @pl.when(jnp.logical_not(is_first))
        def _():
            def row_in(i, carry):
                pl.semaphore_wait(column_sem.at[wrap(my_y + i)], 1)
                return carry

            @pl.when(jnp.logical_not(below_first))
            def _():
                lax.fori_loop(1, side, row_in, 0)

            @pl.when(me == 1)
            def _():
                down_column(lambda to: signal(column_sem.at[0], to - 1))

            @pl.when(below_first)
            def _():
                lax.fori_loop(1, side, row_in, 0)

        peers(but_first, side - 1)

        @pl.when(jnp.logical_not(is_first))
        def _():
            pl.semaphore_wait(first_sem, 1)

            @pl.when(my_y == 0)
            def _():
                down_column(lambda to: signal(first_sem, to))

            act(0)

    barrier = pltpu.get_barrier_semaphore()

    @pl.when(jnp.logical_not(is_first))
    def _():
        along_row(lambda to: signal(barrier, to))
        down_column(lambda to: signal(barrier, to))

    def entered():
        called = side * cores + side - 2

        @pl.when(is_first)
        def _():
            pl.semaphore_wait(barrier, called + side - 1)
            along_row(lambda to: signal(first_sem, to))
            down_column(lambda to: signal(first_sem, to))

        @pl.when(jnp.logical_not(is_first))
        def _():
            with_first = jnp.logical_or(my_y == 0, below_first)
            pl.semaphore_wait(barrier, called - jnp.where(with_first, 1, 0))

            def complete(to):
                @pl.when(to == 0)
                def _():
                    signal(barrier, to)

                @pl.when(to != 0)
                def _():
                    signal(column_sem.at[my_y], to)

            down_column(complete)

    small[0].wait()

    lane = lax.broadcasted_iota(jnp.int32, (8, 128), 1)
    row = lax.broadcasted_iota(jnp.int32, (8, 128), 0)
    low = lane < SEA_DEV

    is_sea = mask2d[...] != 0
    sea_float[...] = mask2d[...].astype(jnp.float32)
    land = jnp.where(is_sea, 0.0, 1.0).astype(jnp.bfloat16)
    earlier = (
        lax.broadcasted_iota(jnp.int32, (128, 128), 0) < lax.broadcasted_iota(jnp.int32, (128, 128), 1)
    ).astype(jnp.bfloat16)
    above = (
        lax.broadcasted_iota(jnp.int32, (chunks, chunks), 1)
        < lax.broadcasted_iota(jnp.int32, (chunks, chunks), 0)
    ).astype(jnp.bfloat16)
    ones = jnp.ones((128, 128), jnp.bfloat16)
    count = functools.partial(jnp.dot, preferred_element_type=jnp.float32)
    before = count(land, earlier).astype(jnp.int32)
    sea_in_row = 128 - count(land, ones).astype(jnp.int32)
    wide_lane = lax.broadcasted_iota(jnp.int32, (chunks, 128), 1)
    wide_row = lax.broadcasted_iota(jnp.int32, (chunks, 128), 0)
    rank0 = wide_row * 128 - count(count(above, land).astype(jnp.bfloat16), ones).astype(jnp.int32)
    put[0] = jnp.bitwise_and(rank0 + wide_lane - before, 127)
    put[1] = jnp.bitwise_and(rank0 + wide_lane - before + SEA_DEV, 127)
    to_go = jnp.where(is_sea, before, 0)
    shifts[chunks:, :] = jnp.zeros((shifts.shape[0] - chunks, 128), jnp.int32)
    go_left[...] = jnp.zeros_like(go_left)
    go_right[...] = jnp.zeros_like(go_right)

    def close_up(i, to_go):
        d = jnp.left_shift(1, i)
        incoming = pltpu.roll(to_go, 128 - d, 1)
        stay = jnp.where(jnp.bitwise_and(to_go, d) != 0, 0, to_go)
        return jnp.where(jnp.bitwise_and(incoming, d) != 0, incoming, stay)

    def plan_rows(to_go):
        nth = jnp.bitwise_and(wide_lane - rank0, 127)
        front = jnp.bitwise_and(wide_lane + to_go, 127)
        took = jnp.take_along_axis(front, nth, axis=1, mode="promise_in_bounds")
        pick[0] = took
        pick[1] = pltpu.roll(took, SEA_DEV, 1)
        up = wide_row - jnp.right_shift(rank0 + nth, 7)
        shifts[0:chunks, :] = jnp.where(nth < sea_in_row, up, 0)
        for b in range(ROW_STEPS):
            here, incoming = shifts[0:chunks, :], shifts[1 << b : chunks + (1 << b), :]
            goes = jnp.bitwise_and(here, 1 << b)
            comes = jnp.bitwise_and(incoming, 1 << b)
            rights, lefts = (goes, comes) if b == 0 else (rights + goes, lefts + comes)
            shifts[0:chunks, :] = jnp.where(comes != 0, incoming, jnp.where(goes != 0, 0, here))
        for words, found in ((go_right, rights), (go_left, lefts)):
            words[0, REACH : REACH + chunks, :] = found
            words[1, REACH : REACH + chunks, :] = pltpu.roll(found, SEA_DEV, 1)

    zero = jnp.zeros((8, 128), jnp.float32)
    pad = per_row
    for t in range(2):
        for v in range(pad):
            for f in (field_a, field_b):
                f[t, v] = zero
                f[t, pad + chunks + v] = zero
    base = (me * bins_dev) % ND
    for copy in small[1:]:
        copy.wait()
    cw, ce, cs, cn = [], [], [], []
    for t in range(2):
        k = ((me * bins_dev + jnp.minimum(2 * row + t, bins_dev - 1)) // ND).astype(jnp.float32)
        pace = 0.2 * jnp.exp(-LOG_RATIO * k)
        ax = pace * tab[pl.ds(at["cos"] + base + t, 8, stride=2), :]
        ay = pace * tab[pl.ds(at["sin"] + base + t, 8, stride=2), :]
        cw.append(jnp.maximum(ax, 0.0))
        ce.append(-jnp.minimum(ax, 0.0))
        cs.append(jnp.maximum(ay, 0.0))
        cn.append(-jnp.minimum(ay, 0.0))

    def split_bins(g, carry):
        for u in range(8):
            v = g * 8 + u
            cols = pl.ds(pl.multiple_of(v * 128, 128), 128)
            stage[u, 0:bins_dev, :] = x[:, cols] * sea_float[pl.ds(v, 1), :]
            for t in range(2):
                field_a[t, pad + v, 0:half, :] = stage[u, pl.ds(t, half, stride=2), :]
        return carry

    def split_part(part, carry):
        load(part).wait()
        per_part = chunks // 8 // parts
        return lax.fori_loop(part * per_part, (part + 1) * per_part, split_bins, carry)

    lax.fori_loop(0, parts, split_part, 0)

    for s in range(SUBSTEPS):
        src, dst = (field_a, field_b) if s % 2 == 0 else (field_b, field_a)

        def advance(g, to_go, src=src, dst=dst, s=s):
            if s == 0:
                to_go = close_up(2 * g + 1, close_up(2 * g, to_go))
            for ru in range(8):
                r = g * 8 + ru
                widen = tab[pl.ds(at["widen"] + r, 1), :]
                first = pad + r * per_row
                for t in range(2):
                    west_c, east_c = cw[t] * widen, ce[t] * widen
                    own_c = 1.0 - west_c - east_c - cs[t] - cn[t]
                    e = [src[t, first + q] for q in range(per_row)]
                    right = [pltpu.roll(a, 1, 1) for a in e]
                    left = [pltpu.roll(a, 127, 1) for a in e]
                    for q in range(per_row):
                        west = jnp.where(lane == 0, right[q - 1], right[q])
                        east = jnp.where(lane == 127, left[(q + 1) % per_row], left[q])
                        new = (
                            own_c * e[q] + west_c * west + east_c * east
                            + cs[t] * src[t, first + q - per_row]
                            + cn[t] * src[t, first + q + per_row]
                        )
                        v = first + q - pad
                        if s < SUBSTEPS - 1:
                            dst[t, first + q] = new * sea_float[pl.ds(v, 1), :]
                        else:
                            wind = (speed2d, angle2d)[t][pl.ds(v, 1), :]
                            dst[t, first + q] = jnp.where(row == half, wind, new)
            return to_go

        to_go = lax.fori_loop(0, lat_count // 8, advance, to_go)
        if s == 0:
            plan_rows(to_go)
    final = field_a if SUBSTEPS % 2 == 0 else field_b
    entered()

    def to_lanes(g, carry):
        for u in range(2 * UNROLL):
            v = g * 2 * UNROLL + u
            for t in range(2):
                moved_a[t, FAR + v] = lanes(final[t, pad + v], pick.at[t], v)
        return carry

    lax.fori_loop(0, chunks // (2 * UNROLL), to_lanes, 0)


    def keep_near(t, u, v, tile):
        moved_b[t, FAR + v] = tile

    near_rows(chunks, go_left, moved_a, keep_near, True, (0, 1, 2))

    def pack(g, carry):
        for u in range(UNROLL):
            v = g * UNROLL + u
            even, odd = (far_rows(go_left, moved_b, t, v, 1, (3, 4, 5)) for t in range(2))
            send[2 * v] = jnp.where(low, even, odd)
            send[2 * v + 1] = jnp.where(low, odd, even)
        return carry

    lax.fori_loop(0, n * SEA_DEV // 128 // UNROLL, pack, 0)


    def exchange(visit, src, dst, rows, k, arrival):
        def push(to):
            pltpu.make_async_remote_copy(
                src_ref=src.at[to, pl.ds(0, rows)],
                dst_ref=dst.at[me, pl.ds(0, rows)],
                send_sem=send_sem.at[k],
                recv_sem=arrival,
                device_id={"spec": to},
                device_id_type=MESH,
            ).start()

        visit(push)
        pltpu.make_async_copy(src.at[me, pl.ds(0, rows)], dst.at[me, pl.ds(0, rows)], arrival).start()

    def finish(ref, count, rows, sem):
        part = ref.at[pl.ds(0, count), pl.ds(0, rows)]
        pltpu.make_async_copy(part, part, sem).wait()

    exchange(peers_but_late, send, recv, half, 0, recv_sem.at[my_x])

    wind = send[me][half : half + 1, :]
    other = pltpu.roll(wind, SEA_DEV, 1)
    odd_side = lax.rem(me, 2) * SEA_DEV
    even_half = lambda shape: jnp.bitwise_xor(lax.broadcasted_iota(jnp.int32, shape, 1), odd_side) < SEA_DEV
    low16 = even_half((PAIRS, 128))
    speed = jnp.where(even_half((1, 128)), wind, other)
    angle = jnp.where(even_half((1, 128)), other, wind)

    def paired(name):
        rows = tab[at[name] : at[name] + PAIRS, :]
        return jnp.where(odd_side == 0, rows, pltpu.roll(rows, SEA_DEV, 1))

    toward = speed * (paired("pair_cos") * jnp.cos(angle) + paired("pair_sin") * jnp.sin(angle))
    zero16 = jnp.zeros((PAIRS, 128), jnp.float32)
    for w in range(4):
        for k in (0, 1, 2, NF + 3, NF + 4):
            rolled[w, k] = zero16
    for k in range(2):
        low_part[k] = zero16
    for k in range(3):
        high_part[NF + k] = zero16

    def turns(a, amounts):
        s = pltpu.roll(a, SEA_DEV, 1)
        need = {1: (1, 0), -1: (0, -1), 3: (2, 1), -3: (-1, -2)}
        by = {0: s}
        for m in amounts:
            for w in need[m]:
                if w not in by:
                    by[w] = pltpu.roll(s, w % PAIRS, 0)
        return [jnp.where(low16, by[need[m][0]], by[need[m][1]]) for m in amounts]

    group = 8
    per_group = half * group // PAIRS

    def arrange(i, carry):
        m0, m1 = carry
        h = lax.rem(i + 1, side)
        finish(recv, side * cores, half, recv_sem.at[h])
        for g in (2 * h, 2 * h + 1):
            for i in range(group):
                flat[g, half * i : half * i + half, :] = recv[g * group + i, 0:half, :]
        for g in (2 * h, 2 * h + 1):
            for q in range(per_group):
                k = g * per_group + q
                a = flat[g, PAIRS * q : PAIRS * (q + 1), :]
                energy[k] = a
                m0 = m0 + a
                m1 = m1 + tab[pl.ds(at["omega"] + k, 1), :] * a
                for w, b in enumerate(turns(a, (1, -1, 3, -3))):
                    rolled[w, k + 3] = b
        return m0, m1

    m0, m1 = lax.fori_loop(0, side, arrange, (zero16, zero16))

    def over_bins(a):
        a = jnp.sum(a, axis=0, keepdims=True)
        return (a + pltpu.roll(a, SEA_DEV, 1)) * (1.0 / (NF * ND))

    m0, m1 = over_bins(m0), over_bins(m1)
    mean_freq = m1 / (m0 + 1e-6)
    steep = m0 * mean_freq * mean_freq
    breaking = steep * steep / (1.0 + steep * steep)

    def transfer(g, carry):
        for q in range(2 * per_group):
            k = g * 2 * per_group + q
            a = energy[k]
            factor = tab[pl.ds(at["rate"] + k, 1), :] * a
            rates = []
            for plus, minus in ((rolled[1, k + 5], rolled[2, k]), (rolled[0, k + 5], rolled[3, k])):
                rates.append(factor * (a * (plus + minus) - 2.0 * plus * minus))
            up, down = turns(rates[0], (1, -3)), turns(rates[1], (-1, 3))
            own[k] = -2.0 * (rates[0] + rates[1])
            low_part[k + 2] = up[0] + down[0]
            high_part[k] = up[1] + down[1]
        return carry

    lax.fori_loop(0, n // group // 2, transfer, 0)

    def renew(g, total):
        for q in range(per_group):
            k = g * per_group + q
            a = energy[k]
            omega = tab[pl.ds(at["omega"] + k, 1), :]
            gain = (0.05 * omega) * jnp.maximum(0.0, omega * toward - 1.0)
            new = a + (gain - (0.03 * omega) * breaking) * a
            new = new + own[k] + low_part[k] + high_part[k + 3]
            total = total + new
            flat[g, PAIRS * q : PAIRS * (q + 1), :] = new
        for i in range(group):
            back[g * group + i, 0:half, :] = flat[g, half * i : half * i + half, :]
        return total

    total = lax.fori_loop(0, n // group, renew, zero16)
    height = 4.0 * jnp.sqrt(over_bins(total) + 1e-6)

    def add_height(g, carry):
        for i in range(group):
            back[g * group + i, half : half + 1, :] = height
        return carry

    lax.fori_loop(0, n // group, add_height, 0)

    exchange(peers, back, home, half + 1, 1, recv_sem.at[side])
    finish(send, n - 1, half, send_sem.at[0])
    finish(home, n, half + 1, recv_sem.at[side])
    finish(back, n - 1, half + 1, send_sem.at[1])


def unpack_kernel(
    n, bins_dev,
    home, go_right, put, mask2d,
    out, height_out, mean_out,
    moved_a, moved_b, stage, heights,
):
    chunks = mask2d.shape[0]
    half = bins_dev // 2
    cells = chunks * 128
    per_row = NLON // 128
    me = lax.axis_index("spec")
    lane = lax.broadcasted_iota(jnp.int32, (8, 128), 1)
    low = lane < SEA_DEV

    def unpack(g, carry):
        for u in range(2 * UNROLL):
            v = g * 2 * UNROLL + u
            a, b = home[2 * v], home[2 * v + 1]
            moved_a[0, FAR + v] = jnp.where(low, a, b)
            moved_a[1, FAR + v] = jnp.where(low, b, a)
        return carry

    lax.fori_loop(0, n * SEA_DEV // 128 // (2 * UNROLL), unpack, 0)

    def spread(g, carry):
        for u in range(4):
            v = g * 4 + u
            for t in range(2):
                moved_b[t, FAR + v] = far_rows(go_right, moved_a, t, v, -1, (5, 4, 3))
        return carry

    lax.fori_loop(0, chunks // 4, spread, 0)

    def keep_apart(t, u, v, tile):
        moved_a[t, FAR + v] = tile

    near_rows(chunks, go_right, moved_b, keep_apart, False, (2, 1, 0))

    def deliver(g, carry):
        for u in range(2 * UNROLL):
            v = g * 2 * UNROLL + u
            sea = jnp.broadcast_to(mask2d[pl.ds(v, 1), :] != 0, (8, 128))
            for t in range(2):
                tile = jnp.where(sea, lanes(moved_a[t, FAR + v], put.at[t], v), 0.0)
                stage[u, pl.ds(t, half, stride=2), :] = tile[0:half]
                if t == 0:
                    heights[pl.ds(v, 1), :] = tile[half : half + 1]
        for u in range(2 * UNROLL):
            v = g * 2 * UNROLL + u
            out[:, pl.ds(pl.multiple_of(v * 128, 128), 128)] = stage[u, 0:bins_dev, :]
        return carry

    lax.fori_loop(0, chunks // (2 * UNROLL), deliver, 0)

    points = cells // n
    together = NLON // points
    start = me // together * per_row
    three = [heights[pl.ds(start + q, 1), :] for q in range(per_row)]
    u = lax.rem(me, together)
    picked = None
    for g in range(together):
        first, offset = g * points // 128, g * points % 128
        piece = three[first]
        if offset:
            after = three[min(first + 1, per_row - 1)]
            piece = jnp.where(
                lane[0:1] < 128 - offset,
                pltpu.roll(piece, 128 - offset, 1),
                pltpu.roll(after, 128 - offset, 1),
            )
        picked = piece if picked is None else jnp.where(u == g, piece, picked)
    height_out[...] = picked[:, 0:points]
    all_heights = jnp.sum(heights[...], axis=0, keepdims=True)
    mean_out[...] = jnp.sum(all_heights, axis=1, keepdims=True) * (1.0 / (SEA_DEV * n))


def solution(mesh):
    n = mesh.shape["spec"]
    cores = 2
    side = math.isqrt(n // cores)

    def local(spectrum, sea_mask, wind_speed, wind_angle):
        bins_dev, cells = spectrum.shape
        chunks = cells // 128
        padded = chunks + 2 * (NLON // 128)
        tab, at = tables(cells // NLON)
        vmem = pl.BlockSpec(memory_space=pltpu.VMEM)
        words = pltpu.VMEM((2, chunks + 2 * REACH, 128), jnp.int32)
        by_freq = lambda *dims: pltpu.VMEM((*dims, PAIRS, 128), jnp.float32)
        messages = lambda count: pltpu.VMEM((count, 8, 128), jnp.float32)
        home, go_right, put = pl.pallas_call(
            functools.partial(step_kernel, n, side, cores, at),
            name="wave_step",
            out_shape=(
                jax.ShapeDtypeStruct((n, 8, 128), jnp.float32),
                jax.ShapeDtypeStruct((2, chunks + 2 * REACH, 128), jnp.int32),
                jax.ShapeDtypeStruct((2, chunks, 128), jnp.int32),
            ),
            in_specs=[pl.BlockSpec(memory_space=pltpu.HBM)] * 5,
            out_specs=(vmem,) * 3,
            scratch_shapes=[
                pltpu.VMEM((bins_dev, cells), jnp.float32),
                pltpu.VMEM((chunks, 128), jnp.int32),
                pltpu.VMEM((chunks, 128), jnp.float32),
                pltpu.VMEM((chunks, 128), jnp.float32),
                pltpu.VMEM((chunks, 128), jnp.float32),
                pltpu.VMEM(tab.shape, jnp.float32),
                pltpu.VMEM((2, padded, 8, 128), jnp.float32),
                pltpu.VMEM((2, padded, 8, 128), jnp.float32),
                pltpu.VMEM((8, 16, 128), jnp.float32),
                pltpu.VMEM((chunks + REACH, 128), jnp.int32),
                words,
                pltpu.VMEM((2, chunks, 128), jnp.int32),
                pltpu.VMEM((2, chunks + 2 * FAR, 8, 128), jnp.float32),
                pltpu.VMEM((2, chunks + 2 * FAR, 8, 128), jnp.float32),
                messages(n),
                messages(n),
                messages(n),
                pltpu.VMEM((n // 8, 8 * bins_dev // 2, 128), jnp.float32),
                by_freq(NF),
                by_freq(4, NF + 5),
                by_freq(NF),
                by_freq(NF + 2),
                by_freq(NF + 3),
                pltpu.SemaphoreType.DMA((2,)),
                pltpu.SemaphoreType.DMA((side + 1,)),
                pltpu.SemaphoreType.DMA((8,)),
                pltpu.SemaphoreType.REGULAR((side,)),
                pltpu.SemaphoreType.REGULAR,
            ],
            compiler_params=pltpu.CompilerParams(
                collective_id=0, has_side_effects=True, vmem_limit_bytes=VMEM_BYTES
            ),
        )(
            *(
                pltpu.with_memory_space_constraint(a, pltpu.HBM)
                for a in (
                    spectrum,
                    sea_mask.reshape(chunks, 128),
                    wind_speed.reshape(chunks, 128),
                    wind_angle.reshape(chunks, 128),
                    jnp.asarray(tab),
                )
            )
        )
        moved = pltpu.VMEM((2, chunks + 2 * FAR, 8, 128), jnp.float32)
        new_spectrum, height, mean = pl.pallas_call(
            functools.partial(unpack_kernel, n, bins_dev),
            name="unpack",
            out_shape=(
                jax.ShapeDtypeStruct((bins_dev, cells), jnp.float32),
                jax.ShapeDtypeStruct((1, cells // n), jnp.float32),
                jax.ShapeDtypeStruct((1, 1), jnp.float32),
            ),
            in_specs=[vmem] * 4,
            out_specs=(vmem,) * 3,
            scratch_shapes=[
                moved,
                moved,
                pltpu.VMEM((16, 16, 128), jnp.float32),
                pltpu.VMEM((chunks, 128), jnp.float32),
            ],
            compiler_params=pltpu.CompilerParams(vmem_limit_bytes=VMEM_BYTES),
        )(home, go_right, put, sea_mask.reshape(chunks, 128))
        return new_spectrum, height.reshape(-1), mean.reshape(1)

    return jax.shard_map(
        local,
        mesh=mesh,
        in_specs=(P(("grp", "spec"), None), P(), P("grp"), P("grp")),
        out_specs=(P(("grp", "spec"), None), P(("grp", "spec")), P("grp")),
        check_vma=False,
    )
```

```python
import functools
import math

import jax
import jax.numpy as jnp
import numpy as np
from jax import lax
from jax.experimental import pallas as pl
from jax.experimental.pallas import tpu as pltpu
from jax.sharding import PartitionSpec as P

NF = 48
ND = 32
NLON = 384
SUBSTEPS = 2
SEA_DEV = 64
MESH = pl.DeviceIdType.MESH
LOG_RATIO = math.log(1.1)
PAIRS = ND // 2
ROW_STEPS = 6
REACH = 32
UNROLL = 8
VMEM_BYTES = 24 * 1024 * 1024
FAR = 56


def tables(lat_count):
    heading = 2.0 * np.pi * (np.arange(ND) + 0.5) / ND
    wrapped = np.concatenate([heading, heading[:24]])
    flat = lambda a: np.repeat(np.asarray(a)[:, None], 128, 1)
    paired = np.repeat(heading.reshape(PAIRS, 2), SEA_DEV, axis=1)
    latitude = np.radians(-75.0 + 150.0 * (np.arange(lat_count) + 0.5) / lat_count)
    k = np.arange(NF)
    rows, at = [], {}
    for name, block in (
        ("cos", flat(np.cos(wrapped))),
        ("sin", flat(np.sin(wrapped))),
        ("pair_cos", np.cos(paired)),
        ("pair_sin", np.sin(paired)),
        ("widen", flat(1.0 / np.cos(latitude))),
        ("omega", flat(np.exp(LOG_RATIO * (k - NF // 2)))),
        ("rate", flat(np.where((k >= 3) & (k <= NF - 3), 0.001, 0.0))),
    ):
        at[name] = sum(len(r) for r in rows)
        rows.append(block)
    return np.concatenate(rows).astype(np.float32), at


def chip_order(side):
    hops = lambda d: min(d, side - d)
    way = lambda d: (d > 0) - 2 * (d > side // 2)
    chips = [(x, y) for x in range(side) for y in range(side)][1:]
    chips.sort(key=lambda o: (-(hops(o[0]) + hops(o[1])), 3 * o[0] + 5 * o[1]))
    kinds = {}
    for o in chips:
        kinds.setdefault((way(o[0]), way(o[1])), []).append(o)
    placed = [((i + 0.5) / len(k), o) for k in kinds.values() for i, o in enumerate(k)]
    return [o for _, o in sorted(placed, key=lambda p: p[0])]


def word_of(words, v):
    return jnp.broadcast_to(words[pl.ds(REACH + v, 1), :], (8, 128))


def has(word, i):
    return jnp.bitwise_and(word, 1 << i) != 0


def lanes(tile, index, v):
    index = jnp.broadcast_to(index[pl.ds(v, 1), :], (8, 128))
    return jnp.take_along_axis(tile, index, axis=1, mode="promise_in_bounds")


def near_rows(chunks, words, src, emit, toward_end, bit_order):
    way = 1 if toward_end else -1

    def block(g, carry):
        first = g * UNROLL
        span = [first + way * u if toward_end else first + UNROLL - 1 - u for u in range(UNROLL + 7)]
        for t in range(2):
            word = [word_of(words.at[t], v) for v in span]
            cur = [src[t, FAR + v] for v in span]
            for b in bit_order:
                d = 1 << b
                cur = [
                    jnp.where(has(word[u], b), cur[u + d], cur[u])
                    for u in range(len(cur) - d)
                ]
            for u in range(UNROLL):
                emit(t, u, span[u], cur[u])
        return carry

    lax.fori_loop(0, chunks // UNROLL, block, 0)


def far_rows(words, src, t, v, way, bit_order):
    def value(v, order):
        if not order:
            return src[t, FAR + v]
        d = way * (1 << order[-1])
        return jnp.where(
            has(word_of(words.at[t], v), order[-1]), value(v + d, order[:-1]), value(v, order[:-1])
        )

    return value(v, bit_order)


def step_kernel(
    n, side, cores, at,
    x_hbm, mask_hbm, speed_hbm, angle_hbm, tab_hbm,
    home, go_right, put,
    x, mask2d, sea_float, speed2d, angle2d, tab, field_a, field_b, stage, shifts, go_left, pick, moved_a, moved_b,
    send, recv, back, flat, energy, rolled, own, low_part, high_part,
    order, send_sem, recv_sem, load_sem, column_sem, first_sem,
):
    bins_dev, cells = x.shape
    half = bins_dev // 2
    chunks = cells // 128
    per_row = NLON // 128
    lat_count = cells // NLON
    me = lax.axis_index("spec")
    my_x, my_y, my_c = me // (side * cores), lax.rem(me // cores, side), lax.rem(me, cores)

    parts = 4
    part_cols = cells // parts
    small = [
        pltpu.make_async_copy(src, dst, load_sem.at[parts + k])
        for k, (src, dst) in enumerate(
            ((mask_hbm, mask2d), (tab_hbm, tab), (speed_hbm, speed2d), (angle_hbm, angle2d))
        )
    ]

    def load(part):
        cols = pl.ds(pl.multiple_of(part * part_cols, 128), part_cols)
        return pltpu.make_async_copy(x_hbm.at[:, cols], x.at[:, cols], load_sem.at[part])

    small[0].start()
    for part in range(parts):
        load(part).start()
    for copy in small[1:]:
        copy.start()

    def wrap(a):
        return jnp.bitwise_and(a, side - 1) if side & (side - 1) == 0 else lax.rem(a, side)

    def hop(u):
        return side // 2 + (1 - 2 * jnp.bitwise_and(u, 1)) * jnp.right_shift(u + 1, 1)

    def both_cores(act, px, py):
        first = (px * side + py) * cores
        act(first + my_c)
        for c in range(1, cores):
            act(first + jnp.where(my_c + c >= cores, my_c + c - cores, my_c + c))

    def own_chip(act):
        for c in range(1, cores):
            act(me - my_c + lax.rem(my_c + c, cores))

    chips = chip_order(side)
    other_rows = [o for o in chips if o[1] != 0]

    def peers(act, which, count):
        def chip(i, carry):
            both_cores(act, wrap(my_x + order[2 * which, i]), wrap(my_y + order[2 * which + 1, i]))
            return carry

        lax.fori_loop(0, count, chip, 0)

    is_first = me == 0
    is_second = me == 1
    below_first = jnp.logical_and(jnp.logical_and(my_x == 0, my_c == 0), my_y != 0)

    def signal(semaphore, to):
        pl.semaphore_signal(semaphore, inc=1, device_id={"spec": to}, device_id_type=MESH)

    def down_column(act):
        def one(u, carry):
            act((my_x * side + wrap(my_y + hop(u))) * cores + my_c)
            return carry

        lax.fori_loop(0, side - 1, one, 0)

    def along_row(act, own=None):
        def one(u, carry):
            both_cores(act, wrap(my_x + hop(u)), my_y)
            return carry

        lax.fori_loop(0, side - 1, one, 0)
        own_chip(act if own is None else own)

    def peers_as_known(act, own):
        along_row(act, own)

        @pl.when(jnp.logical_not(is_first))
        def _():
            def row_in(i, carry):
                pl.semaphore_wait(column_sem.at[wrap(my_y + i)], 1)
                return carry

            @pl.when(jnp.logical_not(below_first))
            def _():
                lax.fori_loop(1, side, row_in, 0)

            @pl.when(is_second)
            def _():
                down_column(lambda to: signal(column_sem.at[0], to - 1))

            @pl.when(below_first)
            def _():
                lax.fori_loop(1, side, row_in, 0)

        peers(act, 1, len(other_rows))

    barrier = pltpu.get_barrier_semaphore()

    @pl.when(jnp.logical_not(is_first))
    def _():
        along_row(lambda to: signal(barrier, to))
        down_column(lambda to: signal(barrier, to))

    def entered():
        called = side * cores + side - 2

        @pl.when(jnp.logical_not(is_first))
        def _():
            with_first = jnp.logical_or(my_y == 0, below_first)
            pl.semaphore_wait(barrier, called - jnp.where(with_first, 1, 0))

            def complete(to):
                @pl.when(to == 0)
                def _():
                    signal(barrier, to)

                @pl.when(to != 0)
                def _():
                    signal(column_sem.at[my_y], to)

            down_column(complete)

    for which, table in enumerate((chips, other_rows)):
        for i, (dx, dy) in enumerate(table):
            order[2 * which, i] = dx
            order[2 * which + 1, i] = dy
    small[0].wait()

    lane = lax.broadcasted_iota(jnp.int32, (8, 128), 1)
    row = lax.broadcasted_iota(jnp.int32, (8, 128), 0)
    low = lane < SEA_DEV

    is_sea = mask2d[...] != 0
    sea_float[...] = mask2d[...].astype(jnp.float32)
    land = jnp.where(is_sea, 0.0, 1.0).astype(jnp.bfloat16)
    earlier = (
        lax.broadcasted_iota(jnp.int32, (128, 128), 0) < lax.broadcasted_iota(jnp.int32, (128, 128), 1)
    ).astype(jnp.bfloat16)
    above = (
        lax.broadcasted_iota(jnp.int32, (chunks, chunks), 1)
        < lax.broadcasted_iota(jnp.int32, (chunks, chunks), 0)
    ).astype(jnp.bfloat16)
    ones = jnp.ones((128, 128), jnp.bfloat16)
    count = functools.partial(jnp.dot, preferred_element_type=jnp.float32)
    before = count(land, earlier).astype(jnp.int32)
    sea_in_row = 128 - count(land, ones).astype(jnp.int32)
    wide_lane = lax.broadcasted_iota(jnp.int32, (chunks, 128), 1)
    wide_row = lax.broadcasted_iota(jnp.int32, (chunks, 128), 0)
    rank0 = wide_row * 128 - count(count(above, land).astype(jnp.bfloat16), ones).astype(jnp.int32)
    put[0] = jnp.bitwise_and(rank0 + wide_lane - before, 127)
    put[1] = jnp.bitwise_and(rank0 + wide_lane - before + SEA_DEV, 127)
    to_go = jnp.where(is_sea, before, 0)
    shifts[chunks:, :] = jnp.zeros((shifts.shape[0] - chunks, 128), jnp.int32)
    go_left[...] = jnp.zeros_like(go_left)
    go_right[...] = jnp.zeros_like(go_right)

    def close_up(i, to_go):
        d = jnp.left_shift(1, i)
        incoming = pltpu.roll(to_go, 128 - d, 1)
        stay = jnp.where(jnp.bitwise_and(to_go, d) != 0, 0, to_go)
        return jnp.where(jnp.bitwise_and(incoming, d) != 0, incoming, stay)

    def plan_rows(to_go):
        nth = jnp.bitwise_and(wide_lane - rank0, 127)
        front = jnp.bitwise_and(wide_lane + to_go, 127)
        took = jnp.take_along_axis(front, nth, axis=1, mode="promise_in_bounds")
        pick[0] = took
        pick[1] = pltpu.roll(took, SEA_DEV, 1)
        up = wide_row - jnp.right_shift(rank0 + nth, 7)
        shifts[0:chunks, :] = jnp.where(nth < sea_in_row, up, 0)
        for b in range(ROW_STEPS):
            here, incoming = shifts[0:chunks, :], shifts[1 << b : chunks + (1 << b), :]
            goes = jnp.bitwise_and(here, 1 << b)
            comes = jnp.bitwise_and(incoming, 1 << b)
            rights, lefts = (goes, comes) if b == 0 else (rights + goes, lefts + comes)
            shifts[0:chunks, :] = jnp.where(comes != 0, incoming, jnp.where(goes != 0, 0, here))
        for words, found in ((go_right, rights), (go_left, lefts)):
            words[0, REACH : REACH + chunks, :] = found
            words[1, REACH : REACH + chunks, :] = pltpu.roll(found, SEA_DEV, 1)

    zero = jnp.zeros((8, 128), jnp.float32)
    pad = per_row
    for t in range(2):
        for v in range(pad):
            for f in (field_a, field_b):
                f[t, v] = zero
                f[t, pad + chunks + v] = zero
    base = (me * bins_dev) % ND
    for copy in small[1:]:
        copy.wait()
    cw, ce, cs, cn = [], [], [], []
    for t in range(2):
        k = ((me * bins_dev + jnp.minimum(2 * row + t, bins_dev - 1)) // ND).astype(jnp.float32)
        pace = 0.2 * jnp.exp(-LOG_RATIO * k)
        ax = pace * tab[pl.ds(at["cos"] + base + t, 8, stride=2), :]
        ay = pace * tab[pl.ds(at["sin"] + base + t, 8, stride=2), :]
        cw.append(jnp.maximum(ax, 0.0))
        ce.append(-jnp.minimum(ax, 0.0))
        cs.append(jnp.maximum(ay, 0.0))
        cn.append(-jnp.minimum(ay, 0.0))

    def split_bins(g, carry):
        for u in range(8):
            v = g * 8 + u
            cols = pl.ds(pl.multiple_of(v * 128, 128), 128)
            stage[u, 0:bins_dev, :] = x[:, cols] * sea_float[pl.ds(v, 1), :]
            for t in range(2):
                field_a[t, pad + v, 0:half, :] = stage[u, pl.ds(t, half, stride=2), :]
        return carry

    def split_part(part, carry):
        load(part).wait()
        per_part = chunks // 8 // parts
        return lax.fori_loop(part * per_part, (part + 1) * per_part, split_bins, carry)

    lax.fori_loop(0, parts, split_part, 0)

    for s in range(SUBSTEPS):
        src, dst = (field_a, field_b) if s % 2 == 0 else (field_b, field_a)

        def advance(g, to_go, src=src, dst=dst, s=s):
            if s == 0:
                to_go = close_up(2 * g + 1, close_up(2 * g, to_go))
            for ru in range(8):
                r = g * 8 + ru
                widen = tab[pl.ds(at["widen"] + r, 1), :]
                first = pad + r * per_row
                for t in range(2):
                    west_c, east_c = cw[t] * widen, ce[t] * widen
                    own_c = 1.0 - west_c - east_c - cs[t] - cn[t]
                    e = [src[t, first + q] for q in range(per_row)]
                    right = [pltpu.roll(a, 1, 1) for a in e]
                    left = [pltpu.roll(a, 127, 1) for a in e]
                    for q in range(per_row):
                        west = jnp.where(lane == 0, right[q - 1], right[q])
                        east = jnp.where(lane == 127, left[(q + 1) % per_row], left[q])
                        new = (
                            own_c * e[q] + west_c * west + east_c * east
                            + cs[t] * src[t, first + q - per_row]
                            + cn[t] * src[t, first + q + per_row]
                        )
                        v = first + q - pad
                        if s < SUBSTEPS - 1:
                            dst[t, first + q] = new * sea_float[pl.ds(v, 1), :]
                        else:
                            wind = (speed2d, angle2d)[t][pl.ds(v, 1), :]
                            dst[t, first + q] = jnp.where(row == half, wind, new)
            return to_go

        to_go = lax.fori_loop(0, lat_count // 8, advance, to_go)
        if s == 0:
            plan_rows(to_go)
    final = field_a if SUBSTEPS % 2 == 0 else field_b
    entered()

    def to_lanes(g, carry):
        for u in range(2 * UNROLL):
            v = g * 2 * UNROLL + u
            for t in range(2):
                moved_a[t, FAR + v] = lanes(final[t, pad + v], pick.at[t], v)
        return carry

    lax.fori_loop(0, chunks // (2 * UNROLL), to_lanes, 0)


    def keep_near(t, u, v, tile):
        moved_b[t, FAR + v] = tile

    near_rows(chunks, go_left, moved_a, keep_near, True, (0, 1, 2))

    def pack(g, carry):
        for u in range(UNROLL):
            v = g * UNROLL + u
            even, odd = (far_rows(go_left, moved_b, t, v, 1, (3, 4, 5)) for t in range(2))
            send[2 * v] = jnp.where(low, even, odd)
            send[2 * v + 1] = jnp.where(low, odd, even)
        return carry

    lax.fori_loop(0, n * SEA_DEV // 128 // UNROLL, pack, 0)


    def copy_to(to, src, dst, k, arrival):
        pltpu.make_async_remote_copy(
            src_ref=src,
            dst_ref=dst,
            send_sem=send_sem.at[k],
            recv_sem=arrival,
            device_id={"spec": to},
            device_id_type=MESH,
        ).start()

    def own_message(src, dst, rows, arrival):
        pltpu.make_async_copy(src.at[me, pl.ds(0, rows)], dst.at[me, pl.ds(0, rows)], arrival).start()

    def finish(ref, count, rows, sem):
        part = ref.at[pl.ds(0, count), pl.ds(0, rows)]
        pltpu.make_async_copy(part, part, sem).wait()

    @pl.when(is_first)
    def _():
        pl.semaphore_wait(barrier, side * cores + 2 * side - 3)
        signal(first_sem, 1)

    def push(to):
        aside = jnp.where(to == 0, 1, 0)
        copy_to(
            to + aside,
            send.at[to, pl.ds(0, half)],
            recv.at[me + aside * n, pl.ds(0, half)],
            0,
            recv_sem.at[my_x + aside * side],
        )

    def push_own_chip(to):
        @pl.when(is_second)
        def _():
            pltpu.make_async_copy(
                send.at[0, pl.ds(0, half)], recv.at[n + 1, pl.ds(0, half)], recv_sem.at[side]
            ).start()

        @pl.when(jnp.logical_not(is_second))
        def _():
            copy_to(to, send.at[to, pl.ds(0, half)], recv.at[me, pl.ds(0, half)], 0, recv_sem.at[my_x])

    peers_as_known(push, push_own_chip)
    own_message(send, recv, half, recv_sem.at[my_x])

    @pl.when(is_second)
    def _():
        pl.semaphore_wait(first_sem, 1)

    def hand_over(h):
        def pass_on(start, count):
            finish(recv, count, half, recv_sem.at[side + h])
            copy_to(
                0,
                recv.at[pl.ds(n + start, count), pl.ds(0, half)],
                recv.at[pl.ds(start, count), pl.ds(0, half)],
                2,
                recv_sem.at[h],
            )

        @pl.when(jnp.logical_and(is_second, h != 0))
        def _():
            pass_on(h * side * cores, side * cores)

        @pl.when(jnp.logical_and(is_second, h == 0))
        def _():
            pass_on(1, side * cores - 1)


    wind = send[me][half : half + 1, :]
    other = pltpu.roll(wind, SEA_DEV, 1)
    odd_side = lax.rem(me, 2) * SEA_DEV
    even_half = lambda shape: jnp.bitwise_xor(lax.broadcasted_iota(jnp.int32, shape, 1), odd_side) < SEA_DEV
    low16 = even_half((PAIRS, 128))
    speed = jnp.where(even_half((1, 128)), wind, other)
    angle = jnp.where(even_half((1, 128)), other, wind)

    def paired(name):
        rows = tab[at[name] : at[name] + PAIRS, :]
        return jnp.where(odd_side == 0, rows, pltpu.roll(rows, SEA_DEV, 1))

    toward = speed * (paired("pair_cos") * jnp.cos(angle) + paired("pair_sin") * jnp.sin(angle))
    zero16 = jnp.zeros((PAIRS, 128), jnp.float32)
    for w in range(4):
        for k in (0, 1, 2, NF + 3, NF + 4):
            rolled[w, k] = zero16
    for k in range(2):
        low_part[k] = zero16
    for k in range(3):
        high_part[NF + k] = zero16

    def turns(a, amounts):
        s = pltpu.roll(a, SEA_DEV, 1)
        need = {1: (1, 0), -1: (0, -1), 3: (2, 1), -3: (-1, -2)}
        by = {0: s}
        for m in amounts:
            for w in need[m]:
                if w not in by:
                    by[w] = pltpu.roll(s, w % PAIRS, 0)
        return [jnp.where(low16, by[need[m][0]], by[need[m][1]]) for m in amounts]

    group = 8
    per_group = half * group // PAIRS

    def arrange(i, carry):
        m0, m1 = carry
        h = lax.rem(i + 1, side)
        hand_over(h)
        finish(recv, side * cores, half, recv_sem.at[h])
        for g in (2 * h, 2 * h + 1):
            for i in range(group):
                flat[g, half * i : half * i + half, :] = recv[g * group + i, 0:half, :]
        for g in (2 * h, 2 * h + 1):
            for q in range(per_group):
                k = g * per_group + q
                a = flat[g, PAIRS * q : PAIRS * (q + 1), :]
                energy[k] = a
                m0 = m0 + a
                m1 = m1 + tab[pl.ds(at["omega"] + k, 1), :] * a
                for w, b in enumerate(turns(a, (1, -1, 3, -3))):
                    rolled[w, k + 3] = b
        return m0, m1

    m0, m1 = lax.fori_loop(0, side, arrange, (zero16, zero16))

    def over_bins(a):
        a = jnp.sum(a, axis=0, keepdims=True)
        return (a + pltpu.roll(a, SEA_DEV, 1)) * (1.0 / (NF * ND))

    m0, m1 = over_bins(m0), over_bins(m1)
    mean_freq = m1 / (m0 + 1e-6)
    steep = m0 * mean_freq * mean_freq
    breaking = steep * steep / (1.0 + steep * steep)

    def transfer(g, carry):
        for q in range(4 * per_group):
            k = g * 4 * per_group + q
            a = energy[k]
            factor = tab[pl.ds(at["rate"] + k, 1), :] * a
            rates = []
            for plus, minus in ((rolled[1, k + 5], rolled[2, k]), (rolled[0, k + 5], rolled[3, k])):
                rates.append(factor * (a * (plus + minus) - 2.0 * plus * minus))
            up, down = turns(rates[0], (1, -3)), turns(rates[1], (-1, 3))
            own[k] = -2.0 * (rates[0] + rates[1])
            low_part[k + 2] = up[0] + down[0]
            high_part[k] = up[1] + down[1]
        return carry

    lax.fori_loop(0, n // group // 4, transfer, 0)

    def renew(g, total):
        for q in range(per_group):
            k = g * per_group + q
            a = energy[k]
            omega = tab[pl.ds(at["omega"] + k, 1), :]
            gain = (0.05 * omega) * jnp.maximum(0.0, omega * toward - 1.0)
            new = a + (gain - (0.03 * omega) * breaking) * a
            new = new + own[k] + low_part[k] + high_part[k + 3]
            total = total + new
            flat[g, PAIRS * q : PAIRS * (q + 1), :] = new
        for i in range(group):
            back[g * group + i, 0:half, :] = flat[g, half * i : half * i + half, :]
        return total

    total = lax.fori_loop(0, n // group, renew, zero16)
    height = 4.0 * jnp.sqrt(over_bins(total) + 1e-6)

    def add_height(g, carry):
        for i in range(group):
            back[g * group + i, half : half + 1, :] = height
        return carry

    lax.fori_loop(0, n // group, add_height, 0)

    def push_back(to):
        copy_to(
            to,
            back.at[to, pl.ds(0, half + 1)],
            home.at[me, pl.ds(0, half + 1)],
            1,
            recv_sem.at[2 * side],
        )

    peers(push_back, 0, len(chips))
    own_chip(push_back)
    own_message(back, home, half + 1, recv_sem.at[2 * side])

    @pl.when(is_second)
    def _():
        finish(send, n - 2, half, send_sem.at[0])
        finish(recv, n - 1, half, send_sem.at[2])

    @pl.when(jnp.logical_not(is_second))
    def _():
        finish(send, n - 1, half, send_sem.at[0])

    finish(home, n, half + 1, recv_sem.at[2 * side])
    finish(back, n - 1, half + 1, send_sem.at[1])


def unpack_kernel(
    n, bins_dev,
    home, go_right, put, mask2d,
    out, height_out, mean_out,
    moved_a, moved_b, stage, heights,
):
    chunks = mask2d.shape[0]
    half = bins_dev // 2
    cells = chunks * 128
    per_row = NLON // 128
    me = lax.axis_index("spec")
    lane = lax.broadcasted_iota(jnp.int32, (8, 128), 1)
    low = lane < SEA_DEV

    def unpack(g, carry):
        for u in range(2 * UNROLL):
            v = g * 2 * UNROLL + u
            a, b = home[2 * v], home[2 * v + 1]
            moved_a[0, FAR + v] = jnp.where(low, a, b)
            moved_a[1, FAR + v] = jnp.where(low, b, a)
        return carry

    lax.fori_loop(0, n * SEA_DEV // 128 // (2 * UNROLL), unpack, 0)

    def spread(g, carry):
        for u in range(4):
            v = g * 4 + u
            for t in range(2):
                moved_b[t, FAR + v] = far_rows(go_right, moved_a, t, v, -1, (5, 4, 3))
        return carry

    lax.fori_loop(0, chunks // 4, spread, 0)

    def keep_apart(t, u, v, tile):
        moved_a[t, FAR + v] = tile

    near_rows(chunks, go_right, moved_b, keep_apart, False, (2, 1, 0))

    def deliver(g, carry):
        for u in range(2 * UNROLL):
            v = g * 2 * UNROLL + u
            sea = jnp.broadcast_to(mask2d[pl.ds(v, 1), :] != 0, (8, 128))
            for t in range(2):
                tile = jnp.where(sea, lanes(moved_a[t, FAR + v], put.at[t], v), 0.0)
                stage[u, pl.ds(t, half, stride=2), :] = tile[0:half]
                if t == 0:
                    heights[pl.ds(v, 1), :] = tile[half : half + 1]
        for u in range(2 * UNROLL):
            v = g * 2 * UNROLL + u
            out[:, pl.ds(pl.multiple_of(v * 128, 128), 128)] = stage[u, 0:bins_dev, :]
        return carry

    lax.fori_loop(0, chunks // (2 * UNROLL), deliver, 0)

    points = cells // n
    together = NLON // points
    start = me // together * per_row
    three = [heights[pl.ds(start + q, 1), :] for q in range(per_row)]
    u = lax.rem(me, together)
    picked = None
    for g in range(together):
        first, offset = g * points // 128, g * points % 128
        piece = three[first]
        if offset:
            after = three[min(first + 1, per_row - 1)]
            piece = jnp.where(
                lane[0:1] < 128 - offset,
                pltpu.roll(piece, 128 - offset, 1),
                pltpu.roll(after, 128 - offset, 1),
            )
        picked = piece if picked is None else jnp.where(u == g, piece, picked)
    height_out[...] = picked[:, 0:points]
    all_heights = jnp.sum(heights[...], axis=0, keepdims=True)
    mean_out[...] = jnp.sum(all_heights, axis=1, keepdims=True) * (1.0 / (SEA_DEV * n))


def solution(mesh):
    n = mesh.shape["spec"]
    cores = 2
    side = math.isqrt(n // cores)

    def local(spectrum, sea_mask, wind_speed, wind_angle):
        bins_dev, cells = spectrum.shape
        chunks = cells // 128
        padded = chunks + 2 * (NLON // 128)
        tab, at = tables(cells // NLON)
        vmem = pl.BlockSpec(memory_space=pltpu.VMEM)
        words = pltpu.VMEM((2, chunks + 2 * REACH, 128), jnp.int32)
        by_freq = lambda *dims: pltpu.VMEM((*dims, PAIRS, 128), jnp.float32)
        messages = lambda count: pltpu.VMEM((count, 8, 128), jnp.float32)
        home, go_right, put = pl.pallas_call(
            functools.partial(step_kernel, n, side, cores, at),
            name="wave_step",
            out_shape=(
                jax.ShapeDtypeStruct((n, 8, 128), jnp.float32),
                jax.ShapeDtypeStruct((2, chunks + 2 * REACH, 128), jnp.int32),
                jax.ShapeDtypeStruct((2, chunks, 128), jnp.int32),
            ),
            in_specs=[pl.BlockSpec(memory_space=pltpu.HBM)] * 5,
            out_specs=(vmem,) * 3,
            scratch_shapes=[
                pltpu.VMEM((bins_dev, cells), jnp.float32),
                pltpu.VMEM((chunks, 128), jnp.int32),
                pltpu.VMEM((chunks, 128), jnp.float32),
                pltpu.VMEM((chunks, 128), jnp.float32),
                pltpu.VMEM((chunks, 128), jnp.float32),
                pltpu.VMEM(tab.shape, jnp.float32),
                pltpu.VMEM((2, padded, 8, 128), jnp.float32),
                pltpu.VMEM((2, padded, 8, 128), jnp.float32),
                pltpu.VMEM((8, 16, 128), jnp.float32),
                pltpu.VMEM((chunks + REACH, 128), jnp.int32),
                words,
                pltpu.VMEM((2, chunks, 128), jnp.int32),
                pltpu.VMEM((2, chunks + 2 * FAR, 8, 128), jnp.float32),
                pltpu.VMEM((2, chunks + 2 * FAR, 8, 128), jnp.float32),
                messages(n),
                messages(2 * n),
                messages(n),
                pltpu.VMEM((n // 8, 8 * bins_dev // 2, 128), jnp.float32),
                by_freq(NF),
                by_freq(4, NF + 5),
                by_freq(NF),
                by_freq(NF + 2),
                by_freq(NF + 3),
                pltpu.SMEM((4, side * side), jnp.int32),
                pltpu.SemaphoreType.DMA((3,)),
                pltpu.SemaphoreType.DMA((2 * side + 1,)),
                pltpu.SemaphoreType.DMA((8,)),
                pltpu.SemaphoreType.REGULAR((side,)),
                pltpu.SemaphoreType.REGULAR,
            ],
            compiler_params=pltpu.CompilerParams(
                collective_id=0, has_side_effects=True, vmem_limit_bytes=VMEM_BYTES
            ),
        )(
            *(
                pltpu.with_memory_space_constraint(a, pltpu.HBM)
                for a in (
                    spectrum,
                    sea_mask.reshape(chunks, 128),
                    wind_speed.reshape(chunks, 128),
                    wind_angle.reshape(chunks, 128),
                    jnp.asarray(tab),
                )
            )
        )
        moved = pltpu.VMEM((2, chunks + 2 * FAR, 8, 128), jnp.float32)
        new_spectrum, height, mean = pl.pallas_call(
            functools.partial(unpack_kernel, n, bins_dev),
            name="unpack",
            out_shape=(
                jax.ShapeDtypeStruct((bins_dev, cells), jnp.float32),
                jax.ShapeDtypeStruct((1, cells // n), jnp.float32),
                jax.ShapeDtypeStruct((1, 1), jnp.float32),
            ),
            in_specs=[vmem] * 4,
            out_specs=(vmem,) * 3,
            scratch_shapes=[
                moved,
                moved,
                pltpu.VMEM((16, 16, 128), jnp.float32),
                pltpu.VMEM((chunks, 128), jnp.float32),
            ],
            compiler_params=pltpu.CompilerParams(vmem_limit_bytes=VMEM_BYTES),
        )(home, go_right, put, sea_mask.reshape(chunks, 128))
        return new_spectrum, height.reshape(-1), mean.reshape(1)

    return jax.shard_map(
        local,
        mesh=mesh,
        in_specs=(P(("grp", "spec"), None), P(), P("grp"), P("grp")),
        out_specs=(P(("grp", "spec"), None), P(("grp", "spec")), P("grp")),
        check_vma=False,
    )
```

```python
import functools
import math

import jax
import jax.numpy as jnp
import numpy as np
from jax import lax
from jax.experimental import pallas as pl
from jax.experimental.pallas import tpu as pltpu
from jax.sharding import PartitionSpec as P

NF = 48
ND = 32
NLON = 384
SUBSTEPS = 2
SEA_DEV = 64
MESH = pl.DeviceIdType.MESH
LOG_RATIO = math.log(1.1)
PAIRS = ND // 2
ROW_STEPS = 6
REACH = 32
UNROLL = 8
VMEM_BYTES = 24 * 1024 * 1024
FAR = 56


def tables(lat_count):
    heading = 2.0 * np.pi * (np.arange(ND) + 0.5) / ND
    wrapped = np.concatenate([heading, heading[:24]])
    flat = lambda a: np.repeat(np.asarray(a)[:, None], 128, 1)
    paired = np.repeat(heading.reshape(PAIRS, 2), SEA_DEV, axis=1)
    latitude = np.radians(-75.0 + 150.0 * (np.arange(lat_count) + 0.5) / lat_count)
    k = np.arange(NF)
    rows, at = [], {}
    for name, block in (
        ("cos", flat(np.cos(wrapped))),
        ("sin", flat(np.sin(wrapped))),
        ("pair_cos", np.cos(paired)),
        ("pair_sin", np.sin(paired)),
        ("widen", flat(1.0 / np.cos(latitude))),
        ("omega", flat(np.exp(LOG_RATIO * (k - NF // 2)))),
        ("rate", flat(np.where((k >= 3) & (k <= NF - 3), 0.001, 0.0))),
    ):
        at[name] = sum(len(r) for r in rows)
        rows.append(block)
    return np.concatenate(rows).astype(np.float32), at


def chip_order(side):
    hops = lambda d: min(d, side - d)
    way = lambda d: (d > 0) - 2 * (d > side // 2)
    chips = [(x, y) for x in range(side) for y in range(side)][1:]
    chips.sort(key=lambda o: (-(hops(o[0]) + hops(o[1])), 3 * o[0] + 5 * o[1]))
    kinds = {}
    for o in chips:
        kinds.setdefault((way(o[0]), way(o[1])), []).append(o)
    placed = [((i + 0.5) / len(k), o) for k in kinds.values() for i, o in enumerate(k)]
    return [o for _, o in sorted(placed, key=lambda p: p[0])]


def word_of(words, v):
    return jnp.broadcast_to(words[pl.ds(REACH + v, 1), :], (8, 128))


def has(word, i):
    return jnp.bitwise_and(word, 1 << i) != 0


def lanes(tile, index, v):
    index = jnp.broadcast_to(index[pl.ds(v, 1), :], (8, 128))
    return jnp.take_along_axis(tile, index, axis=1, mode="promise_in_bounds")


def near_rows(chunks, words, src, emit, toward_end, bit_order):
    way = 1 if toward_end else -1

    def block(g, carry):
        first = g * UNROLL
        span = [first + way * u if toward_end else first + UNROLL - 1 - u for u in range(UNROLL + 7)]
        for t in range(2):
            word = [word_of(words.at[t], v) for v in span]
            cur = [src[t, FAR + v] for v in span]
            for b in bit_order:
                d = 1 << b
                cur = [
                    jnp.where(has(word[u], b), cur[u + d], cur[u])
                    for u in range(len(cur) - d)
                ]
            for u in range(UNROLL):
                emit(t, u, span[u], cur[u])
        return carry

    lax.fori_loop(0, chunks // UNROLL, block, 0)


def far_rows(chunks, words, tiles, t, r, toward_end, bit_order):
    tiles = tiles + [None] * (chunks // 8 - len(tiles))
    word = [word_of(words.at[t], r + 8 * j) for j in range(chunks // 8)]
    for b in bit_order:
        d = (1 << (b - 3)) * (1 if toward_end else -1)
        moved = []
        for j, own in enumerate(tiles):
            other = tiles[j + d] if 0 <= j + d < len(tiles) else None
            if own is None or other is None:
                moved.append(other if own is None else own)
            else:
                moved.append(jnp.where(has(word[j], b), other, own))
        tiles = moved
    return tiles


def step_kernel(
    n, side, cores, at,
    x_hbm, mask_hbm, speed_hbm, angle_hbm, tab_hbm,
    home, go_right, put,
    x, mask2d, sea_float, speed2d, angle2d, tab, field_a, field_b, stage, shifts, go_left, pick, moved_a, moved_b,
    send, recv, back, flat, energy, rolled, own, low_part, high_part,
    order, send_sem, recv_sem, load_sem, column_sem, first_sem,
):
    bins_dev, cells = x.shape
    half = bins_dev // 2
    chunks = cells // 128
    per_row = NLON // 128
    lat_count = cells // NLON
    me = lax.axis_index("spec")
    my_x, my_y, my_c = me // (side * cores), lax.rem(me // cores, side), lax.rem(me, cores)

    parts = 4
    part_cols = cells // parts
    small = [
        pltpu.make_async_copy(src, dst, load_sem.at[parts + k])
        for k, (src, dst) in enumerate(
            ((mask_hbm, mask2d), (tab_hbm, tab), (speed_hbm, speed2d), (angle_hbm, angle2d))
        )
    ]

    def load(part):
        cols = pl.ds(pl.multiple_of(part * part_cols, 128), part_cols)
        return pltpu.make_async_copy(x_hbm.at[:, cols], x.at[:, cols], load_sem.at[part])

    small[0].start()
    for part in range(parts):
        load(part).start()
    for copy in small[1:]:
        copy.start()

    def wrap(a):
        return jnp.bitwise_and(a, side - 1) if side & (side - 1) == 0 else lax.rem(a, side)

    def hop(u):
        return side // 2 + (1 - 2 * jnp.bitwise_and(u, 1)) * jnp.right_shift(u + 1, 1)

    def both_cores(act, px, py):
        first = (px * side + py) * cores
        act(first + my_c)
        for c in range(1, cores):
            act(first + jnp.where(my_c + c >= cores, my_c + c - cores, my_c + c))

    def own_chip(act):
        for c in range(1, cores):
            act(me - my_c + lax.rem(my_c + c, cores))

    chips = chip_order(side)
    other_rows = [o for o in chips if o[1] != 0]

    def peers(act, which, count):
        def chip(i, carry):
            both_cores(act, wrap(my_x + order[2 * which, i]), wrap(my_y + order[2 * which + 1, i]))
            return carry

        lax.fori_loop(0, count, chip, 0)

    is_first = me == 0
    is_second = me == 1
    below_first = jnp.logical_and(jnp.logical_and(my_x == 0, my_c == 0), my_y != 0)

    def signal(semaphore, to):
        pl.semaphore_signal(semaphore, inc=1, device_id={"spec": to}, device_id_type=MESH)

    def down_column(act):
        def one(u, carry):
            act((my_x * side + wrap(my_y + hop(u))) * cores + my_c)
            return carry

        lax.fori_loop(0, side - 1, one, 0)

    def along_row(act, own=None):
        def one(u, carry):
            both_cores(act, wrap(my_x + hop(u)), my_y)
            return carry

        lax.fori_loop(0, side - 1, one, 0)
        own_chip(act if own is None else own)

    def peers_as_known(act, own):
        along_row(act, own)

        @pl.when(jnp.logical_not(is_first))
        def _():
            def row_in(i, carry):
                pl.semaphore_wait(column_sem.at[wrap(my_y + i)], 1)
                return carry

            @pl.when(jnp.logical_not(below_first))
            def _():
                lax.fori_loop(1, side, row_in, 0)

            @pl.when(is_second)
            def _():
                down_column(lambda to: signal(column_sem.at[0], to - 1))

            @pl.when(below_first)
            def _():
                lax.fori_loop(1, side, row_in, 0)

        peers(act, 1, len(other_rows))

    barrier = pltpu.get_barrier_semaphore()

    @pl.when(jnp.logical_not(is_first))
    def _():
        along_row(lambda to: signal(barrier, to))
        down_column(lambda to: signal(barrier, to))

    def entered():
        called = side * cores + side - 2

        @pl.when(jnp.logical_not(is_first))
        def _():
            with_first = jnp.logical_or(my_y == 0, below_first)
            pl.semaphore_wait(barrier, called - jnp.where(with_first, 1, 0))

            def complete(to):
                @pl.when(to == 0)
                def _():
                    signal(barrier, to)

                @pl.when(to != 0)
                def _():
                    signal(column_sem.at[my_y], to)

            down_column(complete)

    for which, table in enumerate((chips, other_rows)):
        for i, (dx, dy) in enumerate(table):
            order[2 * which, i] = dx
            order[2 * which + 1, i] = dy
    small[0].wait()

    lane = lax.broadcasted_iota(jnp.int32, (8, 128), 1)
    row = lax.broadcasted_iota(jnp.int32, (8, 128), 0)
    low = lane < SEA_DEV

    is_sea = mask2d[...] != 0
    sea_float[...] = mask2d[...].astype(jnp.float32)
    land = jnp.where(is_sea, 0.0, 1.0).astype(jnp.bfloat16)
    earlier = (
        lax.broadcasted_iota(jnp.int32, (128, 128), 0) < lax.broadcasted_iota(jnp.int32, (128, 128), 1)
    ).astype(jnp.bfloat16)
    above = (
        lax.broadcasted_iota(jnp.int32, (chunks, chunks), 1)
        < lax.broadcasted_iota(jnp.int32, (chunks, chunks), 0)
    ).astype(jnp.bfloat16)
    ones = jnp.ones((128, 128), jnp.bfloat16)
    count = functools.partial(jnp.dot, preferred_element_type=jnp.float32)
    before = count(land, earlier).astype(jnp.int32)
    sea_in_row = 128 - count(land, ones).astype(jnp.int32)
    wide_lane = lax.broadcasted_iota(jnp.int32, (chunks, 128), 1)
    wide_row = lax.broadcasted_iota(jnp.int32, (chunks, 128), 0)
    rank0 = wide_row * 128 - count(count(above, land).astype(jnp.bfloat16), ones).astype(jnp.int32)
    put[0] = jnp.bitwise_and(rank0 + wide_lane - before, 127)
    put[1] = jnp.bitwise_and(rank0 + wide_lane - before + SEA_DEV, 127)
    to_go = jnp.where(is_sea, before, 0)
    shifts[chunks:, :] = jnp.zeros((shifts.shape[0] - chunks, 128), jnp.int32)
    go_left[...] = jnp.zeros_like(go_left)
    go_right[...] = jnp.zeros_like(go_right)

    def close_up(i, to_go):
        d = jnp.left_shift(1, i)
        incoming = pltpu.roll(to_go, 128 - d, 1)
        stay = jnp.where(jnp.bitwise_and(to_go, d) != 0, 0, to_go)
        return jnp.where(jnp.bitwise_and(incoming, d) != 0, incoming, stay)

    def plan_rows(to_go):
        nth = jnp.bitwise_and(wide_lane - rank0, 127)
        front = jnp.bitwise_and(wide_lane + to_go, 127)
        took = jnp.take_along_axis(front, nth, axis=1, mode="promise_in_bounds")
        pick[0] = took
        pick[1] = pltpu.roll(took, SEA_DEV, 1)
        up = wide_row - jnp.right_shift(rank0 + nth, 7)
        shifts[0:chunks, :] = jnp.where(nth < sea_in_row, up, 0)
        for b in range(ROW_STEPS):
            here, incoming = shifts[0:chunks, :], shifts[1 << b : chunks + (1 << b), :]
            goes = jnp.bitwise_and(here, 1 << b)
            comes = jnp.bitwise_and(incoming, 1 << b)
            rights, lefts = (goes, comes) if b == 0 else (rights + goes, lefts + comes)
            shifts[0:chunks, :] = jnp.where(comes != 0, incoming, jnp.where(goes != 0, 0, here))
        for words, found in ((go_right, rights), (go_left, lefts)):
            words[0, REACH : REACH + chunks, :] = found
            words[1, REACH : REACH + chunks, :] = pltpu.roll(found, SEA_DEV, 1)

    zero = jnp.zeros((8, 128), jnp.float32)
    pad = per_row
    for t in range(2):
        for v in range(pad):
            for f in (field_a, field_b):
                f[t, v] = zero
                f[t, pad + chunks + v] = zero
    base = (me * bins_dev) % ND
    for copy in small[1:]:
        copy.wait()
    pace_x, pace_y, from_west, from_south, beside, edge = [], [], [], [], [], []
    for t in range(2):
        k = ((me * bins_dev + jnp.minimum(2 * row + t, bins_dev - 1)) // ND).astype(jnp.float32)
        pace = 0.2 * jnp.exp(-LOG_RATIO * k)
        ax = pace * tab[pl.ds(at["cos"] + base + t, 8, stride=2), :]
        ay = pace * tab[pl.ds(at["sin"] + base + t, 8, stride=2), :]
        pace_x.append(jnp.abs(ax))
        pace_y.append(jnp.abs(ay))
        from_west.append(ax >= 0.0)
        from_south.append(ay >= 0.0)
        beside.append(jnp.bitwise_and(jnp.where(from_west[t], lane - 1, lane + 1), 127))
        edge.append(
            (
                jnp.logical_and(from_west[t], lane == 0),
                jnp.logical_and(jnp.logical_not(from_west[t]), lane == 127),
            )
        )

    def split_bins(g, carry):
        for u in range(8):
            v = g * 8 + u
            cols = pl.ds(pl.multiple_of(v * 128, 128), 128)
            stage[u, 0:bins_dev, :] = x[:, cols] * sea_float[pl.ds(v, 1), :]
            for t in range(2):
                field_a[t, pad + v, 0:half, :] = stage[u, pl.ds(t, half, stride=2), :]
        return carry

    def split_part(part, carry):
        load(part).wait()
        per_part = chunks // 8 // parts
        return lax.fori_loop(part * per_part, (part + 1) * per_part, split_bins, carry)

    lax.fori_loop(0, parts, split_part, 0)

    for s in range(SUBSTEPS):
        src, dst = (field_a, field_b) if s % 2 == 0 else (field_b, field_a)

        def advance(g, to_go, src=src, dst=dst, s=s):
            if s == 0:
                to_go = close_up(2 * g + 1, close_up(2 * g, to_go))
            for ru in range(8):
                r = g * 8 + ru
                widen = tab[pl.ds(at["widen"] + r, 1), :]
                first = pad + r * per_row
                for t in range(2):
                    side_c = pace_x[t] * widen
                    own_c = 1.0 - side_c - pace_y[t]
                    first = pad + r * per_row
                    e = [src[t, first + q] for q in range(per_row)]
                    turned = [jnp.take_along_axis(a, beside[t], axis=1, mode="promise_in_bounds") for a in e]
                    for q in range(per_row):
                        across = jnp.where(edge[t][0], turned[q - 1], turned[q])
                        across = jnp.where(edge[t][1], turned[(q + 1) % per_row], across)
                        along = jnp.where(
                            from_south[t], src[t, first + q - per_row], src[t, first + q + per_row]
                        )
                        new = own_c * e[q] + side_c * across + pace_y[t] * along
                        v = first + q - pad
                        if s < SUBSTEPS - 1:
                            dst[t, first + q] = new * sea_float[pl.ds(v, 1), :]
                        else:
                            wind = (speed2d, angle2d)[t][pl.ds(v, 1), :]
                            dst[t, first + q] = jnp.where(row == half, wind, new)
            return to_go

        to_go = lax.fori_loop(0, lat_count // 8, advance, to_go)
        if s == 0:
            plan_rows(to_go)
    final = field_a if SUBSTEPS % 2 == 0 else field_b
    entered()

    def to_lanes(g, carry):
        for u in range(2 * UNROLL):
            v = g * 2 * UNROLL + u
            for t in range(2):
                moved_a[t, FAR + v] = lanes(final[t, pad + v], pick.at[t], v)
        return carry

    lax.fori_loop(0, chunks // (2 * UNROLL), to_lanes, 0)


    def keep_near(t, u, v, tile):
        moved_b[t, FAR + v] = tile

    near_rows(chunks, go_left, moved_a, keep_near, True, (0, 1, 2))

    def pack(r, carry):
        even, odd = (
            far_rows(
                chunks, go_left, [moved_b[t, FAR + r + 8 * j] for j in range(chunks // 8)], t, r, True, (3, 4, 5)
            )
            for t in range(2)
        )
        for j in range(n * SEA_DEV // 128 // 8):
            v = r + 8 * j
            send[2 * v] = jnp.where(low, even[j], odd[j])
            send[2 * v + 1] = jnp.where(low, odd[j], even[j])
        return carry

    lax.fori_loop(0, 8, pack, 0)

    def finish(ref, count, rows, sem):
        part = ref.at[pl.ds(0, count), pl.ds(0, rows)]
        pltpu.make_async_copy(part, part, sem).wait()

    def copy_to(to, src, dst, k, arrival):
        pltpu.make_async_remote_copy(
            src_ref=src,
            dst_ref=dst,
            send_sem=send_sem.at[k],
            recv_sem=arrival,
            device_id={"spec": to},
            device_id_type=MESH,
        ).start()

    def own_message(src, dst, rows, arrival):
        pltpu.make_async_copy(src.at[me, pl.ds(0, rows)], dst.at[me, pl.ds(0, rows)], arrival).start()

    @pl.when(is_first)
    def _():
        pl.semaphore_wait(barrier, side * cores + 2 * side - 3)
        signal(first_sem, 1)

    def push(to):
        aside = jnp.where(to == 0, 1, 0)
        copy_to(
            to + aside,
            send.at[to, pl.ds(0, half)],
            recv.at[me + aside * n, pl.ds(0, half)],
            0,
            recv_sem.at[my_x + aside * side],
        )

    def push_own_chip(to):
        @pl.when(is_second)
        def _():
            pltpu.make_async_copy(
                send.at[0, pl.ds(0, half)], recv.at[n + 1, pl.ds(0, half)], recv_sem.at[side]
            ).start()

        @pl.when(jnp.logical_not(is_second))
        def _():
            copy_to(to, send.at[to, pl.ds(0, half)], recv.at[me, pl.ds(0, half)], 0, recv_sem.at[my_x])

    peers_as_known(push, push_own_chip)
    own_message(send, recv, half, recv_sem.at[my_x])

    @pl.when(is_second)
    def _():
        pl.semaphore_wait(first_sem, 1)

    def hand_over(h):
        def pass_on(start, count):
            finish(recv, count, half, recv_sem.at[side + h])
            copy_to(
                0,
                recv.at[pl.ds(n + start, count), pl.ds(0, half)],
                recv.at[pl.ds(start, count), pl.ds(0, half)],
                2,
                recv_sem.at[h],
            )

        @pl.when(jnp.logical_and(is_second, h != 0))
        def _():
            pass_on(h * side * cores, side * cores)

        @pl.when(jnp.logical_and(is_second, h == 0))
        def _():
            pass_on(1, side * cores - 1)


    wind = send[me][half : half + 1, :]
    other = pltpu.roll(wind, SEA_DEV, 1)
    odd_side = lax.rem(me, 2) * SEA_DEV
    even_half = lambda shape: jnp.bitwise_xor(lax.broadcasted_iota(jnp.int32, shape, 1), odd_side) < SEA_DEV
    low16 = even_half((PAIRS, 128))
    speed = jnp.where(even_half((1, 128)), wind, other)
    angle = jnp.where(even_half((1, 128)), other, wind)

    def paired(name):
        rows = tab[at[name] : at[name] + PAIRS, :]
        return jnp.where(odd_side == 0, rows, pltpu.roll(rows, SEA_DEV, 1))

    toward = speed * (paired("pair_cos") * jnp.cos(angle) + paired("pair_sin") * jnp.sin(angle))
    zero16 = jnp.zeros((PAIRS, 128), jnp.float32)
    for w in range(4):
        for k in (0, 1, 2, NF + 3, NF + 4):
            rolled[w, k] = zero16
    for k in range(2):
        low_part[k] = zero16
    for k in range(3):
        high_part[NF + k] = zero16

    def turns(a, amounts):
        s = pltpu.roll(a, SEA_DEV, 1)
        need = {1: (1, 0), -1: (0, -1), 3: (2, 1), -3: (-1, -2)}
        by = {0: s}
        for m in amounts:
            for w in need[m]:
                if w not in by:
                    by[w] = pltpu.roll(s, w % PAIRS, 0)
        return [jnp.where(low16, by[need[m][0]], by[need[m][1]]) for m in amounts]

    group = 8
    per_group = half * group // PAIRS

    def arrange(i, carry):
        m0, m1 = carry
        h = lax.rem(i + 1, side)
        hand_over(h)
        finish(recv, side * cores, half, recv_sem.at[h])
        for g in (2 * h, 2 * h + 1):
            for i in range(group):
                flat[g, half * i : half * i + half, :] = recv[g * group + i, 0:half, :]
        for g in (2 * h, 2 * h + 1):
            for q in range(per_group):
                k = g * per_group + q
                a = flat[g, PAIRS * q : PAIRS * (q + 1), :]
                energy[k] = a
                m0 = m0 + a
                m1 = m1 + tab[pl.ds(at["omega"] + k, 1), :] * a
                for w, b in enumerate(turns(a, (1, -1, 3, -3))):
                    rolled[w, k + 3] = b
        return m0, m1

    m0, m1 = lax.fori_loop(0, side, arrange, (zero16, zero16))

    def over_bins(a):
        a = jnp.sum(a, axis=0, keepdims=True)
        return (a + pltpu.roll(a, SEA_DEV, 1)) * (1.0 / (NF * ND))

    m0, m1 = over_bins(m0), over_bins(m1)
    mean_freq = m1 / (m0 + 1e-6)
    steep = m0 * mean_freq * mean_freq
    breaking = steep * steep / (1.0 + steep * steep)

    def transfer(g, carry):
        for q in range(4 * per_group):
            k = g * 4 * per_group + q
            a = energy[k]
            factor = tab[pl.ds(at["rate"] + k, 1), :] * a
            rates = []
            for plus, minus in ((rolled[1, k + 5], rolled[2, k]), (rolled[0, k + 5], rolled[3, k])):
                rates.append(factor * (a * (plus + minus) - 2.0 * plus * minus))
            up, down = turns(rates[0], (1, -3)), turns(rates[1], (-1, 3))
            own[k] = -2.0 * (rates[0] + rates[1])
            low_part[k + 2] = up[0] + down[0]
            high_part[k] = up[1] + down[1]
        return carry

    lax.fori_loop(0, n // group // 4, transfer, 0)

    def renew(g, total):
        for q in range(per_group):
            k = g * per_group + q
            a = energy[k]
            omega = tab[pl.ds(at["omega"] + k, 1), :]
            gain = (0.05 * omega) * jnp.maximum(0.0, omega * toward - 1.0)
            new = a + (gain - (0.03 * omega) * breaking) * a
            new = new + own[k] + low_part[k] + high_part[k + 3]
            total = total + new
            flat[g, PAIRS * q : PAIRS * (q + 1), :] = new
        for i in range(group):
            back[g * group + i, 0:half, :] = flat[g, half * i : half * i + half, :]
        return total

    total = lax.fori_loop(0, n // group, renew, zero16)
    height = 4.0 * jnp.sqrt(over_bins(total) + 1e-6)

    def add_height(g, carry):
        for i in range(group):
            back[g * group + i, half : half + 1, :] = height
        return carry

    lax.fori_loop(0, n // group, add_height, 0)

    def push_back(to):
        copy_to(
            to,
            back.at[to, pl.ds(0, half + 1)],
            home.at[me, pl.ds(0, half + 1)],
            1,
            recv_sem.at[2 * side],
        )

    peers(push_back, 0, len(chips))
    own_chip(push_back)
    own_message(back, home, half + 1, recv_sem.at[2 * side])

    @pl.when(is_second)
    def _():
        finish(send, n - 2, half, send_sem.at[0])
        finish(recv, n - 1, half, send_sem.at[2])

    @pl.when(jnp.logical_not(is_second))
    def _():
        finish(send, n - 1, half, send_sem.at[0])

    finish(home, n, half + 1, recv_sem.at[2 * side])
    finish(back, n - 1, half + 1, send_sem.at[1])


def unpack_kernel(
    n, bins_dev,
    home, go_right, put, mask2d,
    out, height_out, mean_out,
    moved_a, moved_b, stage, heights, result, own_heights, mean, write_sem,
):
    chunks = mask2d.shape[0]
    half = bins_dev // 2
    cells = chunks * 128
    per_row = NLON // 128
    me = lax.axis_index("spec")
    lane = lax.broadcasted_iota(jnp.int32, (8, 128), 1)
    low = lane < SEA_DEV

    def spread(r, carry):
        pairs = [(home[2 * (r + 8 * j)], home[2 * (r + 8 * j) + 1]) for j in range(n * SEA_DEV // 128 // 8)]
        for t in range(2):
            tiles = [jnp.where(low, p[t], p[1 - t]) for p in pairs]
            for j, tile in enumerate(far_rows(chunks, go_right, tiles, t, r, False, (5, 4, 3))):
                moved_b[t, FAR + r + 8 * j] = tile
        return carry

    lax.fori_loop(0, 8, spread, 0)

    def keep_apart(t, u, v, tile):
        moved_a[t, FAR + v] = tile

    near_rows(chunks, go_right, moved_b, keep_apart, False, (2, 1, 0))

    width = 2 * UNROLL * 128

    def write(g):
        cols = pl.ds(pl.multiple_of(g * width, 128), width)
        return pltpu.make_async_copy(result.at[:, cols], out.at[:, cols], write_sem.at[g])

    def deliver(g, carry):
        for u in range(2 * UNROLL):
            v = g * 2 * UNROLL + u
            sea = jnp.broadcast_to(mask2d[pl.ds(v, 1), :] != 0, (8, 128))
            for t in range(2):
                tile = jnp.where(sea, lanes(moved_a[t, FAR + v], put.at[t], v), 0.0)
                stage[u, pl.ds(t, half, stride=2), :] = tile[0:half]
                if t == 0:
                    heights[pl.ds(v, 1), :] = tile[half : half + 1]
        for u in range(2 * UNROLL):
            v = g * 2 * UNROLL + u
            result[:, pl.ds(pl.multiple_of(v * 128, 128), 128)] = stage[u, 0:bins_dev, :]
        write(g).start()
        return carry

    lax.fori_loop(0, chunks // (2 * UNROLL), deliver, 0)

    points = cells // n
    together = NLON // points
    start = me // together * per_row
    three = [heights[pl.ds(start + q, 1), :] for q in range(per_row)]
    u = lax.rem(me, together)
    picked = None
    for g in range(together):
        first, offset = g * points // 128, g * points % 128
        piece = three[first]
        if offset:
            after = three[min(first + 1, per_row - 1)]
            piece = jnp.where(
                lane[0:1] < 128 - offset,
                pltpu.roll(piece, 128 - offset, 1),
                pltpu.roll(after, 128 - offset, 1),
            )
        picked = piece if picked is None else jnp.where(u == g, piece, picked)
    own_heights[...] = picked[:, 0:points]
    all_heights = jnp.sum(heights[...], axis=0, keepdims=True)
    mean[...] = jnp.sum(all_heights, axis=1, keepdims=True) * (1.0 / (SEA_DEV * n))

    small = (
        pltpu.make_async_copy(own_heights, height_out, write_sem.at[cells // width]),
        pltpu.make_async_copy(mean, mean_out, write_sem.at[cells // width + 1]),
    )
    for copy in small:
        copy.start()

    def written(g, carry):
        write(g).wait()
        return carry

    lax.fori_loop(0, cells // width, written, 0)
    for copy in small:
        copy.wait()


def solution(mesh):
    n = mesh.shape["spec"]
    cores = 2
    side = math.isqrt(n // cores)

    def local(spectrum, sea_mask, wind_speed, wind_angle):
        bins_dev, cells = spectrum.shape
        chunks = cells // 128
        padded = chunks + 2 * (NLON // 128)
        tab, at = tables(cells // NLON)
        vmem = pl.BlockSpec(memory_space=pltpu.VMEM)
        words = pltpu.VMEM((2, chunks + 2 * REACH, 128), jnp.int32)
        by_freq = lambda *dims: pltpu.VMEM((*dims, PAIRS, 128), jnp.float32)
        messages = lambda count: pltpu.VMEM((count, 8, 128), jnp.float32)
        home, go_right, put = pl.pallas_call(
            functools.partial(step_kernel, n, side, cores, at),
            name="wave_step",
            out_shape=(
                jax.ShapeDtypeStruct((n, 8, 128), jnp.float32),
                jax.ShapeDtypeStruct((2, chunks + 2 * REACH, 128), jnp.int32),
                jax.ShapeDtypeStruct((2, chunks, 128), jnp.int32),
            ),
            in_specs=[pl.BlockSpec(memory_space=pltpu.HBM)] * 5,
            out_specs=(vmem,) * 3,
            scratch_shapes=[
                pltpu.VMEM((bins_dev, cells), jnp.float32),
                pltpu.VMEM((chunks, 128), jnp.int32),
                pltpu.VMEM((chunks, 128), jnp.float32),
                pltpu.VMEM((chunks, 128), jnp.float32),
                pltpu.VMEM((chunks, 128), jnp.float32),
                pltpu.VMEM(tab.shape, jnp.float32),
                pltpu.VMEM((2, padded, 8, 128), jnp.float32),
                pltpu.VMEM((2, padded, 8, 128), jnp.float32),
                pltpu.VMEM((8, 16, 128), jnp.float32),
                pltpu.VMEM((chunks + REACH, 128), jnp.int32),
                words,
                pltpu.VMEM((2, chunks, 128), jnp.int32),
                pltpu.VMEM((2, chunks + 2 * FAR, 8, 128), jnp.float32),
                pltpu.VMEM((2, chunks + 2 * FAR, 8, 128), jnp.float32),
                messages(n),
                messages(2 * n),
                messages(n),
                pltpu.VMEM((n // 8, 8 * bins_dev // 2, 128), jnp.float32),
                by_freq(NF),
                by_freq(4, NF + 5),
                by_freq(NF),
                by_freq(NF + 2),
                by_freq(NF + 3),
                pltpu.SMEM((4, side * side), jnp.int32),
                pltpu.SemaphoreType.DMA((3,)),
                pltpu.SemaphoreType.DMA((2 * side + 1,)),
                pltpu.SemaphoreType.DMA((8,)),
                pltpu.SemaphoreType.REGULAR((side,)),
                pltpu.SemaphoreType.REGULAR,
            ],
            compiler_params=pltpu.CompilerParams(
                collective_id=0, has_side_effects=True, vmem_limit_bytes=VMEM_BYTES
            ),
        )(
            *(
                pltpu.with_memory_space_constraint(a, pltpu.HBM)
                for a in (
                    spectrum,
                    sea_mask.reshape(chunks, 128),
                    wind_speed.reshape(chunks, 128),
                    wind_angle.reshape(chunks, 128),
                    jnp.asarray(tab),
                )
            )
        )
        moved = pltpu.VMEM((2, chunks + 2 * FAR, 8, 128), jnp.float32)
        new_spectrum, height, mean = pl.pallas_call(
            functools.partial(unpack_kernel, n, bins_dev),
            name="unpack",
            out_shape=(
                jax.ShapeDtypeStruct((bins_dev, cells), jnp.float32),
                jax.ShapeDtypeStruct((1, cells // n), jnp.float32),
                jax.ShapeDtypeStruct((1, 1), jnp.float32),
            ),
            in_specs=[vmem] * 4,
            out_specs=(pl.BlockSpec(memory_space=pl.ANY),) * 3,
            scratch_shapes=[
                moved,
                moved,
                pltpu.VMEM((16, 16, 128), jnp.float32),
                pltpu.VMEM((chunks, 128), jnp.float32),
                pltpu.VMEM((bins_dev, cells), jnp.float32),
                pltpu.VMEM((1, cells // n), jnp.float32),
                pltpu.VMEM((1, 1), jnp.float32),
                pltpu.SemaphoreType.DMA((chunks // (2 * UNROLL) + 2,)),
            ],
            compiler_params=pltpu.CompilerParams(vmem_limit_bytes=VMEM_BYTES),
        )(home, go_right, put, sea_mask.reshape(chunks, 128))
        return new_spectrum, height.reshape(-1), mean.reshape(1)

    return jax.shard_map(
        local,
        mesh=mesh,
        in_specs=(P(("grp", "spec"), None), P(), P("grp"), P("grp")),
        out_specs=(P(("grp", "spec"), None), P(("grp", "spec")), P("grp")),
        check_vma=False,
    )
```

```python
import functools
import math

import jax
import jax.numpy as jnp
import numpy as np
from jax import lax
from jax.experimental import pallas as pl
from jax.experimental.pallas import tpu as pltpu
from jax.sharding import PartitionSpec as P

NF = 48
ND = 32
NLON = 384
SUBSTEPS = 2
SEA_DEV = 64
MESH = pl.DeviceIdType.MESH
LOG_RATIO = math.log(1.1)
PAIRS = ND // 2
ROW_STEPS = 6
REACH = 32
UNROLL = 8
VMEM_BYTES = 24 * 1024 * 1024
FAR = 56


def tables(lat_count):
    heading = 2.0 * np.pi * (np.arange(ND) + 0.5) / ND
    wrapped = np.concatenate([heading, heading[:24]])
    flat = lambda a: np.repeat(np.asarray(a)[:, None], 128, 1)
    paired = np.repeat(heading.reshape(PAIRS, 2), SEA_DEV, axis=1)
    latitude = np.radians(-75.0 + 150.0 * (np.arange(lat_count) + 0.5) / lat_count)
    k = np.arange(NF)
    rows, at = [], {}
    for name, block in (
        ("cos", flat(np.cos(wrapped))),
        ("sin", flat(np.sin(wrapped))),
        ("pair_cos", np.cos(paired)),
        ("pair_sin", np.sin(paired)),
        ("widen", flat(1.0 / np.cos(latitude))),
        ("omega", flat(np.exp(LOG_RATIO * (k - NF // 2)))),
        ("rate", flat(np.where((k >= 3) & (k <= NF - 3), 0.001, 0.0))),
    ):
        at[name] = sum(len(r) for r in rows)
        rows.append(block)
    return np.concatenate(rows).astype(np.float32), at


def chip_order(side):
    hops = lambda d: min(d, side - d)
    way = lambda d: (d > 0) - 2 * (d > side // 2)
    chips = [(x, y) for x in range(side) for y in range(side)][1:]
    chips.sort(key=lambda o: (-(hops(o[0]) + hops(o[1])), 3 * o[0] + 5 * o[1]))
    kinds = {}
    for o in chips:
        kinds.setdefault((way(o[0]), way(o[1])), []).append(o)
    placed = [((i + 0.5) / len(k), o) for k in kinds.values() for i, o in enumerate(k)]
    return [o for _, o in sorted(placed, key=lambda p: p[0])]


def word_of(words, v):
    return jnp.broadcast_to(words[pl.ds(REACH + v, 1), :], (8, 128))


def has(word, i):
    return jnp.bitwise_and(word, 1 << i) != 0


def lanes(tile, index, v):
    index = jnp.broadcast_to(index[pl.ds(v, 1), :], (8, 128))
    return jnp.take_along_axis(tile, index, axis=1, mode="promise_in_bounds")


def near_rows(chunks, words, src, emit, toward_end, bit_order):
    way = 1 if toward_end else -1

    def block(g, carry):
        first = g * UNROLL
        span = [first + way * u if toward_end else first + UNROLL - 1 - u for u in range(UNROLL + 7)]
        for t in range(2):
            word = [word_of(words.at[t], v) for v in span]
            cur = [src[t, FAR + v] for v in span]
            for b in bit_order:
                d = 1 << b
                cur = [
                    jnp.where(has(word[u], b), cur[u + d], cur[u])
                    for u in range(len(cur) - d)
                ]
            for u in range(UNROLL):
                emit(t, u, span[u], cur[u])
        return carry

    lax.fori_loop(0, chunks // UNROLL, block, 0)


def far_rows(chunks, words, tiles, t, r, toward_end, bit_order):
    tiles = tiles + [None] * (chunks // 8 - len(tiles))
    word = [word_of(words.at[t], r + 8 * j) for j in range(chunks // 8)]
    for b in bit_order:
        d = (1 << (b - 3)) * (1 if toward_end else -1)
        moved = []
        for j, own in enumerate(tiles):
            other = tiles[j + d] if 0 <= j + d < len(tiles) else None
            if own is None or other is None:
                moved.append(other if own is None else own)
            else:
                moved.append(jnp.where(has(word[j], b), other, own))
        tiles = moved
    return tiles


def step_kernel(
    n, side, cores, at,
    x_hbm, mask_hbm, speed_hbm, angle_hbm, tab_hbm,
    home, go_right, put,
    x, mask2d, sea_float, speed2d, angle2d, tab, field_a, field_b, stage, shifts, go_left, pick, moved_a, moved_b,
    send, recv, back, flat, energy, rolled, own, low_part, high_part,
    order, send_sem, recv_sem, load_sem, column_sem, first_sem,
):
    bins_dev, cells = x.shape
    half = bins_dev // 2
    chunks = cells // 128
    per_row = NLON // 128
    lat_count = cells // NLON
    me = lax.axis_index("spec")
    my_x, my_y, my_c = me // (side * cores), lax.rem(me // cores, side), lax.rem(me, cores)

    parts = 4
    part_cols = cells // parts
    small = [
        pltpu.make_async_copy(src, dst, load_sem.at[parts + k])
        for k, (src, dst) in enumerate(
            ((mask_hbm, mask2d), (tab_hbm, tab), (speed_hbm, speed2d), (angle_hbm, angle2d))
        )
    ]

    def load(part):
        cols = pl.ds(pl.multiple_of(part * part_cols, 128), part_cols)
        return pltpu.make_async_copy(x_hbm.at[:, cols], x.at[:, cols], load_sem.at[part])

    small[0].start()
    for part in range(parts):
        load(part).start()
    for copy in small[1:]:
        copy.start()

    def wrap(a):
        return jnp.bitwise_and(a, side - 1) if side & (side - 1) == 0 else lax.rem(a, side)

    def hop(u):
        return side // 2 + (1 - 2 * jnp.bitwise_and(u, 1)) * jnp.right_shift(u + 1, 1)

    def both_cores(act, px, py):
        first = (px * side + py) * cores
        act(first + my_c)
        for c in range(1, cores):
            act(first + jnp.where(my_c + c >= cores, my_c + c - cores, my_c + c))

    def own_chip(act):
        for c in range(1, cores):
            act(me - my_c + lax.rem(my_c + c, cores))

    chips = chip_order(side)
    other_rows = [o for o in chips if o[1] != 0]

    def peers(act, which, count):
        def chip(i, carry):
            both_cores(act, wrap(my_x + order[2 * which, i]), wrap(my_y + order[2 * which + 1, i]))
            return carry

        lax.fori_loop(0, count, chip, 0)

    is_first = me == 0
    is_second = me == 1
    below_first = jnp.logical_and(jnp.logical_and(my_x == 0, my_c == 0), my_y != 0)

    def signal(semaphore, to):
        pl.semaphore_signal(semaphore, inc=1, device_id={"spec": to}, device_id_type=MESH)

    def down_column(act):
        def one(u, carry):
            act((my_x * side + wrap(my_y + hop(u))) * cores + my_c)
            return carry

        lax.fori_loop(0, side - 1, one, 0)

    def along_row(act, own=None):
        def one(u, carry):
            both_cores(act, wrap(my_x + hop(u)), my_y)
            return carry

        lax.fori_loop(0, side - 1, one, 0)
        own_chip(act if own is None else own)

    def peers_as_known(act, own):
        along_row(act, own)

        @pl.when(jnp.logical_not(is_first))
        def _():
            def row_in(i, carry):
                pl.semaphore_wait(column_sem.at[wrap(my_y + i)], 1)
                return carry

            @pl.when(jnp.logical_not(below_first))
            def _():
                lax.fori_loop(1, side, row_in, 0)

            @pl.when(is_second)
            def _():
                down_column(lambda to: signal(column_sem.at[0], to - 1))

            @pl.when(below_first)
            def _():
                lax.fori_loop(1, side, row_in, 0)

        peers(act, 1, len(other_rows))

    barrier = pltpu.get_barrier_semaphore()

    @pl.when(jnp.logical_not(is_first))
    def _():
        along_row(lambda to: signal(barrier, to))
        down_column(lambda to: signal(barrier, to))

    def entered():
        called = side * cores + side - 2

        @pl.when(jnp.logical_not(is_first))
        def _():
            with_first = jnp.logical_or(my_y == 0, below_first)
            pl.semaphore_wait(barrier, called - jnp.where(with_first, 1, 0))

            def complete(to):
                @pl.when(to == 0)
                def _():
                    signal(barrier, to)

                @pl.when(to != 0)
                def _():
                    signal(column_sem.at[my_y], to)

            down_column(complete)

    for which, table in enumerate((chips, other_rows)):
        for i, (dx, dy) in enumerate(table):
            order[2 * which, i] = dx
            order[2 * which + 1, i] = dy
    small[0].wait()

    lane = lax.broadcasted_iota(jnp.int32, (8, 128), 1)
    row = lax.broadcasted_iota(jnp.int32, (8, 128), 0)
    low = lane < SEA_DEV

    is_sea = mask2d[...] != 0
    sea_float[...] = mask2d[...].astype(jnp.float32)
    land = jnp.where(is_sea, 0.0, 1.0).astype(jnp.bfloat16)
    earlier = (
        lax.broadcasted_iota(jnp.int32, (128, 128), 0) < lax.broadcasted_iota(jnp.int32, (128, 128), 1)
    ).astype(jnp.bfloat16)
    above = (
        lax.broadcasted_iota(jnp.int32, (chunks, chunks), 1)
        < lax.broadcasted_iota(jnp.int32, (chunks, chunks), 0)
    ).astype(jnp.bfloat16)
    ones = jnp.ones((128, 128), jnp.bfloat16)
    count = functools.partial(jnp.dot, preferred_element_type=jnp.float32)
    before = count(land, earlier).astype(jnp.int32)
    sea_in_row = 128 - count(land, ones).astype(jnp.int32)
    wide_lane = lax.broadcasted_iota(jnp.int32, (chunks, 128), 1)
    wide_row = lax.broadcasted_iota(jnp.int32, (chunks, 128), 0)
    rank0 = wide_row * 128 - count(count(above, land).astype(jnp.bfloat16), ones).astype(jnp.int32)
    put[0] = jnp.bitwise_and(rank0 + wide_lane - before, 127)
    put[1] = jnp.bitwise_and(rank0 + wide_lane - before + SEA_DEV, 127)
    to_go = jnp.where(is_sea, before, 0)
    shifts[chunks:, :] = jnp.zeros((shifts.shape[0] - chunks, 128), jnp.int32)
    go_left[...] = jnp.zeros_like(go_left)
    go_right[...] = jnp.zeros_like(go_right)

    def close_up(i, to_go):
        d = jnp.left_shift(1, i)
        incoming = pltpu.roll(to_go, 128 - d, 1)
        stay = jnp.where(jnp.bitwise_and(to_go, d) != 0, 0, to_go)
        return jnp.where(jnp.bitwise_and(incoming, d) != 0, incoming, stay)

    def plan_rows(to_go):
        nth = jnp.bitwise_and(wide_lane - rank0, 127)
        front = jnp.bitwise_and(wide_lane + to_go, 127)
        took = jnp.take_along_axis(front, nth, axis=1, mode="promise_in_bounds")
        pick[0] = took
        pick[1] = pltpu.roll(took, SEA_DEV, 1)
        up = wide_row - jnp.right_shift(rank0 + nth, 7)
        shifts[0:chunks, :] = jnp.where(nth < sea_in_row, up, 0)
        for b in range(ROW_STEPS):
            here, incoming = shifts[0:chunks, :], shifts[1 << b : chunks + (1 << b), :]
            goes = jnp.bitwise_and(here, 1 << b)
            comes = jnp.bitwise_and(incoming, 1 << b)
            rights, lefts = (goes, comes) if b == 0 else (rights + goes, lefts + comes)
            shifts[0:chunks, :] = jnp.where(comes != 0, incoming, jnp.where(goes != 0, 0, here))
        for words, found in ((go_right, rights), (go_left, lefts)):
            words[0, REACH : REACH + chunks, :] = found
            words[1, REACH : REACH + chunks, :] = pltpu.roll(found, SEA_DEV, 1)

    zero = jnp.zeros((8, 128), jnp.float32)
    pad = per_row
    for t in range(2):
        for v in range(pad):
            for f in (field_a, field_b):
                f[t, v] = zero
                f[t, pad + chunks + v] = zero
    base = (me * bins_dev) % ND
    for copy in small[1:]:
        copy.wait()
    pace_x, pace_y, from_west, from_south, beside, edge = [], [], [], [], [], []
    for t in range(2):
        k = ((me * bins_dev + jnp.minimum(2 * row + t, bins_dev - 1)) // ND).astype(jnp.float32)
        pace = 0.2 * jnp.exp(-LOG_RATIO * k)
        ax = pace * tab[pl.ds(at["cos"] + base + t, 8, stride=2), :]
        ay = pace * tab[pl.ds(at["sin"] + base + t, 8, stride=2), :]
        pace_x.append(jnp.abs(ax))
        pace_y.append(jnp.abs(ay))
        from_west.append(ax >= 0.0)
        from_south.append(ay >= 0.0)
        beside.append(jnp.bitwise_and(jnp.where(from_west[t], lane - 1, lane + 1), 127))
        edge.append(
            (
                jnp.logical_and(from_west[t], lane == 0),
                jnp.logical_and(jnp.logical_not(from_west[t]), lane == 127),
            )
        )

    def split_bins(g, carry):
        for u in range(8):
            v = g * 8 + u
            cols = pl.ds(pl.multiple_of(v * 128, 128), 128)
            stage[u, 0:bins_dev, :] = x[:, cols] * sea_float[pl.ds(v, 1), :]
            for t in range(2):
                field_a[t, pad + v, 0:half, :] = stage[u, pl.ds(t, half, stride=2), :]
        return carry

    def split_part(part, carry):
        load(part).wait()
        per_part = chunks // 8 // parts
        return lax.fori_loop(part * per_part, (part + 1) * per_part, split_bins, carry)

    lax.fori_loop(0, parts, split_part, 0)

    for s in range(SUBSTEPS):
        src, dst = (field_a, field_b) if s % 2 == 0 else (field_b, field_a)

        def advance(g, to_go, src=src, dst=dst, s=s):
            if s == 0:
                to_go = close_up(2 * g + 1, close_up(2 * g, to_go))
            for ru in range(8):
                r = g * 8 + ru
                widen = tab[pl.ds(at["widen"] + r, 1), :]
                first = pad + r * per_row
                for t in range(2):
                    side_c = pace_x[t] * widen
                    own_c = 1.0 - side_c - pace_y[t]
                    first = pad + r * per_row
                    e = [src[t, first + q] for q in range(per_row)]
                    turned = [jnp.take_along_axis(a, beside[t], axis=1, mode="promise_in_bounds") for a in e]
                    for q in range(per_row):
                        across = jnp.where(edge[t][0], turned[q - 1], turned[q])
                        across = jnp.where(edge[t][1], turned[(q + 1) % per_row], across)
                        along = jnp.where(
                            from_south[t], src[t, first + q - per_row], src[t, first + q + per_row]
                        )
                        new = own_c * e[q] + side_c * across + pace_y[t] * along
                        v = first + q - pad
                        if s < SUBSTEPS - 1:
                            dst[t, first + q] = new * sea_float[pl.ds(v, 1), :]
                        else:
                            wind = (speed2d, angle2d)[t][pl.ds(v, 1), :]
                            dst[t, first + q] = jnp.where(row == half, wind, new)
            return to_go

        to_go = lax.fori_loop(0, lat_count // 8, advance, to_go)
        if s == 0:
            plan_rows(to_go)
    final = field_a if SUBSTEPS % 2 == 0 else field_b
    entered()

    def to_lanes(g, carry):
        for u in range(4 * UNROLL):
            v = g * 4 * UNROLL + u
            for t in range(2):
                moved_a[t, FAR + v] = lanes(final[t, pad + v], pick.at[t], v)
        return carry

    lax.fori_loop(0, chunks // (4 * UNROLL), to_lanes, 0)


    def keep_near(t, u, v, tile):
        moved_b[t, FAR + v] = tile

    near_rows(chunks, go_left, moved_a, keep_near, True, (0, 1, 2))

    def pack(r, carry):
        even, odd = (
            far_rows(
                chunks, go_left, [moved_b[t, FAR + r + 8 * j] for j in range(chunks // 8)], t, r, True, (3, 4, 5)
            )
            for t in range(2)
        )
        for j in range(n * SEA_DEV // 128 // 8):
            v = r + 8 * j
            send[2 * v] = jnp.where(low, even[j], odd[j])
            send[2 * v + 1] = jnp.where(low, odd[j], even[j])
        return carry

    lax.fori_loop(0, 8, pack, 0)

    def finish(ref, count, rows, sem):
        part = ref.at[pl.ds(0, count), pl.ds(0, rows)]
        pltpu.make_async_copy(part, part, sem).wait()

    def copy_to(to, src, dst, k, arrival):
        pltpu.make_async_remote_copy(
            src_ref=src,
            dst_ref=dst,
            send_sem=send_sem.at[k],
            recv_sem=arrival,
            device_id={"spec": to},
            device_id_type=MESH,
        ).start()

    def own_message(src, dst, rows, arrival):
        pltpu.make_async_copy(src.at[me, pl.ds(0, rows)], dst.at[me, pl.ds(0, rows)], arrival).start()

    @pl.when(is_first)
    def _():
        pl.semaphore_wait(barrier, side * cores + 2 * side - 3)
        signal(first_sem, 1)

    def push(to):
        aside = jnp.where(to == 0, 1, 0)
        copy_to(
            to + aside,
            send.at[to, pl.ds(0, half)],
            recv.at[me + aside * n, pl.ds(0, half)],
            0,
            recv_sem.at[my_x + aside * side],
        )

    def push_own_chip(to):
        @pl.when(is_second)
        def _():
            pltpu.make_async_copy(
                send.at[0, pl.ds(0, half)], recv.at[n + 1, pl.ds(0, half)], recv_sem.at[side]
            ).start()

        @pl.when(jnp.logical_not(is_second))
        def _():
            copy_to(to, send.at[to, pl.ds(0, half)], recv.at[me, pl.ds(0, half)], 0, recv_sem.at[my_x])

    peers_as_known(push, push_own_chip)
    own_message(send, recv, half, recv_sem.at[my_x])

    @pl.when(is_second)
    def _():
        pl.semaphore_wait(first_sem, 1)

    def hand_over(h):
        def pass_on(start, count):
            finish(recv, count, half, recv_sem.at[side + h])
            copy_to(
                0,
                recv.at[pl.ds(n + start, count), pl.ds(0, half)],
                recv.at[pl.ds(start, count), pl.ds(0, half)],
                2,
                recv_sem.at[h],
            )

        @pl.when(jnp.logical_and(is_second, h != 0))
        def _():
            pass_on(h * side * cores, side * cores)

        @pl.when(jnp.logical_and(is_second, h == 0))
        def _():
            pass_on(1, side * cores - 1)


    wind = send[me][half : half + 1, :]
    other = pltpu.roll(wind, SEA_DEV, 1)
    odd_side = lax.rem(me, 2) * SEA_DEV
    even_half = lambda shape: jnp.bitwise_xor(lax.broadcasted_iota(jnp.int32, shape, 1), odd_side) < SEA_DEV
    low16 = even_half((PAIRS, 128))
    speed = jnp.where(even_half((1, 128)), wind, other)
    angle = jnp.where(even_half((1, 128)), other, wind)

    def paired(name):
        rows = tab[at[name] : at[name] + PAIRS, :]
        return jnp.where(odd_side == 0, rows, pltpu.roll(rows, SEA_DEV, 1))

    toward = speed * (paired("pair_cos") * jnp.cos(angle) + paired("pair_sin") * jnp.sin(angle))
    zero16 = jnp.zeros((PAIRS, 128), jnp.float32)
    for w in range(4):
        for k in (0, 1, 2, NF + 3, NF + 4):
            rolled[w, k] = zero16
    for k in range(2):
        low_part[k] = zero16
    for k in range(3):
        high_part[NF + k] = zero16

    def turns(a, amounts):
        s = pltpu.roll(a, SEA_DEV, 1)
        need = {1: (1, 0), -1: (0, -1), 3: (2, 1), -3: (-1, -2)}
        by = {0: s}
        for m in amounts:
            for w in need[m]:
                if w not in by:
                    by[w] = pltpu.roll(s, w % PAIRS, 0)
        return [jnp.where(low16, by[need[m][0]], by[need[m][1]]) for m in amounts]

    group = 8
    per_group = half * group // PAIRS

    def arrange(i, carry):
        m0, m1 = carry
        h = lax.rem(i + 1, side)
        hand_over(h)
        finish(recv, side * cores, half, recv_sem.at[h])
        for g in (2 * h, 2 * h + 1):
            for i in range(group):
                flat[g, half * i : half * i + half, :] = recv[g * group + i, 0:half, :]
        for g in (2 * h, 2 * h + 1):
            for q in range(per_group):
                k = g * per_group + q
                a = flat[g, PAIRS * q : PAIRS * (q + 1), :]
                energy[k] = a
                m0 = m0 + a
                m1 = m1 + tab[pl.ds(at["omega"] + k, 1), :] * a
                for w, b in enumerate(turns(a, (1, -1, 3, -3))):
                    rolled[w, k + 3] = b
        return m0, m1

    m0, m1 = lax.fori_loop(0, side, arrange, (zero16, zero16))

    def over_bins(a):
        a = jnp.sum(a, axis=0, keepdims=True)
        return (a + pltpu.roll(a, SEA_DEV, 1)) * (1.0 / (NF * ND))

    m0, m1 = over_bins(m0), over_bins(m1)
    mean_freq = m1 / (m0 + 1e-6)
    steep = m0 * mean_freq * mean_freq
    breaking = steep * steep / (1.0 + steep * steep)

    def transfer(g, carry):
        for q in range(4 * per_group):
            k = g * 4 * per_group + q
            a = energy[k]
            factor = tab[pl.ds(at["rate"] + k, 1), :] * a
            rates = []
            for plus, minus in ((rolled[1, k + 5], rolled[2, k]), (rolled[0, k + 5], rolled[3, k])):
                rates.append(factor * (a * (plus + minus) - 2.0 * plus * minus))
            up, down = turns(rates[0], (1, -3)), turns(rates[1], (-1, 3))
            own[k] = -2.0 * (rates[0] + rates[1])
            low_part[k + 2] = up[0] + down[0]
            high_part[k] = up[1] + down[1]
        return carry

    lax.fori_loop(0, n // group // 4, transfer, 0)

    def renew(g, total):
        for q in range(per_group):
            k = g * per_group + q
            a = energy[k]
            omega = tab[pl.ds(at["omega"] + k, 1), :]
            gain = (0.05 * omega) * jnp.maximum(0.0, omega * toward - 1.0)
            new = a + (gain - (0.03 * omega) * breaking) * a
            new = new + own[k] + low_part[k] + high_part[k + 3]
            total = total + new
            flat[g, PAIRS * q : PAIRS * (q + 1), :] = new
        for i in range(group):
            back[g * group + i, 0:half, :] = flat[g, half * i : half * i + half, :]
        return total

    total = lax.fori_loop(0, n // group, renew, zero16)
    height = 4.0 * jnp.sqrt(over_bins(total) + 1e-6)

    def add_height(g, carry):
        for i in range(group):
            back[g * group + i, half : half + 1, :] = height
        return carry

    lax.fori_loop(0, n // group, add_height, 0)

    def push_back(to):
        copy_to(
            to,
            back.at[to, pl.ds(0, half + 1)],
            home.at[me, pl.ds(0, half + 1)],
            1,
            recv_sem.at[2 * side],
        )

    peers(push_back, 0, len(chips))
    own_chip(push_back)
    own_message(back, home, half + 1, recv_sem.at[2 * side])

    @pl.when(is_second)
    def _():
        finish(send, n - 2, half, send_sem.at[0])
        finish(recv, n - 1, half, send_sem.at[2])

    @pl.when(jnp.logical_not(is_second))
    def _():
        finish(send, n - 1, half, send_sem.at[0])

    finish(home, n, half + 1, recv_sem.at[2 * side])
    finish(back, n - 1, half + 1, send_sem.at[1])


def unpack_kernel(
    n, bins_dev,
    home, go_right, put, mask2d,
    out, height_out, mean_out,
    moved_a, moved_b, stage, heights, result, own_heights, mean, write_sem,
):
    chunks = mask2d.shape[0]
    half = bins_dev // 2
    cells = chunks * 128
    per_row = NLON // 128
    me = lax.axis_index("spec")
    lane = lax.broadcasted_iota(jnp.int32, (8, 128), 1)
    low = lane < SEA_DEV

    def spread(r, carry):
        pairs = [(home[2 * (r + 8 * j)], home[2 * (r + 8 * j) + 1]) for j in range(n * SEA_DEV // 128 // 8)]
        for t in range(2):
            tiles = [jnp.where(low, p[t], p[1 - t]) for p in pairs]
            for j, tile in enumerate(far_rows(chunks, go_right, tiles, t, r, False, (5, 4, 3))):
                moved_b[t, FAR + r + 8 * j] = tile
        return carry

    lax.fori_loop(0, 8, spread, 0)

    def keep_apart(t, u, v, tile):
        moved_a[t, FAR + v] = tile

    near_rows(chunks, go_right, moved_b, keep_apart, False, (2, 1, 0))

    width = 2 * UNROLL * 128

    def write(g):
        cols = pl.ds(pl.multiple_of(g * width, 128), width)
        return pltpu.make_async_copy(result.at[:, cols], out.at[:, cols], write_sem.at[g])

    def deliver(g, carry):
        for u in range(4 * UNROLL):
            v = g * 4 * UNROLL + u
            sea = jnp.broadcast_to(mask2d[pl.ds(v, 1), :] != 0, (8, 128))
            for t in range(2):
                tile = jnp.where(sea, lanes(moved_a[t, FAR + v], put.at[t], v), 0.0)
                stage[u, pl.ds(t, half, stride=2), :] = tile[0:half]
                if t == 0:
                    heights[pl.ds(v, 1), :] = tile[half : half + 1]
        for part in range(2):
            for u in range(part * 2 * UNROLL, (part + 1) * 2 * UNROLL):
                v = g * 4 * UNROLL + u
                result[:, pl.ds(pl.multiple_of(v * 128, 128), 128)] = stage[u, 0:bins_dev, :]
            write(2 * g + part).start()
        return carry

    lax.fori_loop(0, chunks // (4 * UNROLL), deliver, 0)

    points = cells // n
    together = NLON // points
    start = me // together * per_row
    three = [heights[pl.ds(start + q, 1), :] for q in range(per_row)]
    u = lax.rem(me, together)
    picked = None
    for g in range(together):
        first, offset = g * points // 128, g * points % 128
        piece = three[first]
        if offset:
            after = three[min(first + 1, per_row - 1)]
            piece = jnp.where(
                lane[0:1] < 128 - offset,
                pltpu.roll(piece, 128 - offset, 1),
                pltpu.roll(after, 128 - offset, 1),
            )
        picked = piece if picked is None else jnp.where(u == g, piece, picked)
    own_heights[...] = picked[:, 0:points]
    all_heights = jnp.sum(heights[...], axis=0, keepdims=True)
    mean[...] = jnp.sum(all_heights, axis=1, keepdims=True) * (1.0 / (SEA_DEV * n))

    small = (
        pltpu.make_async_copy(own_heights, height_out, write_sem.at[cells // width]),
        pltpu.make_async_copy(mean, mean_out, write_sem.at[cells // width + 1]),
    )
    for copy in small:
        copy.start()

    def written(g, carry):
        write(g).wait()
        return carry

    lax.fori_loop(0, cells // width, written, 0)
    for copy in small:
        copy.wait()


def solution(mesh):
    n = mesh.shape["spec"]
    cores = 2
    side = math.isqrt(n // cores)

    def local(spectrum, sea_mask, wind_speed, wind_angle):
        bins_dev, cells = spectrum.shape
        chunks = cells // 128
        padded = chunks + 2 * (NLON // 128)
        tab, at = tables(cells // NLON)
        vmem = pl.BlockSpec(memory_space=pltpu.VMEM)
        words = pltpu.VMEM((2, chunks + 2 * REACH, 128), jnp.int32)
        by_freq = lambda *dims: pltpu.VMEM((*dims, PAIRS, 128), jnp.float32)
        messages = lambda count: pltpu.VMEM((count, 8, 128), jnp.float32)
        home, go_right, put = pl.pallas_call(
            functools.partial(step_kernel, n, side, cores, at),
            name="wave_step",
            out_shape=(
                jax.ShapeDtypeStruct((n, 8, 128), jnp.float32),
                jax.ShapeDtypeStruct((2, chunks + 2 * REACH, 128), jnp.int32),
                jax.ShapeDtypeStruct((2, chunks, 128), jnp.int32),
            ),
            in_specs=[pl.BlockSpec(memory_space=pltpu.HBM)] * 5,
            out_specs=(vmem,) * 3,
            scratch_shapes=[
                pltpu.VMEM((bins_dev, cells), jnp.float32),
                pltpu.VMEM((chunks, 128), jnp.int32),
                pltpu.VMEM((chunks, 128), jnp.float32),
                pltpu.VMEM((chunks, 128), jnp.float32),
                pltpu.VMEM((chunks, 128), jnp.float32),
                pltpu.VMEM(tab.shape, jnp.float32),
                pltpu.VMEM((2, padded, 8, 128), jnp.float32),
                pltpu.VMEM((2, padded, 8, 128), jnp.float32),
                pltpu.VMEM((8, 16, 128), jnp.float32),
                pltpu.VMEM((chunks + REACH, 128), jnp.int32),
                words,
                pltpu.VMEM((2, chunks, 128), jnp.int32),
                pltpu.VMEM((2, chunks + 2 * FAR, 8, 128), jnp.float32),
                pltpu.VMEM((2, chunks + 2 * FAR, 8, 128), jnp.float32),
                messages(n),
                messages(2 * n),
                messages(n),
                pltpu.VMEM((n // 8, 8 * bins_dev // 2, 128), jnp.float32),
                by_freq(NF),
                by_freq(4, NF + 5),
                by_freq(NF),
                by_freq(NF + 2),
                by_freq(NF + 3),
                pltpu.SMEM((4, side * side), jnp.int32),
                pltpu.SemaphoreType.DMA((3,)),
                pltpu.SemaphoreType.DMA((2 * side + 1,)),
                pltpu.SemaphoreType.DMA((8,)),
                pltpu.SemaphoreType.REGULAR((side,)),
                pltpu.SemaphoreType.REGULAR,
            ],
            compiler_params=pltpu.CompilerParams(
                collective_id=0, has_side_effects=True, vmem_limit_bytes=VMEM_BYTES
            ),
        )(
            *(
                pltpu.with_memory_space_constraint(a, pltpu.HBM)
                for a in (
                    spectrum,
                    sea_mask.reshape(chunks, 128),
                    wind_speed.reshape(chunks, 128),
                    wind_angle.reshape(chunks, 128),
                    jnp.asarray(tab),
                )
            )
        )
        moved = pltpu.VMEM((2, chunks + 2 * FAR, 8, 128), jnp.float32)
        new_spectrum, height, mean = pl.pallas_call(
            functools.partial(unpack_kernel, n, bins_dev),
            name="unpack",
            out_shape=(
                jax.ShapeDtypeStruct((bins_dev, cells), jnp.float32),
                jax.ShapeDtypeStruct((1, cells // n), jnp.float32),
                jax.ShapeDtypeStruct((1, 1), jnp.float32),
            ),
            in_specs=[vmem] * 4,
            out_specs=(pl.BlockSpec(memory_space=pl.ANY),) * 3,
            scratch_shapes=[
                moved,
                moved,
                pltpu.VMEM((32, 16, 128), jnp.float32),
                pltpu.VMEM((chunks, 128), jnp.float32),
                pltpu.VMEM((bins_dev, cells), jnp.float32),
                pltpu.VMEM((1, cells // n), jnp.float32),
                pltpu.VMEM((1, 1), jnp.float32),
                pltpu.SemaphoreType.DMA((chunks // (2 * UNROLL) + 2,)),
            ],
            compiler_params=pltpu.CompilerParams(vmem_limit_bytes=VMEM_BYTES),
        )(home, go_right, put, sea_mask.reshape(chunks, 128))
        return new_spectrum, height.reshape(-1), mean.reshape(1)

    return jax.shard_map(
        local,
        mesh=mesh,
        in_specs=(P(("grp", "spec"), None), P(), P("grp"), P("grp")),
        out_specs=(P(("grp", "spec"), None), P(("grp", "spec")), P("grp")),
        check_vma=False,
    )
```

```python
import functools
import math

import jax
import jax.numpy as jnp
import numpy as np
from jax import lax
from jax.experimental import pallas as pl
from jax.experimental.pallas import tpu as pltpu
from jax.sharding import PartitionSpec as P

NF = 48
ND = 32
NLON = 384
SUBSTEPS = 2
SEA_DEV = 64
MESH = pl.DeviceIdType.MESH
LOG_RATIO = math.log(1.1)
PAIRS = ND // 2
ROW_STEPS = 6
REACH = 32
UNROLL = 8
VMEM_BYTES = 24 * 1024 * 1024
FAR = 56


def tables(lat_count):
    heading = 2.0 * np.pi * (np.arange(ND) + 0.5) / ND
    wrapped = np.concatenate([heading, heading[:24]])
    flat = lambda a: np.repeat(np.asarray(a)[:, None], 128, 1)
    paired = np.repeat(heading.reshape(PAIRS, 2), SEA_DEV, axis=1)
    latitude = np.radians(-75.0 + 150.0 * (np.arange(lat_count) + 0.5) / lat_count)
    k = np.arange(NF)
    rows, at = [], {}
    for name, block in (
        ("cos", flat(np.cos(wrapped))),
        ("sin", flat(np.sin(wrapped))),
        ("pair_cos", np.cos(paired)),
        ("pair_sin", np.sin(paired)),
        ("widen", flat(1.0 / np.cos(latitude))),
        ("omega", flat(np.exp(LOG_RATIO * (k - NF // 2)))),
        ("rate", flat(np.where((k >= 3) & (k <= NF - 3), 0.001, 0.0))),
    ):
        at[name] = sum(len(r) for r in rows)
        rows.append(block)
    return np.concatenate(rows).astype(np.float32), at


def chip_order(side):
    hops = lambda d: min(d, side - d)
    way = lambda d: (d > 0) - 2 * (d > side // 2)
    chips = [(x, y) for x in range(side) for y in range(side)][1:]
    chips.sort(key=lambda o: (-(hops(o[0]) + hops(o[1])), 3 * o[0] + 5 * o[1]))
    kinds = {}
    for o in chips:
        kinds.setdefault((way(o[0]), way(o[1])), []).append(o)
    placed = [((i + 0.5) / len(k), o) for k in kinds.values() for i, o in enumerate(k)]
    return [o for _, o in sorted(placed, key=lambda p: p[0])]


def word_of(words, v):
    return jnp.broadcast_to(words[pl.ds(REACH + v, 1), :], (8, 128))


def has(word, i):
    return jnp.bitwise_and(word, 1 << i) != 0


def lanes(tile, index, v):
    index = jnp.broadcast_to(index[pl.ds(v, 1), :], (8, 128))
    return jnp.take_along_axis(tile, index, axis=1, mode="promise_in_bounds")


def near_rows(chunks, words, src, emit, toward_end, bit_order):
    way = 1 if toward_end else -1

    def block(g, carry):
        first = g * UNROLL
        span = [first + way * u if toward_end else first + UNROLL - 1 - u for u in range(UNROLL + 7)]
        for t in range(2):
            word = [word_of(words.at[t], v) for v in span]
            cur = [src[t, FAR + v] for v in span]
            for b in bit_order:
                d = 1 << b
                cur = [
                    jnp.where(has(word[u], b), cur[u + d], cur[u])
                    for u in range(len(cur) - d)
                ]
            for u in range(UNROLL):
                emit(t, u, span[u], cur[u])
        return carry

    lax.fori_loop(0, chunks // UNROLL, block, 0)


def far_rows(chunks, words, tiles, t, r, toward_end, bit_order):
    tiles = tiles + [None] * (chunks // 8 - len(tiles))
    word = [word_of(words.at[t], r + 8 * j) for j in range(chunks // 8)]
    for b in bit_order:
        d = (1 << (b - 3)) * (1 if toward_end else -1)
        moved = []
        for j, own in enumerate(tiles):
            other = tiles[j + d] if 0 <= j + d < len(tiles) else None
            if own is None or other is None:
                moved.append(other if own is None else own)
            else:
                moved.append(jnp.where(has(word[j], b), other, own))
        tiles = moved
    return tiles


def step_kernel(
    n, side, cores, at,
    x_hbm, mask_hbm, speed_hbm, angle_hbm, tab_hbm,
    home, go_right, put,
    x, mask2d, sea_float, speed2d, angle2d, tab, field_a, field_b, stage, shifts, go_left, pick, moved_a, moved_b,
    send, recv, back, swap, flat, energy, rolled, own, low_part, high_part,
    order, send_sem, recv_sem, load_sem, column_sem, first_sem,
):
    bins_dev, cells = x.shape
    half = bins_dev // 2
    chunks = cells // 128
    per_row = NLON // 128
    lat_count = cells // NLON
    me = lax.axis_index("spec")
    my_x, my_y, my_c = me // (side * cores), lax.rem(me // cores, side), lax.rem(me, cores)

    parts = 4
    part_cols = cells // parts
    small = [
        pltpu.make_async_copy(src, dst, load_sem.at[parts + k])
        for k, (src, dst) in enumerate(
            ((mask_hbm, mask2d), (tab_hbm, tab), (speed_hbm, speed2d), (angle_hbm, angle2d))
        )
    ]

    def load(part):
        cols = pl.ds(pl.multiple_of(part * part_cols, 128), part_cols)
        return pltpu.make_async_copy(x_hbm.at[:, cols], x.at[:, cols], load_sem.at[part])

    small[0].start()
    for part in range(parts):
        load(part).start()
    for copy in small[1:]:
        copy.start()

    def wrap(a):
        return jnp.bitwise_and(a, side - 1) if side & (side - 1) == 0 else lax.rem(a, side)

    def hop(u):
        return side // 2 + (1 - 2 * jnp.bitwise_and(u, 1)) * jnp.right_shift(u + 1, 1)

    def both_cores(act, px, py):
        first = (px * side + py) * cores
        act(first + my_c)
        for c in range(1, cores):
            act(first + jnp.where(my_c + c >= cores, my_c + c - cores, my_c + c))

    def own_chip(act):
        for c in range(1, cores):
            act(me - my_c + lax.rem(my_c + c, cores))

    chips = chip_order(side)
    other_rows = [o for o in chips if o[1] != 0]

    def peers(act, which, count):
        def chip(i, carry):
            both_cores(act, wrap(my_x + order[2 * which, i]), wrap(my_y + order[2 * which + 1, i]))
            return carry

        lax.fori_loop(0, count, chip, 0)

    is_first = me == 0
    is_second = me == 1
    below_first = jnp.logical_and(jnp.logical_and(my_x == 0, my_c == 0), my_y != 0)

    def signal(semaphore, to):
        pl.semaphore_signal(semaphore, inc=1, device_id={"spec": to}, device_id_type=MESH)

    def down_column(act):
        def one(u, carry):
            act((my_x * side + wrap(my_y + hop(u))) * cores + my_c)
            return carry

        lax.fori_loop(0, side - 1, one, 0)

    def along_row(act, own=None):
        def one(u, carry):
            both_cores(act, wrap(my_x + hop(u)), my_y)
            return carry

        lax.fori_loop(0, side - 1, one, 0)
        own_chip(act if own is None else own)

    def peers_as_known(act, own):
        along_row(act, own)

        @pl.when(jnp.logical_not(is_first))
        def _():
            def row_in(i, carry):
                pl.semaphore_wait(column_sem.at[wrap(my_y + i)], 1)
                return carry

            @pl.when(jnp.logical_not(below_first))
            def _():
                lax.fori_loop(1, side, row_in, 0)

            @pl.when(is_second)
            def _():
                down_column(lambda to: signal(column_sem.at[0], to - 1))

            @pl.when(below_first)
            def _():
                lax.fori_loop(1, side, row_in, 0)

        peers(act, 1, len(other_rows))

    barrier = pltpu.get_barrier_semaphore()

    @pl.when(jnp.logical_not(is_first))
    def _():
        along_row(lambda to: signal(barrier, to))
        down_column(lambda to: signal(barrier, to))

    def entered():
        called = side * cores + side - 2

        @pl.when(jnp.logical_not(is_first))
        def _():
            with_first = jnp.logical_or(my_y == 0, below_first)
            pl.semaphore_wait(barrier, called - jnp.where(with_first, 1, 0))

            def complete(to):
                @pl.when(to == 0)
                def _():
                    signal(barrier, to)

                @pl.when(to != 0)
                def _():
                    signal(column_sem.at[my_y], to)

            down_column(complete)

    for which, table in enumerate((chips, other_rows)):
        for i, (dx, dy) in enumerate(table):
            order[2 * which, i] = dx
            order[2 * which + 1, i] = dy
    small[0].wait()

    lane = lax.broadcasted_iota(jnp.int32, (8, 128), 1)
    row = lax.broadcasted_iota(jnp.int32, (8, 128), 0)
    low = lane < SEA_DEV

    is_sea = mask2d[...] != 0
    sea_float[...] = mask2d[...].astype(jnp.float32)
    land = jnp.where(is_sea, 0.0, 1.0).astype(jnp.bfloat16)
    earlier = (
        lax.broadcasted_iota(jnp.int32, (128, 128), 0) < lax.broadcasted_iota(jnp.int32, (128, 128), 1)
    ).astype(jnp.bfloat16)
    above = (
        lax.broadcasted_iota(jnp.int32, (chunks, chunks), 1)
        < lax.broadcasted_iota(jnp.int32, (chunks, chunks), 0)
    ).astype(jnp.bfloat16)
    ones = jnp.ones((128, 128), jnp.bfloat16)
    count = functools.partial(jnp.dot, preferred_element_type=jnp.float32)
    before = count(land, earlier).astype(jnp.int32)
    sea_in_row = 128 - count(land, ones).astype(jnp.int32)
    wide_lane = lax.broadcasted_iota(jnp.int32, (chunks, 128), 1)
    wide_row = lax.broadcasted_iota(jnp.int32, (chunks, 128), 0)
    rank0 = wide_row * 128 - count(count(above, land).astype(jnp.bfloat16), ones).astype(jnp.int32)
    put[0] = jnp.bitwise_and(rank0 + wide_lane - before, 127)
    put[1] = jnp.bitwise_and(rank0 + wide_lane - before + SEA_DEV, 127)
    to_go = jnp.where(is_sea, before, 0)
    shifts[chunks:, :] = jnp.zeros((shifts.shape[0] - chunks, 128), jnp.int32)
    go_left[...] = jnp.zeros_like(go_left)
    go_right[...] = jnp.zeros_like(go_right)

    def close_up(i, to_go):
        d = jnp.left_shift(1, i)
        incoming = pltpu.roll(to_go, 128 - d, 1)
        stay = jnp.where(jnp.bitwise_and(to_go, d) != 0, 0, to_go)
        return jnp.where(jnp.bitwise_and(incoming, d) != 0, incoming, stay)

    def plan_rows(to_go):
        nth = jnp.bitwise_and(wide_lane - rank0, 127)
        front = jnp.bitwise_and(wide_lane + to_go, 127)
        took = jnp.take_along_axis(front, nth, axis=1, mode="promise_in_bounds")
        pick[0] = took
        pick[1] = pltpu.roll(took, SEA_DEV, 1)
        up = wide_row - jnp.right_shift(rank0 + nth, 7)
        shifts[0:chunks, :] = jnp.where(nth < sea_in_row, up, 0)
        for b in range(ROW_STEPS):
            here, incoming = shifts[0:chunks, :], shifts[1 << b : chunks + (1 << b), :]
            goes = jnp.bitwise_and(here, 1 << b)
            comes = jnp.bitwise_and(incoming, 1 << b)
            rights, lefts = (goes, comes) if b == 0 else (rights + goes, lefts + comes)
            shifts[0:chunks, :] = jnp.where(comes != 0, incoming, jnp.where(goes != 0, 0, here))
        for words, found in ((go_right, rights), (go_left, lefts)):
            words[0, REACH : REACH + chunks, :] = found
            words[1, REACH : REACH + chunks, :] = pltpu.roll(found, SEA_DEV, 1)

    zero = jnp.zeros((8, 128), jnp.float32)
    pad = per_row
    for t in range(2):
        for v in range(pad):
            for f in (field_a, field_b):
                f[t, v] = zero
                f[t, pad + chunks + v] = zero
    base = (me * bins_dev) % ND
    for copy in small[1:]:
        copy.wait()
    pace_x, pace_y, from_west, from_south, beside, edge = [], [], [], [], [], []
    for t in range(2):
        k = ((me * bins_dev + jnp.minimum(2 * row + t, bins_dev - 1)) // ND).astype(jnp.float32)
        pace = 0.2 * jnp.exp(-LOG_RATIO * k)
        ax = pace * tab[pl.ds(at["cos"] + base + t, 8, stride=2), :]
        ay = pace * tab[pl.ds(at["sin"] + base + t, 8, stride=2), :]
        pace_x.append(jnp.abs(ax))
        pace_y.append(jnp.abs(ay))
        from_west.append(ax >= 0.0)
        from_south.append(ay >= 0.0)
        beside.append(jnp.bitwise_and(jnp.where(from_west[t], lane - 1, lane + 1), 127))
        edge.append(
            (
                jnp.logical_and(from_west[t], lane == 0),
                jnp.logical_and(jnp.logical_not(from_west[t]), lane == 127),
            )
        )

    def split_bins(g, carry):
        for u in range(8):
            v = g * 8 + u
            cols = pl.ds(pl.multiple_of(v * 128, 128), 128)
            stage[u, 0:bins_dev, :] = x[:, cols] * sea_float[pl.ds(v, 1), :]
            for t in range(2):
                field_a[t, pad + v, 0:half, :] = stage[u, pl.ds(t, half, stride=2), :]
        return carry

    def split_part(part, carry):
        load(part).wait()
        per_part = chunks // 8 // parts
        return lax.fori_loop(part * per_part, (part + 1) * per_part, split_bins, carry)

    lax.fori_loop(0, parts, split_part, 0)

    for s in range(SUBSTEPS):
        src, dst = (field_a, field_b) if s % 2 == 0 else (field_b, field_a)

        def advance(g, to_go, src=src, dst=dst, s=s):
            if s == 0:
                to_go = close_up(2 * g + 1, close_up(2 * g, to_go))
            for ru in range(8):
                r = g * 8 + ru
                widen = tab[pl.ds(at["widen"] + r, 1), :]
                first = pad + r * per_row
                for t in range(2):
                    side_c = pace_x[t] * widen
                    own_c = 1.0 - side_c - pace_y[t]
                    first = pad + r * per_row
                    e = [src[t, first + q] for q in range(per_row)]
                    turned = [jnp.take_along_axis(a, beside[t], axis=1, mode="promise_in_bounds") for a in e]
                    for q in range(per_row):
                        across = jnp.where(edge[t][0], turned[q - 1], turned[q])
                        across = jnp.where(edge[t][1], turned[(q + 1) % per_row], across)
                        along = jnp.where(
                            from_south[t], src[t, first + q - per_row], src[t, first + q + per_row]
                        )
                        new = own_c * e[q] + side_c * across + pace_y[t] * along
                        v = first + q - pad
                        if s < SUBSTEPS - 1:
                            dst[t, first + q] = new * sea_float[pl.ds(v, 1), :]
                        else:
                            wind = (speed2d, angle2d)[t][pl.ds(v, 1), :]
                            dst[t, first + q] = jnp.where(row == half, wind, new)
            return to_go

        to_go = lax.fori_loop(0, lat_count // 8, advance, to_go)
        if s == 0:
            plan_rows(to_go)
    final = field_a if SUBSTEPS % 2 == 0 else field_b
    entered()

    def to_lanes(g, carry):
        for u in range(4 * UNROLL):
            v = g * 4 * UNROLL + u
            for t in range(2):
                moved_a[t, FAR + v] = lanes(final[t, pad + v], pick.at[t], v)
        return carry

    lax.fori_loop(0, chunks // (4 * UNROLL), to_lanes, 0)


    def keep_near(t, u, v, tile):
        moved_b[t, FAR + v] = tile

    near_rows(chunks, go_left, moved_a, keep_near, True, (0, 1, 2))

    def pack(r, carry):
        even, odd = (
            far_rows(
                chunks, go_left, [moved_b[t, FAR + r + 8 * j] for j in range(chunks // 8)], t, r, True, (3, 4, 5)
            )
            for t in range(2)
        )
        for j in range(n * SEA_DEV // 128 // 8):
            v = r + 8 * j
            send[2 * v] = jnp.where(low, even[j], odd[j])
            send[2 * v + 1] = jnp.where(low, odd[j], even[j])
        return carry

    lax.fori_loop(0, 8, pack, 0)

    def finish(ref, count, rows, sem):
        part = ref.at[pl.ds(0, count), pl.ds(0, rows)]
        pltpu.make_async_copy(part, part, sem).wait()

    def copy_to(to, src, dst, k, arrival):
        pltpu.make_async_remote_copy(
            src_ref=src,
            dst_ref=dst,
            send_sem=send_sem.at[k],
            recv_sem=arrival,
            device_id={"spec": to},
            device_id_type=MESH,
        ).start()

    def own_message(src, dst, rows, arrival):
        pltpu.make_async_copy(src.at[me, pl.ds(0, rows)], dst.at[me, pl.ds(0, rows)], arrival).start()

    @pl.when(is_first)
    def _():
        pl.semaphore_wait(barrier, side * cores + 2 * side - 3)
        signal(first_sem, 1)

    def push(to):
        aside = jnp.where(to == 0, 1, 0)
        copy_to(
            to + aside,
            send.at[to, pl.ds(0, half)],
            recv.at[me + aside * n, pl.ds(0, half)],
            0,
            recv_sem.at[my_x + aside * side],
        )

    def push_own_chip(to):
        @pl.when(is_second)
        def _():
            pltpu.make_async_copy(
                send.at[0, pl.ds(0, half)], recv.at[n + 1, pl.ds(0, half)], recv_sem.at[side]
            ).start()

        @pl.when(jnp.logical_not(is_second))
        def _():
            copy_to(to, send.at[to, pl.ds(0, half)], recv.at[me, pl.ds(0, half)], 0, recv_sem.at[my_x])

    peers_as_known(push, push_own_chip)
    own_message(send, recv, half, recv_sem.at[my_x])

    @pl.when(is_second)
    def _():
        pl.semaphore_wait(first_sem, 1)

    def hand_over(h):
        def pass_on(start, count):
            finish(recv, count, half, recv_sem.at[side + h])
            copy_to(
                0,
                recv.at[pl.ds(n + start, count), pl.ds(0, half)],
                recv.at[pl.ds(start, count), pl.ds(0, half)],
                2,
                recv_sem.at[h],
            )

        @pl.when(jnp.logical_and(is_second, h != 0))
        def _():
            pass_on(h * side * cores, side * cores)

        @pl.when(jnp.logical_and(is_second, h == 0))
        def _():
            pass_on(1, side * cores - 1)


    wind = send[me][half : half + 1, :]
    other = pltpu.roll(wind, SEA_DEV, 1)
    odd_side = lax.rem(me, 2) * SEA_DEV
    even_half = lambda shape: jnp.bitwise_xor(lax.broadcasted_iota(jnp.int32, shape, 1), odd_side) < SEA_DEV
    low16 = even_half((PAIRS, 128))
    speed = jnp.where(even_half((1, 128)), wind, other)
    angle = jnp.where(even_half((1, 128)), other, wind)

    def paired(name):
        rows = tab[at[name] : at[name] + PAIRS, :]
        return jnp.where(odd_side == 0, rows, pltpu.roll(rows, SEA_DEV, 1))

    toward = speed * (paired("pair_cos") * jnp.cos(angle) + paired("pair_sin") * jnp.sin(angle))
    zero16 = jnp.zeros((PAIRS, 128), jnp.float32)
    for w in range(4):
        for k in (0, 1, 2, NF + 3, NF + 4):
            rolled[w, k] = zero16
    for k in range(2):
        low_part[k] = zero16
    for k in range(3):
        high_part[NF + k] = zero16

    def turns(a, amounts):
        s = pltpu.roll(a, SEA_DEV, 1)
        need = {1: (1, 0), -1: (0, -1), 3: (2, 1), -3: (-1, -2)}
        by = {0: s}
        for m in amounts:
            for w in need[m]:
                if w not in by:
                    by[w] = pltpu.roll(s, w % PAIRS, 0)
        return [jnp.where(low16, by[need[m][0]], by[need[m][1]]) for m in amounts]

    group = 8
    per_group = half * group // PAIRS

    def arrange(i, carry):
        m0, m1 = carry
        h = lax.rem(i + 1, side)
        hand_over(h)
        finish(recv, side * cores, half, recv_sem.at[h])
        for g in (2 * h, 2 * h + 1):
            for i in range(group):
                flat[g, half * i : half * i + half, :] = recv[g * group + i, 0:half, :]
        for g in (2 * h, 2 * h + 1):
            for q in range(per_group):
                k = g * per_group + q
                a = flat[g, PAIRS * q : PAIRS * (q + 1), :]
                energy[k] = a
                m0 = m0 + a
                m1 = m1 + tab[pl.ds(at["omega"] + k, 1), :] * a
                for w, b in enumerate(turns(a, (1, -1, 3, -3))):
                    rolled[w, k + 3] = b
        return m0, m1

    m0, m1 = lax.fori_loop(0, side, arrange, (zero16, zero16))

    def over_bins(a):
        a = jnp.sum(a, axis=0, keepdims=True)
        return (a + pltpu.roll(a, SEA_DEV, 1)) * (1.0 / (NF * ND))

    m0, m1 = over_bins(m0), over_bins(m1)
    mean_freq = m1 / (m0 + 1e-6)
    steep = m0 * mean_freq * mean_freq
    breaking = steep * steep / (1.0 + steep * steep)

    def transfer(g, carry):
        for q in range(4 * per_group):
            k = g * 4 * per_group + q
            a = energy[k]
            factor = tab[pl.ds(at["rate"] + k, 1), :] * a
            rates = []
            for plus, minus in ((rolled[1, k + 5], rolled[2, k]), (rolled[0, k + 5], rolled[3, k])):
                rates.append(factor * (a * (plus + minus) - 2.0 * plus * minus))
            up, down = turns(rates[0], (1, -3)), turns(rates[1], (-1, 3))
            own[k] = -2.0 * (rates[0] + rates[1])
            low_part[k + 2] = up[0] + down[0]
            high_part[k] = up[1] + down[1]
        return carry

    lax.fori_loop(0, n // group // 4, transfer, 0)

    def renew(g, total):
        for q in range(per_group):
            k = g * per_group + q
            a = energy[k]
            omega = tab[pl.ds(at["omega"] + k, 1), :]
            gain = (0.05 * omega) * jnp.maximum(0.0, omega * toward - 1.0)
            new = a + (gain - (0.03 * omega) * breaking) * a
            new = new + own[k] + low_part[k] + high_part[k + 3]
            total = total + new
            flat[g, PAIRS * q : PAIRS * (q + 1), :] = new
        for i in range(group):
            back[g * group + i, 0:half, :] = flat[g, half * i : half * i + half, :]
        return total

    total = lax.fori_loop(0, n // group, renew, zero16)
    height = 4.0 * jnp.sqrt(over_bins(total) + 1e-6)

    swap[0, 0:1, :] = height
    partner = me + 1 - 2 * my_c
    copy_to(partner, swap.at[0, pl.ds(0, 1)], swap.at[1, pl.ds(0, 1)], 4, recv_sem.at[2 * side + 2])

    def push_back(to, rows, k):
        copy_to(
            to,
            back.at[to, pl.ds(0, rows)],
            home.at[me, pl.ds(0, rows)],
            (1, 3)[k],
            recv_sem.at[2 * side + k],
        )

    def on_core(core, rows, k):
        def chip(i, carry):
            px, py = wrap(my_x + order[0, i]), wrap(my_y + order[1, i])
            push_back((px * side + py) * cores + core, rows, k)
            return carry

        lax.fori_loop(0, len(chips), chip, 0)

    on_core(1 - my_c, half, 0)
    push_back(partner, half, 0)
    swapped = swap.at[1, pl.ds(0, 1)]
    pltpu.make_async_copy(swapped, swapped, recv_sem.at[2 * side + 2]).wait()
    theirs = swap[1, 0:1, :]
    both_heights = jnp.where(even_half((1, 128)), height, theirs)

    def add_height(g, carry):
        for i in range(group):
            back[g * group + i, half : half + 1, :] = both_heights
        return carry

    lax.fori_loop(0, n // group, add_height, 0)
    on_core(my_c, half + 1, 1)
    own_message(back, home, half + 1, recv_sem.at[2 * side + 1])

    @pl.when(is_second)
    def _():
        finish(send, n - 2, half, send_sem.at[0])
        finish(recv, n - 1, half, send_sem.at[2])

    @pl.when(jnp.logical_not(is_second))
    def _():
        finish(send, n - 1, half, send_sem.at[0])

    finish(home, n // cores, half, recv_sem.at[2 * side])
    finish(home, n // cores, half + 1, recv_sem.at[2 * side + 1])
    finish(back, n // cores, half, send_sem.at[1])
    finish(back, n // cores - 1, half + 1, send_sem.at[3])
    pltpu.make_async_copy(swapped, swapped, send_sem.at[4]).wait()


def unpack_kernel(
    n, bins_dev,
    home, go_right, put, mask2d,
    out, height_out, mean_out,
    moved_a, moved_b, stage, heights, result, own_heights, mean, write_sem,
):
    chunks = mask2d.shape[0]
    half = bins_dev // 2
    cells = chunks * 128
    per_row = NLON // 128
    me = lax.axis_index("spec")
    lane = lax.broadcasted_iota(jnp.int32, (8, 128), 1)
    low = lane < SEA_DEV

    row = lax.broadcasted_iota(jnp.int32, (8, 128), 0)
    own_core = jnp.where(lax.rem(me, 2) == 0, 0, SEA_DEV)
    from_even = (jnp.where(row == half, own_core, lane) < SEA_DEV, jnp.logical_not(low))

    def spread(r, carry):
        pairs = [(home[2 * (r + 8 * j)], home[2 * (r + 8 * j) + 1]) for j in range(n * SEA_DEV // 128 // 8)]
        for t in range(2):
            tiles = [jnp.where(from_even[t], p[0], p[1]) for p in pairs]
            for j, tile in enumerate(far_rows(chunks, go_right, tiles, t, r, False, (5, 4, 3))):
                moved_b[t, FAR + r + 8 * j] = tile
        return carry

    lax.fori_loop(0, 8, spread, 0)

    def keep_apart(t, u, v, tile):
        moved_a[t, FAR + v] = tile

    near_rows(chunks, go_right, moved_b, keep_apart, False, (2, 1, 0))

    width = 2 * UNROLL * 128

    def write(g):
        cols = pl.ds(pl.multiple_of(g * width, 128), width)
        return pltpu.make_async_copy(result.at[:, cols], out.at[:, cols], write_sem.at[g])

    def deliver(g, carry):
        for u in range(4 * UNROLL):
            v = g * 4 * UNROLL + u
            sea = jnp.broadcast_to(mask2d[pl.ds(v, 1), :] != 0, (8, 128))
            for t in range(2):
                tile = jnp.where(sea, lanes(moved_a[t, FAR + v], put.at[t], v), 0.0)
                stage[u, pl.ds(t, half, stride=2), :] = tile[0:half]
                if t == 0:
                    heights[pl.ds(v, 1), :] = tile[half : half + 1]
        for part in range(2):
            for u in range(part * 2 * UNROLL, (part + 1) * 2 * UNROLL):
                v = g * 4 * UNROLL + u
                result[:, pl.ds(pl.multiple_of(v * 128, 128), 128)] = stage[u, 0:bins_dev, :]
            write(2 * g + part).start()
        return carry

    lax.fori_loop(0, chunks // (4 * UNROLL), deliver, 0)

    points = cells // n
    together = NLON // points
    start = me // together * per_row
    three = [heights[pl.ds(start + q, 1), :] for q in range(per_row)]
    u = lax.rem(me, together)
    picked = None
    for g in range(together):
        first, offset = g * points // 128, g * points % 128
        piece = three[first]
        if offset:
            after = three[min(first + 1, per_row - 1)]
            piece = jnp.where(
                lane[0:1] < 128 - offset,
                pltpu.roll(piece, 128 - offset, 1),
                pltpu.roll(after, 128 - offset, 1),
            )
        picked = piece if picked is None else jnp.where(u == g, piece, picked)
    own_heights[...] = picked[:, 0:points]
    all_heights = jnp.sum(heights[...], axis=0, keepdims=True)
    mean[...] = jnp.sum(all_heights, axis=1, keepdims=True) * (1.0 / (SEA_DEV * n))

    small = (
        pltpu.make_async_copy(own_heights, height_out, write_sem.at[cells // width]),
        pltpu.make_async_copy(mean, mean_out, write_sem.at[cells // width + 1]),
    )
    for copy in small:
        copy.start()

    def written(g, carry):
        write(g).wait()
        return carry

    lax.fori_loop(0, cells // width, written, 0)
    for copy in small:
        copy.wait()


def solution(mesh):
    n = mesh.shape["spec"]
    cores = 2
    side = math.isqrt(n // cores)

    def local(spectrum, sea_mask, wind_speed, wind_angle):
        bins_dev, cells = spectrum.shape
        chunks = cells // 128
        padded = chunks + 2 * (NLON // 128)
        tab, at = tables(cells // NLON)
        vmem = pl.BlockSpec(memory_space=pltpu.VMEM)
        words = pltpu.VMEM((2, chunks + 2 * REACH, 128), jnp.int32)
        by_freq = lambda *dims: pltpu.VMEM((*dims, PAIRS, 128), jnp.float32)
        messages = lambda count: pltpu.VMEM((count, 8, 128), jnp.float32)
        home, go_right, put = pl.pallas_call(
            functools.partial(step_kernel, n, side, cores, at),
            name="wave_step",
            out_shape=(
                jax.ShapeDtypeStruct((n, 8, 128), jnp.float32),
                jax.ShapeDtypeStruct((2, chunks + 2 * REACH, 128), jnp.int32),
                jax.ShapeDtypeStruct((2, chunks, 128), jnp.int32),
            ),
            in_specs=[pl.BlockSpec(memory_space=pltpu.HBM)] * 5,
            out_specs=(vmem,) * 3,
            scratch_shapes=[
                pltpu.VMEM((bins_dev, cells), jnp.float32),
                pltpu.VMEM((chunks, 128), jnp.int32),
                pltpu.VMEM((chunks, 128), jnp.float32),
                pltpu.VMEM((chunks, 128), jnp.float32),
                pltpu.VMEM((chunks, 128), jnp.float32),
                pltpu.VMEM(tab.shape, jnp.float32),
                pltpu.VMEM((2, padded, 8, 128), jnp.float32),
                pltpu.VMEM((2, padded, 8, 128), jnp.float32),
                pltpu.VMEM((8, 16, 128), jnp.float32),
                pltpu.VMEM((chunks + REACH, 128), jnp.int32),
                words,
                pltpu.VMEM((2, chunks, 128), jnp.int32),
                pltpu.VMEM((2, chunks + 2 * FAR, 8, 128), jnp.float32),
                pltpu.VMEM((2, chunks + 2 * FAR, 8, 128), jnp.float32),
                messages(n),
                messages(2 * n),
                messages(n),
                messages(2),
                pltpu.VMEM((n // 8, 8 * bins_dev // 2, 128), jnp.float32),
                by_freq(NF),
                by_freq(4, NF + 5),
                by_freq(NF),
                by_freq(NF + 2),
                by_freq(NF + 3),
                pltpu.SMEM((4, side * side), jnp.int32),
                pltpu.SemaphoreType.DMA((5,)),
                pltpu.SemaphoreType.DMA((2 * side + 3,)),
                pltpu.SemaphoreType.DMA((8,)),
                pltpu.SemaphoreType.REGULAR((side,)),
                pltpu.SemaphoreType.REGULAR,
            ],
            compiler_params=pltpu.CompilerParams(
                collective_id=0, has_side_effects=True, vmem_limit_bytes=VMEM_BYTES
            ),
        )(
            *(
                pltpu.with_memory_space_constraint(a, pltpu.HBM)
                for a in (
                    spectrum,
                    sea_mask.reshape(chunks, 128),
                    wind_speed.reshape(chunks, 128),
                    wind_angle.reshape(chunks, 128),
                    jnp.asarray(tab),
                )
            )
        )
        moved = pltpu.VMEM((2, chunks + 2 * FAR, 8, 128), jnp.float32)
        new_spectrum, height, mean = pl.pallas_call(
            functools.partial(unpack_kernel, n, bins_dev),
            name="unpack",
            out_shape=(
                jax.ShapeDtypeStruct((bins_dev, cells), jnp.float32),
                jax.ShapeDtypeStruct((1, cells // n), jnp.float32),
                jax.ShapeDtypeStruct((1, 1), jnp.float32),
            ),
            in_specs=[vmem] * 4,
            out_specs=(pl.BlockSpec(memory_space=pl.ANY),) * 3,
            scratch_shapes=[
                moved,
                moved,
                pltpu.VMEM((32, 16, 128), jnp.float32),
                pltpu.VMEM((chunks, 128), jnp.float32),
                pltpu.VMEM((bins_dev, cells), jnp.float32),
                pltpu.VMEM((1, cells // n), jnp.float32),
                pltpu.VMEM((1, 1), jnp.float32),
                pltpu.SemaphoreType.DMA((chunks // (2 * UNROLL) + 2,)),
            ],
            compiler_params=pltpu.CompilerParams(vmem_limit_bytes=VMEM_BYTES),
        )(home, go_right, put, sea_mask.reshape(chunks, 128))
        return new_spectrum, height.reshape(-1), mean.reshape(1)

    return jax.shard_map(
        local,
        mesh=mesh,
        in_specs=(P(("grp", "spec"), None), P(), P("grp"), P("grp")),
        out_specs=(P(("grp", "spec"), None), P(("grp", "spec")), P("grp")),
        check_vma=False,
    )
```

```python
import functools
import math

import jax
import jax.numpy as jnp
import numpy as np
from jax import lax
from jax.experimental import pallas as pl
from jax.experimental.pallas import tpu as pltpu
from jax.sharding import PartitionSpec as P

NF = 48
ND = 32
NLON = 384
SUBSTEPS = 2
SEA_DEV = 64
MESH = pl.DeviceIdType.MESH
LOG_RATIO = math.log(1.1)
PAIRS = ND // 2
ROW_STEPS = 6
REACH = 32
UNROLL = 8
VMEM_BYTES = 24 * 1024 * 1024
FAR = 56


def tables(lat_count):
    heading = 2.0 * np.pi * (np.arange(ND) + 0.5) / ND
    wrapped = np.concatenate([heading, heading[:24]])
    flat = lambda a: np.repeat(np.asarray(a)[:, None], 128, 1)
    paired = np.repeat(heading.reshape(PAIRS, 2), SEA_DEV, axis=1)
    latitude = np.radians(-75.0 + 150.0 * (np.arange(lat_count) + 0.5) / lat_count)
    k = np.arange(NF)
    rows, at = [], {}
    for name, block in (
        ("cos", flat(np.cos(wrapped))),
        ("sin", flat(np.sin(wrapped))),
        ("pair_cos", np.cos(paired)),
        ("pair_sin", np.sin(paired)),
        ("widen", flat(1.0 / np.cos(latitude))),
        ("omega", flat(np.exp(LOG_RATIO * (k - NF // 2)))),
        ("rate", flat(np.where((k >= 3) & (k <= NF - 3), 0.001, 0.0))),
    ):
        at[name] = sum(len(r) for r in rows)
        rows.append(block)
    return np.concatenate(rows).astype(np.float32), at


def chip_order(side):
    hops = lambda d: min(d, side - d)
    way = lambda d: (d > 0) - 2 * (d > side // 2)
    chips = [(x, y) for x in range(side) for y in range(side)][1:]
    chips.sort(key=lambda o: (-(hops(o[0]) + hops(o[1])), 3 * o[0] + 5 * o[1]))
    kinds = {}
    for o in chips:
        kinds.setdefault((way(o[0]), way(o[1])), []).append(o)
    placed = [((i + 0.5) / len(k), o) for k in kinds.values() for i, o in enumerate(k)]
    return [o for _, o in sorted(placed, key=lambda p: p[0])]


def word_of(words, v):
    return jnp.broadcast_to(words[pl.ds(REACH + v, 1), :], (8, 128))


def has(word, i):
    return jnp.bitwise_and(word, 1 << i) != 0


def lanes(tile, index, v):
    index = jnp.broadcast_to(index[pl.ds(v, 1), :], (8, 128))
    return jnp.take_along_axis(tile, index, axis=1, mode="promise_in_bounds")


def near_rows(chunks, words, src, emit, toward_end, bit_order):
    way = 1 if toward_end else -1

    def block(g, carry):
        first = g * UNROLL
        span = [first + way * u if toward_end else first + UNROLL - 1 - u for u in range(UNROLL + 7)]
        for t in range(2):
            word = [word_of(words.at[t], v) for v in span]
            cur = [src[t, FAR + v] for v in span]
            for b in bit_order:
                d = 1 << b
                cur = [
                    jnp.where(has(word[u], b), cur[u + d], cur[u])
                    for u in range(len(cur) - d)
                ]
            for u in range(UNROLL):
                emit(t, u, span[u], cur[u])
        return carry

    lax.fori_loop(0, chunks // UNROLL, block, 0)


def far_rows(chunks, words, tiles, t, r, toward_end, bit_order):
    tiles = tiles + [None] * (chunks // 8 - len(tiles))
    word = [word_of(words.at[t], r + 8 * j) for j in range(chunks // 8)]
    for b in bit_order:
        d = (1 << (b - 3)) * (1 if toward_end else -1)
        moved = []
        for j, own in enumerate(tiles):
            other = tiles[j + d] if 0 <= j + d < len(tiles) else None
            if own is None or other is None:
                moved.append(other if own is None else own)
            else:
                moved.append(jnp.where(has(word[j], b), other, own))
        tiles = moved
    return tiles


def step_kernel(
    n, side, cores, at,
    x_hbm, mask_hbm, speed_hbm, angle_hbm, tab_hbm,
    home, go_right, put,
    x, mask2d, sea_float, speed2d, angle2d, tab, field_a, field_b, stage, shifts, go_left, pick, moved_a, moved_b,
    send, recv, back, swap, flat, energy, rolled, own, low_part, high_part,
    order, send_sem, recv_sem, load_sem, column_sem, first_sem,
):
    bins_dev, cells = x.shape
    half = bins_dev // 2
    chunks = cells // 128
    per_row = NLON // 128
    lat_count = cells // NLON
    me = lax.axis_index("spec")
    my_x, my_y, my_c = me // (side * cores), lax.rem(me // cores, side), lax.rem(me, cores)

    parts = 4
    part_cols = cells // parts
    small = [
        pltpu.make_async_copy(src, dst, load_sem.at[parts + k])
        for k, (src, dst) in enumerate(
            ((mask_hbm, mask2d), (tab_hbm, tab), (speed_hbm, speed2d), (angle_hbm, angle2d))
        )
    ]

    def load(part):
        cols = pl.ds(pl.multiple_of(part * part_cols, 128), part_cols)
        return pltpu.make_async_copy(x_hbm.at[:, cols], x.at[:, cols], load_sem.at[part])

    small[0].start()
    for part in range(parts):
        load(part).start()
    for copy in small[1:]:
        copy.start()

    def wrap(a):
        return jnp.bitwise_and(a, side - 1) if side & (side - 1) == 0 else lax.rem(a, side)

    def hop(u):
        return side // 2 + (1 - 2 * jnp.bitwise_and(u, 1)) * jnp.right_shift(u + 1, 1)

    def both_cores(act, px, py):
        first = (px * side + py) * cores
        act(first + my_c)
        for c in range(1, cores):
            act(first + jnp.where(my_c + c >= cores, my_c + c - cores, my_c + c))

    def own_chip(act):
        for c in range(1, cores):
            act(me - my_c + lax.rem(my_c + c, cores))

    chips = chip_order(side)
    other_rows = [o for o in chips if o[1] != 0]

    def peers(act, which, count):
        def chip(i, carry):
            both_cores(act, wrap(my_x + order[2 * which, i]), wrap(my_y + order[2 * which + 1, i]))
            return carry

        lax.fori_loop(0, count, chip, 0)

    is_first = me == 0
    is_second = me == 1
    below_first = jnp.logical_and(jnp.logical_and(my_x == 0, my_c == 0), my_y != 0)

    def signal(semaphore, to):
        pl.semaphore_signal(semaphore, inc=1, device_id={"spec": to}, device_id_type=MESH)

    def down_column(act):
        def one(u, carry):
            act((my_x * side + wrap(my_y + hop(u))) * cores + my_c)
            return carry

        lax.fori_loop(0, side - 1, one, 0)

    def along_row(act, own=None):
        def one(u, carry):
            both_cores(act, wrap(my_x + hop(u)), my_y)
            return carry

        lax.fori_loop(0, side - 1, one, 0)
        own_chip(act if own is None else own)

    def peers_as_known(act, own):
        along_row(act, own)

        @pl.when(jnp.logical_not(is_first))
        def _():
            def row_in(i, carry):
                pl.semaphore_wait(column_sem.at[wrap(my_y + i)], 1)
                return carry

            @pl.when(jnp.logical_not(below_first))
            def _():
                lax.fori_loop(1, side, row_in, 0)

            @pl.when(is_second)
            def _():
                down_column(lambda to: signal(column_sem.at[0], to - 1))

            @pl.when(below_first)
            def _():
                lax.fori_loop(1, side, row_in, 0)

        peers(act, 1, len(other_rows))

    barrier = pltpu.get_barrier_semaphore()

    @pl.when(jnp.logical_not(is_first))
    def _():
        along_row(lambda to: signal(barrier, to))
        down_column(lambda to: signal(barrier, to))

    def entered():
        called = side * cores + side - 2

        @pl.when(jnp.logical_not(is_first))
        def _():
            with_first = jnp.logical_or(my_y == 0, below_first)
            pl.semaphore_wait(barrier, called - jnp.where(with_first, 1, 0))

            def complete(to):
                @pl.when(to == 0)
                def _():
                    signal(barrier, to)

                @pl.when(to != 0)
                def _():
                    signal(column_sem.at[my_y], to)

            down_column(complete)

    for which, table in enumerate((chips, other_rows)):
        for i, (dx, dy) in enumerate(table):
            order[2 * which, i] = dx
            order[2 * which + 1, i] = dy
    small[0].wait()

    lane = lax.broadcasted_iota(jnp.int32, (8, 128), 1)
    row = lax.broadcasted_iota(jnp.int32, (8, 128), 0)
    low = lane < SEA_DEV

    is_sea = mask2d[...] != 0
    sea_float[...] = mask2d[...].astype(jnp.float32)
    land = jnp.where(is_sea, 0.0, 1.0).astype(jnp.bfloat16)
    earlier = (
        lax.broadcasted_iota(jnp.int32, (128, 128), 0) < lax.broadcasted_iota(jnp.int32, (128, 128), 1)
    ).astype(jnp.bfloat16)
    above = (
        lax.broadcasted_iota(jnp.int32, (chunks, chunks), 1)
        < lax.broadcasted_iota(jnp.int32, (chunks, chunks), 0)
    ).astype(jnp.bfloat16)
    ones = jnp.ones((128, 128), jnp.bfloat16)
    count = functools.partial(jnp.dot, preferred_element_type=jnp.float32)
    before = count(land, earlier).astype(jnp.int32)
    sea_in_row = 128 - count(land, ones).astype(jnp.int32)
    wide_lane = lax.broadcasted_iota(jnp.int32, (chunks, 128), 1)
    wide_row = lax.broadcasted_iota(jnp.int32, (chunks, 128), 0)
    rank0 = wide_row * 128 - count(count(above, land).astype(jnp.bfloat16), ones).astype(jnp.int32)
    put[0] = jnp.bitwise_and(rank0 + wide_lane - before, 127)
    put[1] = jnp.bitwise_and(rank0 + wide_lane - before + SEA_DEV, 127)
    to_go = jnp.where(is_sea, before, 0)
    shifts[chunks:, :] = jnp.zeros((shifts.shape[0] - chunks, 128), jnp.int32)
    go_left[...] = jnp.zeros_like(go_left)
    go_right[...] = jnp.zeros_like(go_right)

    def close_up(i, to_go):
        d = jnp.left_shift(1, i)
        incoming = pltpu.roll(to_go, 128 - d, 1)
        stay = jnp.where(jnp.bitwise_and(to_go, d) != 0, 0, to_go)
        return jnp.where(jnp.bitwise_and(incoming, d) != 0, incoming, stay)

    def plan_rows(to_go):
        nth = jnp.bitwise_and(wide_lane - rank0, 127)
        front = jnp.bitwise_and(wide_lane + to_go, 127)
        took = jnp.take_along_axis(front, nth, axis=1, mode="promise_in_bounds")
        pick[0] = took
        pick[1] = pltpu.roll(took, SEA_DEV, 1)
        up = wide_row - jnp.right_shift(rank0 + nth, 7)
        shifts[0:chunks, :] = jnp.where(nth < sea_in_row, up, 0)
        for b in range(ROW_STEPS):
            here, incoming = shifts[0:chunks, :], shifts[1 << b : chunks + (1 << b), :]
            goes = jnp.bitwise_and(here, 1 << b)
            comes = jnp.bitwise_and(incoming, 1 << b)
            rights, lefts = (goes, comes) if b == 0 else (rights + goes, lefts + comes)
            shifts[0:chunks, :] = jnp.where(comes != 0, incoming, jnp.where(goes != 0, 0, here))
        for words, found in ((go_right, rights), (go_left, lefts)):
            words[0, REACH : REACH + chunks, :] = found
            words[1, REACH : REACH + chunks, :] = pltpu.roll(found, SEA_DEV, 1)

    zero = jnp.zeros((8, 128), jnp.float32)
    pad = per_row
    for t in range(2):
        for v in range(pad):
            for f in (field_a, field_b):
                f[t, v] = zero
                f[t, pad + chunks + v] = zero
    base = (me * bins_dev) % ND
    for copy in small[1:]:
        copy.wait()
    pace_x, pace_y, from_west, from_south, beside, edge = [], [], [], [], [], []
    for t in range(2):
        k = ((me * bins_dev + jnp.minimum(2 * row + t, bins_dev - 1)) // ND).astype(jnp.float32)
        pace = 0.2 * jnp.exp(-LOG_RATIO * k)
        ax = pace * tab[pl.ds(at["cos"] + base + t, 8, stride=2), :]
        ay = pace * tab[pl.ds(at["sin"] + base + t, 8, stride=2), :]
        pace_x.append(jnp.abs(ax))
        pace_y.append(jnp.abs(ay))
        from_west.append(ax >= 0.0)
        from_south.append(ay >= 0.0)
        beside.append(jnp.bitwise_and(jnp.where(from_west[t], lane - 1, lane + 1), 127))
        edge.append(
            (
                jnp.logical_and(from_west[t], lane == 0),
                jnp.logical_and(jnp.logical_not(from_west[t]), lane == 127),
            )
        )

    def split_bins(g, carry):
        for u in range(8):
            v = g * 8 + u
            cols = pl.ds(pl.multiple_of(v * 128, 128), 128)
            stage[u, 0:bins_dev, :] = x[:, cols] * sea_float[pl.ds(v, 1), :]
            for t in range(2):
                field_a[t, pad + v, 0:half, :] = stage[u, pl.ds(t, half, stride=2), :]
        return carry

    def split_part(part, carry):
        load(part).wait()
        per_part = chunks // 8 // parts
        return lax.fori_loop(part * per_part, (part + 1) * per_part, split_bins, carry)

    lax.fori_loop(0, parts, split_part, 0)

    for s in range(SUBSTEPS):
        src, dst = (field_a, field_b) if s % 2 == 0 else (field_b, field_a)

        def advance(g, to_go, src=src, dst=dst, s=s):
            if s == 0:
                for i in range(4):
                    to_go = close_up(4 * g + i, to_go)
            for ru in range(16):
                r = g * 16 + ru
                widen = tab[pl.ds(at["widen"] + r, 1), :]
                first = pad + r * per_row
                for t in range(2):
                    side_c = pace_x[t] * widen
                    own_c = 1.0 - side_c - pace_y[t]
                    first = pad + r * per_row
                    e = [src[t, first + q] for q in range(per_row)]
                    turned = [jnp.take_along_axis(a, beside[t], axis=1, mode="promise_in_bounds") for a in e]
                    for q in range(per_row):
                        across = jnp.where(edge[t][0], turned[q - 1], turned[q])
                        across = jnp.where(edge[t][1], turned[(q + 1) % per_row], across)
                        along = jnp.where(
                            from_south[t], src[t, first + q - per_row], src[t, first + q + per_row]
                        )
                        new = own_c * e[q] + side_c * across + pace_y[t] * along
                        v = first + q - pad
                        if s < SUBSTEPS - 1:
                            dst[t, first + q] = new * sea_float[pl.ds(v, 1), :]
                        else:
                            wind = (speed2d, angle2d)[t][pl.ds(v, 1), :]
                            dst[t, first + q] = jnp.where(row == half, wind, new)
            return to_go

        to_go = lax.fori_loop(0, lat_count // 16, advance, to_go)
        if s == 0:
            plan_rows(to_go)
    final = field_a if SUBSTEPS % 2 == 0 else field_b
    entered()

    def to_lanes(g, carry):
        for u in range(4 * UNROLL):
            v = g * 4 * UNROLL + u
            for t in range(2):
                moved_a[t, FAR + v] = lanes(final[t, pad + v], pick.at[t], v)
        return carry

    lax.fori_loop(0, chunks // (4 * UNROLL), to_lanes, 0)


    def keep_near(t, u, v, tile):
        moved_b[t, FAR + v] = tile

    near_rows(chunks, go_left, moved_a, keep_near, True, (0, 1, 2))

    def pack(r, carry):
        even, odd = (
            far_rows(
                chunks, go_left, [moved_b[t, FAR + r + 8 * j] for j in range(chunks // 8)], t, r, True, (3, 4, 5)
            )
            for t in range(2)
        )
        for j in range(n * SEA_DEV // 128 // 8):
            v = r + 8 * j
            send[2 * v] = jnp.where(low, even[j], odd[j])
            send[2 * v + 1] = jnp.where(low, odd[j], even[j])
        return carry

    lax.fori_loop(0, 8, pack, 0)

    def finish(ref, count, rows, sem):
        part = ref.at[pl.ds(0, count), pl.ds(0, rows)]
        pltpu.make_async_copy(part, part, sem).wait()

    def copy_to(to, src, dst, k, arrival):
        pltpu.make_async_remote_copy(
            src_ref=src,
            dst_ref=dst,
            send_sem=send_sem.at[k],
            recv_sem=arrival,
            device_id={"spec": to},
            device_id_type=MESH,
        ).start()

    def own_message(src, dst, rows, arrival):
        pltpu.make_async_copy(src.at[me, pl.ds(0, rows)], dst.at[me, pl.ds(0, rows)], arrival).start()

    @pl.when(is_first)
    def _():
        pl.semaphore_wait(barrier, side * cores + 2 * side - 3)
        signal(first_sem, 1)

    def push(to):
        aside = jnp.where(to == 0, 1, 0)
        copy_to(
            to + aside,
            send.at[to, pl.ds(0, half)],
            recv.at[me + aside * n, pl.ds(0, half)],
            0,
            recv_sem.at[my_x + aside * side],
        )

    def push_own_chip(to):
        @pl.when(is_second)
        def _():
            pltpu.make_async_copy(
                send.at[0, pl.ds(0, half)], recv.at[n + 1, pl.ds(0, half)], recv_sem.at[side]
            ).start()

        @pl.when(jnp.logical_not(is_second))
        def _():
            copy_to(to, send.at[to, pl.ds(0, half)], recv.at[me, pl.ds(0, half)], 0, recv_sem.at[my_x])

    peers_as_known(push, push_own_chip)
    own_message(send, recv, half, recv_sem.at[my_x])

    @pl.when(is_second)
    def _():
        pl.semaphore_wait(first_sem, 1)

    def hand_over(h):
        def pass_on(start, count):
            finish(recv, count, half, recv_sem.at[side + h])
            copy_to(
                0,
                recv.at[pl.ds(n + start, count), pl.ds(0, half)],
                recv.at[pl.ds(start, count), pl.ds(0, half)],
                2,
                recv_sem.at[h],
            )

        @pl.when(jnp.logical_and(is_second, h != 0))
        def _():
            pass_on(h * side * cores, side * cores)

        @pl.when(jnp.logical_and(is_second, h == 0))
        def _():
            pass_on(1, side * cores - 1)


    wind = send[me][half : half + 1, :]
    other = pltpu.roll(wind, SEA_DEV, 1)
    odd_side = lax.rem(me, 2) * SEA_DEV
    even_half = lambda shape: jnp.bitwise_xor(lax.broadcasted_iota(jnp.int32, shape, 1), odd_side) < SEA_DEV
    low16 = even_half((PAIRS, 128))
    speed = jnp.where(even_half((1, 128)), wind, other)
    angle = jnp.where(even_half((1, 128)), other, wind)

    def paired(name):
        rows = tab[at[name] : at[name] + PAIRS, :]
        return jnp.where(odd_side == 0, rows, pltpu.roll(rows, SEA_DEV, 1))

    toward = speed * (paired("pair_cos") * jnp.cos(angle) + paired("pair_sin") * jnp.sin(angle))
    zero16 = jnp.zeros((PAIRS, 128), jnp.float32)
    for w in range(4):
        for k in (0, 1, 2, NF + 3, NF + 4):
            rolled[w, k] = zero16
    for k in range(2):
        low_part[k] = zero16
    for k in range(3):
        high_part[NF + k] = zero16

    def turns(a, amounts):
        s = pltpu.roll(a, SEA_DEV, 1)
        need = {1: (1, 0), -1: (0, -1), 3: (2, 1), -3: (-1, -2)}
        by = {0: s}
        for m in amounts:
            for w in need[m]:
                if w not in by:
                    by[w] = pltpu.roll(s, w % PAIRS, 0)
        return [jnp.where(low16, by[need[m][0]], by[need[m][1]]) for m in amounts]

    group = 8
    per_group = half * group // PAIRS

    def arrange(i, carry):
        m0, m1 = carry
        h = lax.rem(i + 1, side)
        hand_over(h)
        finish(recv, side * cores, half, recv_sem.at[h])
        for g in (2 * h, 2 * h + 1):
            for i in range(group):
                flat[g, half * i : half * i + half, :] = recv[g * group + i, 0:half, :]
        for g in (2 * h, 2 * h + 1):
            for q in range(per_group):
                k = g * per_group + q
                a = flat[g, PAIRS * q : PAIRS * (q + 1), :]
                energy[k] = a
                m0 = m0 + a
                m1 = m1 + tab[pl.ds(at["omega"] + k, 1), :] * a
                for w, b in enumerate(turns(a, (1, -1, 3, -3))):
                    rolled[w, k + 3] = b
        return m0, m1

    m0, m1 = lax.fori_loop(0, side, arrange, (zero16, zero16))

    def over_bins(a):
        a = jnp.sum(a, axis=0, keepdims=True)
        return (a + pltpu.roll(a, SEA_DEV, 1)) * (1.0 / (NF * ND))

    m0, m1 = over_bins(m0), over_bins(m1)
    mean_freq = m1 / (m0 + 1e-6)
    steep = m0 * mean_freq * mean_freq
    breaking = steep * steep / (1.0 + steep * steep)

    def transfer(g, carry):
        for q in range(4 * per_group):
            k = g * 4 * per_group + q
            a = energy[k]
            factor = tab[pl.ds(at["rate"] + k, 1), :] * a
            rates = []
            for plus, minus in ((rolled[1, k + 5], rolled[2, k]), (rolled[0, k + 5], rolled[3, k])):
                rates.append(factor * (a * (plus + minus) - 2.0 * plus * minus))
            up, down = turns(rates[0], (1, -3)), turns(rates[1], (-1, 3))
            own[k] = -2.0 * (rates[0] + rates[1])
            low_part[k + 2] = up[0] + down[0]
            high_part[k] = up[1] + down[1]
        return carry

    lax.fori_loop(0, n // group // 4, transfer, 0)

    def renew(h, total):
        for g in (2 * h, 2 * h + 1):
            for q in range(per_group):
                k = g * per_group + q
                a = energy[k]
                omega = tab[pl.ds(at["omega"] + k, 1), :]
                gain = (0.05 * omega) * jnp.maximum(0.0, omega * toward - 1.0)
                new = a + (gain - (0.03 * omega) * breaking) * a
                new = new + own[k] + low_part[k] + high_part[k + 3]
                total = total + new
                flat[g, PAIRS * q : PAIRS * (q + 1), :] = new
        for g in (2 * h, 2 * h + 1):
            for i in range(group):
                back[g * group + i, 0:half, :] = flat[g, half * i : half * i + half, :]
        return total

    total = lax.fori_loop(0, n // group // 2, renew, zero16)
    height = 4.0 * jnp.sqrt(over_bins(total) + 1e-6)

    swap[0, 0:1, :] = height
    partner = me + 1 - 2 * my_c
    copy_to(partner, swap.at[0, pl.ds(0, 1)], swap.at[1, pl.ds(0, 1)], 4, recv_sem.at[2 * side + 2])

    def push_back(to, rows, k):
        copy_to(
            to,
            back.at[to, pl.ds(0, rows)],
            home.at[me, pl.ds(0, rows)],
            (1, 3)[k],
            recv_sem.at[2 * side + k],
        )

    def on_core(core, rows, k):
        def chip(i, carry):
            px, py = wrap(my_x + order[0, i]), wrap(my_y + order[1, i])
            push_back((px * side + py) * cores + core, rows, k)
            return carry

        lax.fori_loop(0, len(chips), chip, 0)

    on_core(1 - my_c, half, 0)
    push_back(partner, half, 0)
    swapped = swap.at[1, pl.ds(0, 1)]
    pltpu.make_async_copy(swapped, swapped, recv_sem.at[2 * side + 2]).wait()
    theirs = swap[1, 0:1, :]
    both_heights = jnp.where(even_half((1, 128)), height, theirs)

    def add_height(g, carry):
        for i in range(group):
            back[g * group + i, half : half + 1, :] = both_heights
        return carry

    lax.fori_loop(0, n // group, add_height, 0)
    on_core(my_c, half + 1, 1)
    own_message(back, home, half + 1, recv_sem.at[2 * side + 1])

    @pl.when(is_second)
    def _():
        finish(send, n - 2, half, send_sem.at[0])
        finish(recv, n - 1, half, send_sem.at[2])

    @pl.when(jnp.logical_not(is_second))
    def _():
        finish(send, n - 1, half, send_sem.at[0])

    finish(home, n // cores, half, recv_sem.at[2 * side])
    finish(home, n // cores, half + 1, recv_sem.at[2 * side + 1])
    finish(back, n // cores, half, send_sem.at[1])
    finish(back, n // cores - 1, half + 1, send_sem.at[3])
    pltpu.make_async_copy(swapped, swapped, send_sem.at[4]).wait()


def unpack_kernel(
    n, bins_dev,
    home, go_right, put, mask2d,
    out, height_out, mean_out,
    moved_a, moved_b, stage, heights, result, own_heights, mean, write_sem,
):
    chunks = mask2d.shape[0]
    half = bins_dev // 2
    cells = chunks * 128
    per_row = NLON // 128
    me = lax.axis_index("spec")
    lane = lax.broadcasted_iota(jnp.int32, (8, 128), 1)
    low = lane < SEA_DEV

    row = lax.broadcasted_iota(jnp.int32, (8, 128), 0)
    own_core = jnp.where(lax.rem(me, 2) == 0, 0, SEA_DEV)
    from_even = (jnp.where(row == half, own_core, lane) < SEA_DEV, jnp.logical_not(low))

    def spread(r, carry):
        pairs = [(home[2 * (r + 8 * j)], home[2 * (r + 8 * j) + 1]) for j in range(n * SEA_DEV // 128 // 8)]
        for t in range(2):
            tiles = [jnp.where(from_even[t], p[0], p[1]) for p in pairs]
            for j, tile in enumerate(far_rows(chunks, go_right, tiles, t, r, False, (5, 4, 3))):
                moved_b[t, FAR + r + 8 * j] = tile
        return carry

    lax.fori_loop(0, 8, spread, 0)

    def keep_apart(t, u, v, tile):
        moved_a[t, FAR + v] = tile

    near_rows(chunks, go_right, moved_b, keep_apart, False, (2, 1, 0))

    width = 2 * UNROLL * 128

    def write(g):
        cols = pl.ds(pl.multiple_of(g * width, 128), width)
        return pltpu.make_async_copy(result.at[:, cols], out.at[:, cols], write_sem.at[g])

    def deliver(g, carry):
        for u in range(4 * UNROLL):
            v = g * 4 * UNROLL + u
            sea = jnp.broadcast_to(mask2d[pl.ds(v, 1), :] != 0, (8, 128))
            for t in range(2):
                tile = jnp.where(sea, lanes(moved_a[t, FAR + v], put.at[t], v), 0.0)
                stage[u, pl.ds(t, half, stride=2), :] = tile[0:half]
                if t == 0:
                    heights[pl.ds(v, 1), :] = tile[half : half + 1]
        for part in range(2):
            for u in range(part * 2 * UNROLL, (part + 1) * 2 * UNROLL):
                v = g * 4 * UNROLL + u
                result[:, pl.ds(pl.multiple_of(v * 128, 128), 128)] = stage[u, 0:bins_dev, :]
            write(2 * g + part).start()
        return carry

    lax.fori_loop(0, chunks // (4 * UNROLL), deliver, 0)

    points = cells // n
    together = NLON // points
    start = me // together * per_row
    three = [heights[pl.ds(start + q, 1), :] for q in range(per_row)]
    u = lax.rem(me, together)
    picked = None
    for g in range(together):
        first, offset = g * points // 128, g * points % 128
        piece = three[first]
        if offset:
            after = three[min(first + 1, per_row - 1)]
            piece = jnp.where(
                lane[0:1] < 128 - offset,
                pltpu.roll(piece, 128 - offset, 1),
                pltpu.roll(after, 128 - offset, 1),
            )
        picked = piece if picked is None else jnp.where(u == g, piece, picked)
    own_heights[...] = picked[:, 0:points]
    all_heights = jnp.sum(heights[...], axis=0, keepdims=True)
    mean[...] = jnp.sum(all_heights, axis=1, keepdims=True) * (1.0 / (SEA_DEV * n))

    small = (
        pltpu.make_async_copy(own_heights, height_out, write_sem.at[cells // width]),
        pltpu.make_async_copy(mean, mean_out, write_sem.at[cells // width + 1]),
    )
    for copy in small:
        copy.start()

    def written(g, carry):
        write(g).wait()
        return carry

    lax.fori_loop(0, cells // width, written, 0)
    for copy in small:
        copy.wait()


def solution(mesh):
    n = mesh.shape["spec"]
    cores = 2
    side = math.isqrt(n // cores)

    def local(spectrum, sea_mask, wind_speed, wind_angle):
        bins_dev, cells = spectrum.shape
        chunks = cells // 128
        padded = chunks + 2 * (NLON // 128)
        tab, at = tables(cells // NLON)
        vmem = pl.BlockSpec(memory_space=pltpu.VMEM)
        words = pltpu.VMEM((2, chunks + 2 * REACH, 128), jnp.int32)
        by_freq = lambda *dims: pltpu.VMEM((*dims, PAIRS, 128), jnp.float32)
        messages = lambda count: pltpu.VMEM((count, 8, 128), jnp.float32)
        home, go_right, put = pl.pallas_call(
            functools.partial(step_kernel, n, side, cores, at),
            name="wave_step",
            out_shape=(
                jax.ShapeDtypeStruct((n, 8, 128), jnp.float32),
                jax.ShapeDtypeStruct((2, chunks + 2 * REACH, 128), jnp.int32),
                jax.ShapeDtypeStruct((2, chunks, 128), jnp.int32),
            ),
            in_specs=[pl.BlockSpec(memory_space=pltpu.HBM)] * 5,
            out_specs=(vmem,) * 3,
            scratch_shapes=[
                pltpu.VMEM((bins_dev, cells), jnp.float32),
                pltpu.VMEM((chunks, 128), jnp.int32),
                pltpu.VMEM((chunks, 128), jnp.float32),
                pltpu.VMEM((chunks, 128), jnp.float32),
                pltpu.VMEM((chunks, 128), jnp.float32),
                pltpu.VMEM(tab.shape, jnp.float32),
                pltpu.VMEM((2, padded, 8, 128), jnp.float32),
                pltpu.VMEM((2, padded, 8, 128), jnp.float32),
                pltpu.VMEM((8, 16, 128), jnp.float32),
                pltpu.VMEM((chunks + REACH, 128), jnp.int32),
                words,
                pltpu.VMEM((2, chunks, 128), jnp.int32),
                pltpu.VMEM((2, chunks + 2 * FAR, 8, 128), jnp.float32),
                pltpu.VMEM((2, chunks + 2 * FAR, 8, 128), jnp.float32),
                messages(n),
                messages(2 * n),
                messages(n),
                messages(2),
                pltpu.VMEM((n // 8, 8 * bins_dev // 2, 128), jnp.float32),
                by_freq(NF),
                by_freq(4, NF + 5),
                by_freq(NF),
                by_freq(NF + 2),
                by_freq(NF + 3),
                pltpu.SMEM((4, side * side), jnp.int32),
                pltpu.SemaphoreType.DMA((5,)),
                pltpu.SemaphoreType.DMA((2 * side + 3,)),
                pltpu.SemaphoreType.DMA((8,)),
                pltpu.SemaphoreType.REGULAR((side,)),
                pltpu.SemaphoreType.REGULAR,
            ],
            compiler_params=pltpu.CompilerParams(
                collective_id=0, has_side_effects=True, vmem_limit_bytes=VMEM_BYTES
            ),
        )(
            *(
                pltpu.with_memory_space_constraint(a, pltpu.HBM)
                for a in (
                    spectrum,
                    sea_mask.reshape(chunks, 128),
                    wind_speed.reshape(chunks, 128),
                    wind_angle.reshape(chunks, 128),
                    jnp.asarray(tab),
                )
            )
        )
        moved = pltpu.VMEM((2, chunks + 2 * FAR, 8, 128), jnp.float32)
        new_spectrum, height, mean = pl.pallas_call(
            functools.partial(unpack_kernel, n, bins_dev),
            name="unpack",
            out_shape=(
                jax.ShapeDtypeStruct((bins_dev, cells), jnp.float32),
                jax.ShapeDtypeStruct((1, cells // n), jnp.float32),
                jax.ShapeDtypeStruct((1, 1), jnp.float32),
            ),
            in_specs=[vmem] * 4,
            out_specs=(pl.BlockSpec(memory_space=pl.ANY),) * 3,
            scratch_shapes=[
                moved,
                moved,
                pltpu.VMEM((32, 16, 128), jnp.float32),
                pltpu.VMEM((chunks, 128), jnp.float32),
                pltpu.VMEM((bins_dev, cells), jnp.float32),
                pltpu.VMEM((1, cells // n), jnp.float32),
                pltpu.VMEM((1, 1), jnp.float32),
                pltpu.SemaphoreType.DMA((chunks // (2 * UNROLL) + 2,)),
            ],
            compiler_params=pltpu.CompilerParams(vmem_limit_bytes=VMEM_BYTES),
        )(home, go_right, put, sea_mask.reshape(chunks, 128))
        return new_spectrum, height.reshape(-1), mean.reshape(1)

    return jax.shard_map(
        local,
        mesh=mesh,
        in_specs=(P(("grp", "spec"), None), P(), P("grp"), P("grp")),
        out_specs=(P(("grp", "spec"), None), P(("grp", "spec")), P("grp")),
        check_vma=False,
    )
```

```python
import functools
import math

import jax
import jax.numpy as jnp
import numpy as np
from jax import lax
from jax.experimental import pallas as pl
from jax.experimental.pallas import tpu as pltpu
from jax.sharding import PartitionSpec as P

NF = 48
ND = 32
NLON = 384
SUBSTEPS = 2
SEA_DEV = 64
MESH = pl.DeviceIdType.MESH
LOG_RATIO = math.log(1.1)
PAIRS = ND // 2
ROW_STEPS = 6
REACH = 32
UNROLL = 8
VMEM_BYTES = 24 * 1024 * 1024
FAR = 56


def tables(lat_count):
    heading = 2.0 * np.pi * (np.arange(ND) + 0.5) / ND
    wrapped = np.concatenate([heading, heading[:24]])
    flat = lambda a: np.repeat(np.asarray(a)[:, None], 128, 1)
    paired = np.repeat(heading.reshape(PAIRS, 2), SEA_DEV, axis=1)
    latitude = np.radians(-75.0 + 150.0 * (np.arange(lat_count) + 0.5) / lat_count)
    k = np.arange(NF)
    rows, at = [], {}
    for name, block in (
        ("cos", flat(np.cos(wrapped))),
        ("sin", flat(np.sin(wrapped))),
        ("pair_cos", np.cos(paired)),
        ("pair_sin", np.sin(paired)),
        ("widen", flat(1.0 / np.cos(latitude))),
        ("omega", flat(np.exp(LOG_RATIO * (k - NF // 2)))),
        ("rate", flat(np.where((k >= 3) & (k <= NF - 3), 0.001, 0.0))),
    ):
        at[name] = sum(len(r) for r in rows)
        rows.append(block)
    return np.concatenate(rows).astype(np.float32), at


def chip_order(side):
    hops = lambda d: min(d, side - d)
    way = lambda d: (d > 0) - 2 * (d > side // 2)
    chips = [(x, y) for x in range(side) for y in range(side)][1:]
    chips.sort(key=lambda o: (-(hops(o[0]) + hops(o[1])), 3 * o[0] + 5 * o[1]))
    kinds = {}
    for o in chips:
        kinds.setdefault((way(o[0]), way(o[1])), []).append(o)
    placed = [((i + 0.5) / len(k), o) for k in kinds.values() for i, o in enumerate(k)]
    return [o for _, o in sorted(placed, key=lambda p: p[0])]


def word_of(words, v):
    return jnp.broadcast_to(words[pl.ds(REACH + v, 1), :], (8, 128))


def has(word, i):
    return jnp.bitwise_and(word, 1 << i) != 0


def lanes(tile, index, v):
    index = jnp.broadcast_to(index[pl.ds(v, 1), :], (8, 128))
    return jnp.take_along_axis(tile, index, axis=1, mode="promise_in_bounds")


def near_rows(chunks, words, src, emit, toward_end, bit_order):
    way = 1 if toward_end else -1

    def block(g, carry):
        first = g * UNROLL
        span = [first + way * u if toward_end else first + UNROLL - 1 - u for u in range(UNROLL + 7)]
        for t in range(2):
            word = [word_of(words.at[t], v) for v in span]
            cur = [src[t, FAR + v] for v in span]
            for b in bit_order:
                d = 1 << b
                cur = [
                    jnp.where(has(word[u], b), cur[u + d], cur[u])
                    for u in range(len(cur) - d)
                ]
            for u in range(UNROLL):
                emit(t, u, span[u], cur[u])
        return carry

    lax.fori_loop(0, chunks // UNROLL, block, 0)


def far_rows(chunks, words, tiles, t, r, toward_end, bit_order):
    tiles = tiles + [None] * (chunks // 8 - len(tiles))
    word = [word_of(words.at[t], r + 8 * j) for j in range(chunks // 8)]
    for b in bit_order:
        d = (1 << (b - 3)) * (1 if toward_end else -1)
        moved = []
        for j, own in enumerate(tiles):
            other = tiles[j + d] if 0 <= j + d < len(tiles) else None
            if own is None or other is None:
                moved.append(other if own is None else own)
            else:
                moved.append(jnp.where(has(word[j], b), other, own))
        tiles = moved
    return tiles


def step_kernel(
    n, side, cores, at,
    x_hbm, mask_hbm, speed_hbm, angle_hbm, tab_hbm,
    home, go_right, put,
    x, mask2d, sea_float, speed2d, angle2d, tab, field_a, field_b, stage, shifts, go_left, pick, moved_a, moved_b,
    send, recv, back, swap, flat, energy, rolled, own, low_part, high_part,
    order, send_sem, recv_sem, load_sem, column_sem, first_sem,
):
    bins_dev, cells = x.shape
    half = bins_dev // 2
    chunks = cells // 128
    per_row = NLON // 128
    lat_count = cells // NLON
    me = lax.axis_index("spec")
    my_x, my_y, my_c = me // (side * cores), lax.rem(me // cores, side), lax.rem(me, cores)

    parts = 4
    part_cols = cells // parts
    small = [
        pltpu.make_async_copy(src, dst, load_sem.at[parts + k])
        for k, (src, dst) in enumerate(
            ((mask_hbm, mask2d), (tab_hbm, tab), (speed_hbm, speed2d), (angle_hbm, angle2d))
        )
    ]

    def load(part):
        cols = pl.ds(pl.multiple_of(part * part_cols, 128), part_cols)
        return pltpu.make_async_copy(x_hbm.at[:, cols], x.at[:, cols], load_sem.at[part])

    small[0].start()
    for part in range(parts):
        load(part).start()
    for copy in small[1:]:
        copy.start()

    def wrap(a):
        return jnp.bitwise_and(a, side - 1) if side & (side - 1) == 0 else lax.rem(a, side)

    def hop(u):
        return side // 2 + (1 - 2 * jnp.bitwise_and(u, 1)) * jnp.right_shift(u + 1, 1)

    def both_cores(act, px, py):
        first = (px * side + py) * cores
        act(first + my_c)
        for c in range(1, cores):
            act(first + jnp.where(my_c + c >= cores, my_c + c - cores, my_c + c))

    def own_chip(act):
        for c in range(1, cores):
            act(me - my_c + lax.rem(my_c + c, cores))

    chips = chip_order(side)
    other_rows = [o for o in chips if o[1] != 0]

    def peers(act, which, count):
        def chip(i, carry):
            both_cores(act, wrap(my_x + order[2 * which, i]), wrap(my_y + order[2 * which + 1, i]))
            return carry

        lax.fori_loop(0, count, chip, 0)

    is_first = me == 0
    is_second = me == 1
    below_first = jnp.logical_and(jnp.logical_and(my_x == 0, my_c == 0), my_y != 0)

    def signal(semaphore, to):
        pl.semaphore_signal(semaphore, inc=1, device_id={"spec": to}, device_id_type=MESH)

    def down_column(act):
        def one(u, carry):
            act((my_x * side + wrap(my_y + hop(u))) * cores + my_c)
            return carry

        lax.fori_loop(0, side - 1, one, 0)

    def along_row(act, own=None):
        def one(u, carry):
            both_cores(act, wrap(my_x + hop(u)), my_y)
            return carry

        lax.fori_loop(0, side - 1, one, 0)
        own_chip(act if own is None else own)

    def peers_as_known(act, own):
        along_row(act, own)

        @pl.when(jnp.logical_not(is_first))
        def _():
            def row_in(i, carry):
                pl.semaphore_wait(column_sem.at[wrap(my_y + i)], 1)
                return carry

            @pl.when(jnp.logical_not(below_first))
            def _():
                lax.fori_loop(1, side, row_in, 0)

            @pl.when(is_second)
            def _():
                down_column(lambda to: signal(column_sem.at[0], to - 1))

            @pl.when(below_first)
            def _():
                lax.fori_loop(1, side, row_in, 0)

        peers(act, 1, len(other_rows))

    barrier = pltpu.get_barrier_semaphore()

    @pl.when(jnp.logical_not(is_first))
    def _():
        along_row(lambda to: signal(barrier, to))
        down_column(lambda to: signal(barrier, to))

    def entered():
        called = side * cores + side - 2

        @pl.when(jnp.logical_not(is_first))
        def _():
            with_first = jnp.logical_or(my_y == 0, below_first)
            pl.semaphore_wait(barrier, called - jnp.where(with_first, 1, 0))

            def complete(to):
                @pl.when(to == 0)
                def _():
                    signal(barrier, to)

                @pl.when(to != 0)
                def _():
                    signal(column_sem.at[my_y], to)

            down_column(complete)

    for which, table in enumerate((chips, other_rows)):
        for i, (dx, dy) in enumerate(table):
            order[2 * which, i] = dx
            order[2 * which + 1, i] = dy
    small[0].wait()

    lane = lax.broadcasted_iota(jnp.int32, (8, 128), 1)
    row = lax.broadcasted_iota(jnp.int32, (8, 128), 0)
    low = lane < SEA_DEV

    is_sea = mask2d[...] != 0
    sea_float[...] = mask2d[...].astype(jnp.float32)
    land = jnp.where(is_sea, 0.0, 1.0).astype(jnp.bfloat16)
    earlier = (
        lax.broadcasted_iota(jnp.int32, (128, 128), 0) < lax.broadcasted_iota(jnp.int32, (128, 128), 1)
    ).astype(jnp.bfloat16)
    above = (
        lax.broadcasted_iota(jnp.int32, (chunks, chunks), 1)
        < lax.broadcasted_iota(jnp.int32, (chunks, chunks), 0)
    ).astype(jnp.bfloat16)
    ones = jnp.ones((128, 128), jnp.bfloat16)
    count = functools.partial(jnp.dot, preferred_element_type=jnp.float32)
    before = count(land, earlier).astype(jnp.int32)
    sea_in_row = 128 - count(land, ones).astype(jnp.int32)
    wide_lane = lax.broadcasted_iota(jnp.int32, (chunks, 128), 1)
    wide_row = lax.broadcasted_iota(jnp.int32, (chunks, 128), 0)
    rank0 = wide_row * 128 - count(count(above, land).astype(jnp.bfloat16), ones).astype(jnp.int32)
    put[0] = jnp.bitwise_and(rank0 + wide_lane - before, 127)
    put[1] = jnp.bitwise_and(rank0 + wide_lane - before + SEA_DEV, 127)
    to_go = jnp.where(is_sea, before, 0)
    shifts[chunks:, :] = jnp.zeros((shifts.shape[0] - chunks, 128), jnp.int32)
    go_left[...] = jnp.zeros_like(go_left)
    go_right[...] = jnp.zeros_like(go_right)

    def close_up(i, to_go):
        d = jnp.left_shift(1, i)
        incoming = pltpu.roll(to_go, 128 - d, 1)
        stay = jnp.where(jnp.bitwise_and(to_go, d) != 0, 0, to_go)
        return jnp.where(jnp.bitwise_and(incoming, d) != 0, incoming, stay)

    def plan_rows(to_go):
        nth = jnp.bitwise_and(wide_lane - rank0, 127)
        front = jnp.bitwise_and(wide_lane + to_go, 127)
        took = jnp.take_along_axis(front, nth, axis=1, mode="promise_in_bounds")
        pick[0] = took
        pick[1] = pltpu.roll(took, SEA_DEV, 1)
        up = wide_row - jnp.right_shift(rank0 + nth, 7)
        shifts[0:chunks, :] = jnp.where(nth < sea_in_row, up, 0)
        for b in range(ROW_STEPS):
            here, incoming = shifts[0:chunks, :], shifts[1 << b : chunks + (1 << b), :]
            goes = jnp.bitwise_and(here, 1 << b)
            comes = jnp.bitwise_and(incoming, 1 << b)
            rights, lefts = (goes, comes) if b == 0 else (rights + goes, lefts + comes)
            shifts[0:chunks, :] = jnp.where(comes != 0, incoming, jnp.where(goes != 0, 0, here))
        for words, found in ((go_right, rights), (go_left, lefts)):
            words[0, REACH : REACH + chunks, :] = found
            words[1, REACH : REACH + chunks, :] = pltpu.roll(found, SEA_DEV, 1)

    zero = jnp.zeros((8, 128), jnp.float32)
    pad = per_row
    for t in range(2):
        for v in range(pad):
            for f in (field_a, field_b):
                f[t, v] = zero
                f[t, pad + chunks + v] = zero
    base = (me * bins_dev) % ND
    for copy in small[1:]:
        copy.wait()
    pace_x, pace_y, from_west, from_south, beside, edge = [], [], [], [], [], []
    for t in range(2):
        k = ((me * bins_dev + jnp.minimum(2 * row + t, bins_dev - 1)) // ND).astype(jnp.float32)
        pace = 0.2 * jnp.exp(-LOG_RATIO * k)
        ax = pace * tab[pl.ds(at["cos"] + base + t, 8, stride=2), :]
        ay = pace * tab[pl.ds(at["sin"] + base + t, 8, stride=2), :]
        pace_x.append(jnp.abs(ax))
        pace_y.append(jnp.abs(ay))
        from_west.append(ax >= 0.0)
        from_south.append(ay >= 0.0)
        beside.append(jnp.bitwise_and(jnp.where(from_west[t], lane - 1, lane + 1), 127))
        edge.append(
            (
                jnp.logical_and(from_west[t], lane == 0),
                jnp.logical_and(jnp.logical_not(from_west[t]), lane == 127),
            )
        )

    def split_bins(g, carry):
        for u in range(8):
            v = g * 8 + u
            cols = pl.ds(pl.multiple_of(v * 128, 128), 128)
            stage[u, 0:bins_dev, :] = x[:, cols] * sea_float[pl.ds(v, 1), :]
            for t in range(2):
                field_a[t, pad + v, 0:half, :] = stage[u, pl.ds(t, half, stride=2), :]
        return carry

    def split_part(part, carry):
        load(part).wait()
        per_part = chunks // 8 // parts
        return lax.fori_loop(part * per_part, (part + 1) * per_part, split_bins, carry)

    lax.fori_loop(0, parts, split_part, 0)

    for s in range(SUBSTEPS):
        src, dst = (field_a, field_b) if s % 2 == 0 else (field_b, field_a)

        def advance(g, to_go, src=src, dst=dst, s=s):
            if s == 0:
                for i in range(4):
                    to_go = close_up(4 * g + i, to_go)
            for ru in range(16):
                r = g * 16 + ru
                widen = tab[pl.ds(at["widen"] + r, 1), :]
                first = pad + r * per_row
                for t in range(2):
                    side_c = pace_x[t] * widen
                    own_c = 1.0 - side_c - pace_y[t]
                    first = pad + r * per_row
                    e = [src[t, first + q] for q in range(per_row)]
                    turned = [jnp.take_along_axis(a, beside[t], axis=1, mode="promise_in_bounds") for a in e]
                    for q in range(per_row):
                        across = jnp.where(edge[t][0], turned[q - 1], turned[q])
                        across = jnp.where(edge[t][1], turned[(q + 1) % per_row], across)
                        along = jnp.where(
                            from_south[t], src[t, first + q - per_row], src[t, first + q + per_row]
                        )
                        new = own_c * e[q] + side_c * across + pace_y[t] * along
                        v = first + q - pad
                        if s < SUBSTEPS - 1:
                            dst[t, first + q] = new * sea_float[pl.ds(v, 1), :]
                        else:
                            wind = (speed2d, angle2d)[t][pl.ds(v, 1), :]
                            dst[t, first + q] = jnp.where(row == half, wind, new)
            return to_go

        to_go = lax.fori_loop(0, lat_count // 16, advance, to_go)
        if s == 0:
            plan_rows(to_go)
    final = field_a if SUBSTEPS % 2 == 0 else field_b
    entered()

    def to_lanes(g, carry):
        for u in range(6 * UNROLL):
            v = g * 6 * UNROLL + u
            for t in range(2):
                moved_a[t, FAR + v] = lanes(final[t, pad + v], pick.at[t], v)
        return carry

    lax.fori_loop(0, chunks // (6 * UNROLL), to_lanes, 0)


    def keep_near(t, u, v, tile):
        moved_b[t, FAR + v] = tile

    near_rows(chunks, go_left, moved_a, keep_near, True, (0, 1, 2))

    def pack(r, carry):
        even, odd = (
            far_rows(
                chunks, go_left, [moved_b[t, FAR + r + 8 * j] for j in range(chunks // 8)], t, r, True, (3, 4, 5)
            )
            for t in range(2)
        )
        for j in range(n * SEA_DEV // 128 // 8):
            v = r + 8 * j
            send[2 * v] = jnp.where(low, even[j], odd[j])
            send[2 * v + 1] = jnp.where(low, odd[j], even[j])
        return carry

    lax.fori_loop(0, 8, pack, 0)

    def finish(ref, count, rows, sem):
        part = ref.at[pl.ds(0, count), pl.ds(0, rows)]
        pltpu.make_async_copy(part, part, sem).wait()

    def copy_to(to, src, dst, k, arrival):
        pltpu.make_async_remote_copy(
            src_ref=src,
            dst_ref=dst,
            send_sem=send_sem.at[k],
            recv_sem=arrival,
            device_id={"spec": to},
            device_id_type=MESH,
        ).start()

    def own_message(src, dst, rows, arrival):
        pltpu.make_async_copy(src.at[me, pl.ds(0, rows)], dst.at[me, pl.ds(0, rows)], arrival).start()

    @pl.when(is_first)
    def _():
        pl.semaphore_wait(barrier, side * cores + 2 * side - 3)
        signal(first_sem, 1)

    def push(to):
        aside = jnp.where(to == 0, 1, 0)
        copy_to(
            to + aside,
            send.at[to, pl.ds(0, half)],
            recv.at[me + aside * n, pl.ds(0, half)],
            0,
            recv_sem.at[my_x + aside * side],
        )

    def push_own_chip(to):
        @pl.when(is_second)
        def _():
            pltpu.make_async_copy(
                send.at[0, pl.ds(0, half)], recv.at[n + 1, pl.ds(0, half)], recv_sem.at[side]
            ).start()

        @pl.when(jnp.logical_not(is_second))
        def _():
            copy_to(to, send.at[to, pl.ds(0, half)], recv.at[me, pl.ds(0, half)], 0, recv_sem.at[my_x])

    peers_as_known(push, push_own_chip)
    own_message(send, recv, half, recv_sem.at[my_x])

    @pl.when(is_second)
    def _():
        pl.semaphore_wait(first_sem, 1)

    def hand_over(h):
        def pass_on(start, count):
            finish(recv, count, half, recv_sem.at[side + h])
            copy_to(
                0,
                recv.at[pl.ds(n + start, count), pl.ds(0, half)],
                recv.at[pl.ds(start, count), pl.ds(0, half)],
                2,
                recv_sem.at[h],
            )

        @pl.when(jnp.logical_and(is_second, h != 0))
        def _():
            pass_on(h * side * cores, side * cores)

        @pl.when(jnp.logical_and(is_second, h == 0))
        def _():
            pass_on(1, side * cores - 1)


    wind = send[me][half : half + 1, :]
    other = pltpu.roll(wind, SEA_DEV, 1)
    odd_side = lax.rem(me, 2) * SEA_DEV
    even_half = lambda shape: jnp.bitwise_xor(lax.broadcasted_iota(jnp.int32, shape, 1), odd_side) < SEA_DEV
    low16 = even_half((PAIRS, 128))
    speed = jnp.where(even_half((1, 128)), wind, other)
    angle = jnp.where(even_half((1, 128)), other, wind)

    def paired(name):
        rows = tab[at[name] : at[name] + PAIRS, :]
        return jnp.where(odd_side == 0, rows, pltpu.roll(rows, SEA_DEV, 1))

    toward = speed * (paired("pair_cos") * jnp.cos(angle) + paired("pair_sin") * jnp.sin(angle))
    zero16 = jnp.zeros((PAIRS, 128), jnp.float32)
    for w in range(4):
        for k in (0, 1, 2, NF + 3, NF + 4):
            rolled[w, k] = zero16
    for k in range(2):
        low_part[k] = zero16
    for k in range(3):
        high_part[NF + k] = zero16

    def turns(a, amounts):
        s = pltpu.roll(a, SEA_DEV, 1)
        need = {1: (1, 0), -1: (0, -1), 3: (2, 1), -3: (-1, -2)}
        by = {0: s}
        for m in amounts:
            for w in need[m]:
                if w not in by:
                    by[w] = pltpu.roll(s, w % PAIRS, 0)
        return [jnp.where(low16, by[need[m][0]], by[need[m][1]]) for m in amounts]

    group = 8
    per_group = half * group // PAIRS

    def arrange(i, carry):
        m0, m1 = carry
        h = lax.rem(i + 1, side)
        hand_over(h)
        finish(recv, side * cores, half, recv_sem.at[h])
        for g in (2 * h, 2 * h + 1):
            for i in range(group):
                flat[g, half * i : half * i + half, :] = recv[g * group + i, 0:half, :]
        for g in (2 * h, 2 * h + 1):
            for q in range(per_group):
                k = g * per_group + q
                a = flat[g, PAIRS * q : PAIRS * (q + 1), :]
                energy[k] = a
                m0 = m0 + a
                m1 = m1 + tab[pl.ds(at["omega"] + k, 1), :] * a
                for w, b in enumerate(turns(a, (1, -1, 3, -3))):
                    rolled[w, k + 3] = b
        return m0, m1

    m0, m1 = lax.fori_loop(0, side, arrange, (zero16, zero16))

    def over_bins(a):
        a = jnp.sum(a, axis=0, keepdims=True)
        return (a + pltpu.roll(a, SEA_DEV, 1)) * (1.0 / (NF * ND))

    m0, m1 = over_bins(m0), over_bins(m1)
    mean_freq = m1 / (m0 + 1e-6)
    steep = m0 * mean_freq * mean_freq
    breaking = steep * steep / (1.0 + steep * steep)

    def transfer(g, carry):
        for q in range(4 * per_group):
            k = g * 4 * per_group + q
            a = energy[k]
            factor = tab[pl.ds(at["rate"] + k, 1), :] * a
            rates = []
            for plus, minus in ((rolled[1, k + 5], rolled[2, k]), (rolled[0, k + 5], rolled[3, k])):
                rates.append(factor * (a * (plus + minus) - 2.0 * plus * minus))
            up, down = turns(rates[0], (1, -3)), turns(rates[1], (-1, 3))
            own[k] = -2.0 * (rates[0] + rates[1])
            low_part[k + 2] = up[0] + down[0]
            high_part[k] = up[1] + down[1]
        return carry

    lax.fori_loop(0, n // group // 4, transfer, 0)

    def renew(h, total):
        for g in (2 * h, 2 * h + 1):
            for q in range(per_group):
                k = g * per_group + q
                a = energy[k]
                omega = tab[pl.ds(at["omega"] + k, 1), :]
                gain = (0.05 * omega) * jnp.maximum(0.0, omega * toward - 1.0)
                new = a + (gain - (0.03 * omega) * breaking) * a
                new = new + own[k] + low_part[k] + high_part[k + 3]
                total = total + new
                flat[g, PAIRS * q : PAIRS * (q + 1), :] = new
        for g in (2 * h, 2 * h + 1):
            for i in range(group):
                back[g * group + i, 0:half, :] = flat[g, half * i : half * i + half, :]
        return total

    total = lax.fori_loop(0, n // group // 2, renew, zero16)
    height = 4.0 * jnp.sqrt(over_bins(total) + 1e-6)

    swap[0, 0:1, :] = height
    partner = me + 1 - 2 * my_c
    copy_to(partner, swap.at[0, pl.ds(0, 1)], swap.at[1, pl.ds(0, 1)], 4, recv_sem.at[2 * side + 2])

    def push_back(to, rows, k):
        copy_to(
            to,
            back.at[to, pl.ds(0, rows)],
            home.at[me, pl.ds(0, rows)],
            (1, 3)[k],
            recv_sem.at[2 * side + k],
        )

    def on_core(core, rows, k):
        def chip(i, carry):
            px, py = wrap(my_x + order[0, i]), wrap(my_y + order[1, i])
            push_back((px * side + py) * cores + core, rows, k)
            return carry

        lax.fori_loop(0, len(chips), chip, 0)

    on_core(1 - my_c, half, 0)
    push_back(partner, half, 0)
    swapped = swap.at[1, pl.ds(0, 1)]
    pltpu.make_async_copy(swapped, swapped, recv_sem.at[2 * side + 2]).wait()
    theirs = swap[1, 0:1, :]
    both_heights = jnp.where(even_half((1, 128)), height, theirs)

    def add_height(g, carry):
        for i in range(group):
            back[g * group + i, half : half + 1, :] = both_heights
        return carry

    lax.fori_loop(0, n // group, add_height, 0)
    on_core(my_c, half + 1, 1)
    own_message(back, home, half + 1, recv_sem.at[2 * side + 1])

    @pl.when(is_second)
    def _():
        finish(send, n - 2, half, send_sem.at[0])
        finish(recv, n - 1, half, send_sem.at[2])

    @pl.when(jnp.logical_not(is_second))
    def _():
        finish(send, n - 1, half, send_sem.at[0])

    finish(home, n // cores, half, recv_sem.at[2 * side])
    finish(home, n // cores, half + 1, recv_sem.at[2 * side + 1])
    finish(back, n // cores, half, send_sem.at[1])
    finish(back, n // cores - 1, half + 1, send_sem.at[3])
    pltpu.make_async_copy(swapped, swapped, send_sem.at[4]).wait()


def unpack_kernel(
    n, bins_dev,
    home, go_right, put, mask2d,
    out, height_out, mean_out,
    moved_a, moved_b, stage, heights, result, own_heights, mean, write_sem,
):
    chunks = mask2d.shape[0]
    half = bins_dev // 2
    cells = chunks * 128
    per_row = NLON // 128
    me = lax.axis_index("spec")
    lane = lax.broadcasted_iota(jnp.int32, (8, 128), 1)
    low = lane < SEA_DEV

    row = lax.broadcasted_iota(jnp.int32, (8, 128), 0)
    own_core = jnp.where(lax.rem(me, 2) == 0, 0, SEA_DEV)
    from_even = (jnp.where(row == half, own_core, lane) < SEA_DEV, jnp.logical_not(low))

    def spread(r, carry):
        pairs = [(home[2 * (r + 8 * j)], home[2 * (r + 8 * j) + 1]) for j in range(n * SEA_DEV // 128 // 8)]
        for t in range(2):
            tiles = [jnp.where(from_even[t], p[0], p[1]) for p in pairs]
            for j, tile in enumerate(far_rows(chunks, go_right, tiles, t, r, False, (5, 4, 3))):
                moved_b[t, FAR + r + 8 * j] = tile
        return carry

    lax.fori_loop(0, 8, spread, 0)

    def keep_apart(t, u, v, tile):
        moved_a[t, FAR + v] = tile

    near_rows(chunks, go_right, moved_b, keep_apart, False, (2, 1, 0))

    width = 2 * UNROLL * 128

    def write(g):
        cols = pl.ds(pl.multiple_of(g * width, 128), width)
        return pltpu.make_async_copy(result.at[:, cols], out.at[:, cols], write_sem.at[g])

    def deliver(g, carry):
        for u in range(6 * UNROLL):
            v = g * 6 * UNROLL + u
            sea = jnp.broadcast_to(mask2d[pl.ds(v, 1), :] != 0, (8, 128))
            for t in range(2):
                tile = jnp.where(sea, lanes(moved_a[t, FAR + v], put.at[t], v), 0.0)
                stage[u, pl.ds(t, half, stride=2), :] = tile[0:half]
                if t == 0:
                    heights[pl.ds(v, 1), :] = tile[half : half + 1]
        for part in range(3):
            for u in range(part * 2 * UNROLL, (part + 1) * 2 * UNROLL):
                v = g * 6 * UNROLL + u
                result[:, pl.ds(pl.multiple_of(v * 128, 128), 128)] = stage[u, 0:bins_dev, :]
            write(3 * g + part).start()
        return carry

    lax.fori_loop(0, chunks // (6 * UNROLL), deliver, 0)

    points = cells // n
    together = NLON // points
    start = me // together * per_row
    three = [heights[pl.ds(start + q, 1), :] for q in range(per_row)]
    u = lax.rem(me, together)
    picked = None
    for g in range(together):
        first, offset = g * points // 128, g * points % 128
        piece = three[first]
        if offset:
            after = three[min(first + 1, per_row - 1)]
            piece = jnp.where(
                lane[0:1] < 128 - offset,
                pltpu.roll(piece, 128 - offset, 1),
                pltpu.roll(after, 128 - offset, 1),
            )
        picked = piece if picked is None else jnp.where(u == g, piece, picked)
    own_heights[...] = picked[:, 0:points]
    all_heights = jnp.sum(heights[...], axis=0, keepdims=True)
    mean[...] = jnp.sum(all_heights, axis=1, keepdims=True) * (1.0 / (SEA_DEV * n))

    small = (
        pltpu.make_async_copy(own_heights, height_out, write_sem.at[cells // width]),
        pltpu.make_async_copy(mean, mean_out, write_sem.at[cells // width + 1]),
    )
    for copy in small:
        copy.start()

    def written(g, carry):
        write(g).wait()
        return carry

    lax.fori_loop(0, cells // width, written, 0)
    for copy in small:
        copy.wait()


def solution(mesh):
    n = mesh.shape["spec"]
    cores = 2
    side = math.isqrt(n // cores)

    def local(spectrum, sea_mask, wind_speed, wind_angle):
        bins_dev, cells = spectrum.shape
        chunks = cells // 128
        padded = chunks + 2 * (NLON // 128)
        tab, at = tables(cells // NLON)
        vmem = pl.BlockSpec(memory_space=pltpu.VMEM)
        words = pltpu.VMEM((2, chunks + 2 * REACH, 128), jnp.int32)
        by_freq = lambda *dims: pltpu.VMEM((*dims, PAIRS, 128), jnp.float32)
        messages = lambda count: pltpu.VMEM((count, 8, 128), jnp.float32)
        home, go_right, put = pl.pallas_call(
            functools.partial(step_kernel, n, side, cores, at),
            name="wave_step",
            out_shape=(
                jax.ShapeDtypeStruct((n, 8, 128), jnp.float32),
                jax.ShapeDtypeStruct((2, chunks + 2 * REACH, 128), jnp.int32),
                jax.ShapeDtypeStruct((2, chunks, 128), jnp.int32),
            ),
            in_specs=[pl.BlockSpec(memory_space=pltpu.HBM)] * 5,
            out_specs=(vmem,) * 3,
            scratch_shapes=[
                pltpu.VMEM((bins_dev, cells), jnp.float32),
                pltpu.VMEM((chunks, 128), jnp.int32),
                pltpu.VMEM((chunks, 128), jnp.float32),
                pltpu.VMEM((chunks, 128), jnp.float32),
                pltpu.VMEM((chunks, 128), jnp.float32),
                pltpu.VMEM(tab.shape, jnp.float32),
                pltpu.VMEM((2, padded, 8, 128), jnp.float32),
                pltpu.VMEM((2, padded, 8, 128), jnp.float32),
                pltpu.VMEM((8, 16, 128), jnp.float32),
                pltpu.VMEM((chunks + REACH, 128), jnp.int32),
                words,
                pltpu.VMEM((2, chunks, 128), jnp.int32),
                pltpu.VMEM((2, chunks + 2 * FAR, 8, 128), jnp.float32),
                pltpu.VMEM((2, chunks + 2 * FAR, 8, 128), jnp.float32),
                messages(n),
                messages(2 * n),
                messages(n),
                messages(2),
                pltpu.VMEM((n // 8, 8 * bins_dev // 2, 128), jnp.float32),
                by_freq(NF),
                by_freq(4, NF + 5),
                by_freq(NF),
                by_freq(NF + 2),
                by_freq(NF + 3),
                pltpu.SMEM((4, side * side), jnp.int32),
                pltpu.SemaphoreType.DMA((5,)),
                pltpu.SemaphoreType.DMA((2 * side + 3,)),
                pltpu.SemaphoreType.DMA((8,)),
                pltpu.SemaphoreType.REGULAR((side,)),
                pltpu.SemaphoreType.REGULAR,
            ],
            compiler_params=pltpu.CompilerParams(
                collective_id=0, has_side_effects=True, vmem_limit_bytes=VMEM_BYTES
            ),
        )(
            *(
                pltpu.with_memory_space_constraint(a, pltpu.HBM)
                for a in (
                    spectrum,
                    sea_mask.reshape(chunks, 128),
                    wind_speed.reshape(chunks, 128),
                    wind_angle.reshape(chunks, 128),
                    jnp.asarray(tab),
                )
            )
        )
        moved = pltpu.VMEM((2, chunks + 2 * FAR, 8, 128), jnp.float32)
        new_spectrum, height, mean = pl.pallas_call(
            functools.partial(unpack_kernel, n, bins_dev),
            name="unpack",
            out_shape=(
                jax.ShapeDtypeStruct((bins_dev, cells), jnp.float32),
                jax.ShapeDtypeStruct((1, cells // n), jnp.float32),
                jax.ShapeDtypeStruct((1, 1), jnp.float32),
            ),
            in_specs=[vmem] * 4,
            out_specs=(pl.BlockSpec(memory_space=pl.ANY),) * 3,
            scratch_shapes=[
                moved,
                moved,
                pltpu.VMEM((48, 16, 128), jnp.float32),
                pltpu.VMEM((chunks, 128), jnp.float32),
                pltpu.VMEM((bins_dev, cells), jnp.float32),
                pltpu.VMEM((1, cells // n), jnp.float32),
                pltpu.VMEM((1, 1), jnp.float32),
                pltpu.SemaphoreType.DMA((chunks // (2 * UNROLL) + 2,)),
            ],
            compiler_params=pltpu.CompilerParams(vmem_limit_bytes=VMEM_BYTES),
        )(home, go_right, put, sea_mask.reshape(chunks, 128))
        return new_spectrum, height.reshape(-1), mean.reshape(1)

    return jax.shard_map(
        local,
        mesh=mesh,
        in_specs=(P(("grp", "spec"), None), P(), P("grp"), P("grp")),
        out_specs=(P(("grp", "spec"), None), P(("grp", "spec")), P("grp")),
        check_vma=False,
    )
```
